16 devices in a mesh: dp: 4 (over z, y), tp: 4 (over x, core).
Axes of the slice: x: 2, y: 2, z: 2, core: 2. Of those that a mesh axis runs over, the one named last changes fastest.
Arguments:
- hidden: bfloat16 [8, 512, 768], P('dp', None, 'tp'), parts along dimension 0
- ln_scale: float32 [768], P('tp')
- w_head: bfloat16 [768, 32128], P(None, 'tp')
- targets: int32 [8, 512], P('dp'), parts along dimension 0
- valid_mask: int32 [8, 512], P('dp'), parts along dimension 0
Outputs:
- output 1: float32 [8, 512], P('dp'), parts along dimension 0
- output 2: float32 [8], P('dp'), parts along dimension 0
There are 4 independent parts. The reference program is written for one: setup_inputs(seed, part) draws one part's arguments, and reference() takes and returns one part's arrays. A program takes and returns all parts, laid end to end along the dimension named above; an argument that names none is the same for every part.
All inputs are finite; a program needn't handle non-finite values.
Results may differ from the reference program's by a relative error of at most 0.001.
Values are sent between devices in bfloat16 or wider.
A program may use at most 1 GiB of HBM per device.

```python
import math
import jax
import jax.numpy as jnp
from jax import lax

D = 768
VOCAB_SIZE = 32128
SEQ_COUNT = 2
SEQ_LEN = 512
REGIONS = 16
ROW_BLOCK = 32

NORM_EPS = 1e-6


def setup_inputs(seed: int = 0, part: int = 0) -> dict:
    base_key = jax.random.key(seed)
    key_head, key_scale = jax.random.split(base_key, 2)
    part_key = jax.random.fold_in(base_key, part)
    key_noise, key_gain, key_boost, key_route = jax.random.split(part_key, 4)
    key_tgt, key_len, key_pick = jax.random.split(key_route, 3)
    tokens = SEQ_COUNT * SEQ_LEN
    w_f32 = jax.random.normal(key_head, (D, VOCAB_SIZE), jnp.float32) * (2.0 / math.sqrt(D))
    w_head = w_f32.astype(jnp.bfloat16)
    ln_scale = jax.random.uniform(key_scale, (D,), jnp.float32, 0.5, 1.5)
    target_ids = jax.random.randint(key_tgt, (SEQ_COUNT, SEQ_LEN), 0, VOCAB_SIZE, jnp.int32)
    target_ids = target_ids.at[0, 0].set(VOCAB_SIZE - 1).at[0, 1].set(0)
    lengths = jax.random.randint(key_len, (SEQ_COUNT,), 1, SEQ_LEN, jnp.int32)
    full_pick = jax.random.randint(key_pick, (), 0, SEQ_COUNT, jnp.int32)
    lengths = jnp.where(jnp.arange(SEQ_COUNT) == full_pick, SEQ_LEN, lengths)
    valid_mask = (jnp.arange(SEQ_LEN)[None, :] < lengths[:, None]).astype(jnp.int32)
    noise_f32 = jax.random.normal(key_noise, (SEQ_COUNT, SEQ_LEN, D), jnp.float32)
    region_gain = jnp.exp(0.8 * jax.random.normal(key_gain, (SEQ_COUNT, SEQ_LEN, REGIONS), jnp.float32))
    base_rows = noise_f32 * jnp.repeat(region_gain, D // REGIONS, axis=2)
    base_rms = jnp.sqrt(jnp.mean(base_rows * base_rows, axis=-1, keepdims=True))
    boost_amt = jax.random.uniform(key_boost, (SEQ_COUNT, SEQ_LEN, 1), jnp.float32, 0.0, 6.0)
    target_cols = jnp.take(w_head, target_ids.reshape(tokens), axis=1).T.reshape(SEQ_COUNT, SEQ_LEN, D)
    hidden = (base_rows + boost_amt * base_rms * target_cols.astype(jnp.float32)).astype(jnp.bfloat16)
    return {"hidden": hidden, "ln_scale": ln_scale, "w_head": w_head, "targets": target_ids, "valid_mask": valid_mask}


def reference(hidden, ln_scale, w_head, targets, valid_mask):
    tokens = SEQ_COUNT * SEQ_LEN
    row_blocks = hidden.reshape(tokens // ROW_BLOCK, ROW_BLOCK, D)
    tgt_blocks = targets.reshape(tokens // ROW_BLOCK, ROW_BLOCK)

    def score_block(block_args):
        row_blk, tgt_blk = block_args
        row_f32 = row_blk.astype(jnp.float32)
        inv_rms = lax.rsqrt(jnp.mean(row_f32 * row_f32, axis=-1, keepdims=True) + NORM_EPS)
        normed = (row_f32 * inv_rms * ln_scale).astype(jnp.bfloat16)
        logits = jnp.dot(normed, w_head, preferred_element_type=jnp.float32)
        row_max = jnp.max(logits, axis=-1, keepdims=True)
        log_norm = row_max[:, 0] + jnp.log(jnp.sum(jnp.exp(logits - row_max), axis=-1))
        picked = jnp.take_along_axis(logits, tgt_blk[:, None], axis=1)[:, 0]
        return picked - log_norm

    tok_all = lax.map(score_block, (row_blocks, tgt_blocks)).reshape(SEQ_COUNT, SEQ_LEN)
    token_logp = valid_mask.astype(jnp.float32) * tok_all
    seq_logp = jnp.sum(token_logp, axis=1)
    return (token_logp, seq_logp)
```

```python
import functools

import jax
import jax.numpy as jnp
from jax import lax
from jax.experimental import pallas as pl
from jax.experimental.pallas import tpu as pltpu
from jax.sharding import PartitionSpec as P

NORM_EPS = 1e-6
LOG2E = 1.4426950408889634
MESH = pl.DeviceIdType.MESH
LANES = 128


def head_kernel(
    cfg, h_ref, g_ref, w_ref, tgt_ref, out_ref,
    wbuf, hrx, grx, tbuf, gcol, xbuf, zbuf, stx, srx,
    w_sem, own_sem, small_sem, psend, precv, xsend, xrecv, fsend, frecv, gsend, grecv, ssend, srecv,
):
    d_local, v_local, rows, chunk, block = cfg
    n_chunks = rows // chunk
    d_full = 4 * d_local
    per_seq = h_ref.shape[2]
    per_chunk = per_seq // chunk
    starts = list(range(0, v_local, block))
    n_blocks = len(starts)

    me = lax.axis_index("tp")
    peer = me + 1 - 2 * lax.rem(me, 2)
    cross = lax.rem(me + 2, 4)
    diag = lax.rem(peer + 2, 4)
    others = (peer, cross, diag)

    def piece(owner, k):
        return hrx.at[k, pl.ds(pl.multiple_of(owner * d_local, d_local), d_local)]

    own = [
        pltpu.make_async_copy(
            h_ref.at[k // per_chunk, :, pl.ds((k % per_chunk) * chunk, chunk)], piece(me, k), own_sem.at[k]
        )
        for k in range(n_chunks)
    ]
    own_g = pltpu.make_async_copy(g_ref, grx.at[me], small_sem.at[0])
    own_t = pltpu.make_async_copy(tgt_ref, tbuf, small_sem.at[1])
    load_w = pltpu.make_async_copy(w_ref, wbuf, w_sem)
    own[0].start()
    own_g.start()
    own_t.start()
    for k in range(1, n_chunks):
        own[k].start()
    load_w.start()

    barrier = pltpu.get_barrier_semaphore()
    for other in others:
        pl.semaphore_signal(barrier, inc=1, device_id={"tp": other}, device_id_type=MESH)
    pl.semaphore_wait(barrier, 3)

    def remote(src, dst, send, recv, dev):
        return pltpu.make_async_remote_copy(
            src_ref=src, dst_ref=dst, send_sem=send, recv_sem=recv, device_id={"tp": dev}, device_id_type=MESH
        )

    def cross_copy(k):
        return remote(piece(me, k), piece(me, k), xsend.at[k], xrecv.at[k], cross)

    def peer_copy(k):
        return remote(piece(me, k), piece(me, k), psend.at[k], precv.at[k], peer)

    def forward_copy(k):
        return remote(piece(cross, k), piece(cross, k), fsend.at[k], frecv.at[k], peer)

    def gain_copy(n):
        return remote(grx.at[me], grx.at[me], gsend.at[n], grecv.at[n], others[n])

    def stat_copy(n, k):
        return remote(stx.at[k], srx.at[n, k], ssend.at[n, k], srecv.at[n, k], others[n])

    own[0].wait()
    cross_copy(0).start()
    peer_copy(0).start()
    own_g.wait()
    for n in range(3):
        gain_copy(n).start()
    for k in range(1, n_chunks):
        own[k].wait()
        cross_copy(k).start()
        peer_copy(k).start()
    own_t.wait()

    for n in range(3):
        gain_copy(n).wait_recv()
    for s in range(4):
        for lo in range(0, d_local, LANES):
            size = min(LANES, d_local - lo)
            row = grx[s, :, lo : lo + size]
            row = jnp.concatenate([row] * (LANES // size), axis=-1)
            gcol[s * d_local + lo : s * d_local + lo + size, :] = jnp.broadcast_to(row, (LANES, LANES)).T[0:size]

    group = 32

    def normalise(k, slot):
        def square(i, acc):
            at = pl.ds(pl.multiple_of(i * group, group), group)
            part = hrx[k, at, :].astype(jnp.float32)
            return acc + part * part

        sq = lax.fori_loop(0, d_full // group, square, jnp.zeros((group, chunk), jnp.float32), unroll=True)
        inv = lax.rsqrt(jnp.sum(sq, axis=0, keepdims=True) / d_full + NORM_EPS)

        def scale(i, carry):
            at = pl.ds(pl.multiple_of(i * group, group), group)
            gain = gcol[at, :]
            part = hrx[k, at, :].astype(jnp.float32)
            gains = jnp.concatenate([gain] * (chunk // LANES), axis=-1)
            xbuf[slot, at, :] = (part * inv * gains).astype(jnp.bfloat16)
            return carry

        lax.fori_loop(0, d_full // group, scale, 0, unroll=True)

    sub = lax.broadcasted_iota(jnp.int32, (8, chunk), 0)

    def logits(j, xslot, zslot):
        lo = starts[j]
        size = min(block, v_local - lo)
        z = jnp.dot(wbuf[lo : lo + size, :], xbuf[xslot], preferred_element_type=jnp.float32)
        zbuf[zslot, 0:size, :] = z

    def epilogue(j, zslot, want, state):
        lo = starts[j]
        size = min(block, v_local - lo)

        def tile(i):
            return zbuf[zslot, pl.ds(pl.multiple_of(i * 8, 8), 8), :]

        top = lax.fori_loop(1, size // 8, lambda i, t: jnp.maximum(t, tile(i)), tile(0), unroll=True)
        if state is None:
            total = jnp.zeros((8, chunk), jnp.float32)
            pick = total
        else:
            old, total, pick = state
            top = jnp.maximum(top, old)
            total = total * jnp.exp2((old - top) * LOG2E)

        def add(i, carry):
            total, pick = carry
            z = tile(i)
            total = total + jnp.exp2((z - top) * LOG2E)
            pick = jnp.where(want == lo + i * 8, z, pick)
            return total, pick

        total, pick = lax.fori_loop(0, size // 8, add, (total, pick), unroll=True)
        return top, total, pick

    def finish_chunk(k, state):
        m, total, pick = state
        top = jnp.max(m, axis=0, keepdims=True)
        stx[k, 0:1, :] = top
        stx[k, 1:2, :] = jnp.sum(total * jnp.exp2((m - top) * LOG2E), axis=0, keepdims=True)
        stx[k, 2:3, :] = jnp.sum(pick, axis=0, keepdims=True)

    cross_copy(0).wait_recv()
    forward_copy(0).start()
    peer_copy(0).wait_recv()
    forward_copy(0).wait_recv()
    normalise(0, 0)
    load_w.wait()

    half = n_blocks // 2

    def step(k, carry):
        xslot = lax.rem(k, 2)
        row = tbuf[pl.ds(k // per_chunk, 1), pl.ds(pl.multiple_of(lax.rem(k, per_chunk) * chunk, chunk), chunk)]
        local = row - me * v_local
        local = jnp.where((local >= 0) & (local < v_local), local, jnp.int32(-(1 << 20)))
        want = jnp.broadcast_to(local, (8, chunk)) - sub
        state = None
        for j in range(n_blocks):
            if j == half:
                @pl.when(k < n_chunks - 1)
                def _():
                    cross_copy(k + 1).wait_recv()
                    forward_copy(k + 1).start()

            if j == n_blocks - 1:
                @pl.when(k < n_chunks - 1)
                def _():
                    peer_copy(k + 1).wait_recv()
                    forward_copy(k + 1).wait_recv()

            logits(j, xslot, j % 2)
            if j:
                state = epilogue(j - 1, (j - 1) % 2, want, state)
            if j == n_blocks - 1:
                normalise(lax.min(k + 1, n_chunks - 1), 1 - xslot)
        state = epilogue(n_blocks - 1, (n_blocks - 1) % 2, want, state)
        finish_chunk(k, state)
        for n in range(3):
            stat_copy(n, k).start()
        return carry

    lax.fori_loop(0, n_chunks, step, 0)

    for k in range(n_chunks):
        for n in range(3):
            stat_copy(n, k).wait_recv()
        stats = [stx[k]] + [srx[n, k] for n in range(3)]
        top = stats[0][0:1]
        for st in stats[1:]:
            top = jnp.maximum(top, st[0:1])
        total = jnp.zeros_like(top)
        pick = jnp.zeros_like(top)
        for st in stats:
            total = total + st[1:2] * jnp.exp2((st[0:1] - top) * LOG2E)
            pick = pick + st[2:3]
        seq, pos = divmod(k * chunk, per_seq)
        out_ref[seq : seq + 1, pos : pos + chunk] = pick - (top + jnp.log(total))

    for k in range(n_chunks):
        cross_copy(k).wait_send()
        peer_copy(k).wait_send()
        forward_copy(k).wait_send()
        for n in range(3):
            stat_copy(n, k).wait_send()
    for n in range(3):
        gain_copy(n).wait_send()


def solution(mesh):
    def local_score(hidden, ln_scale, w_head, targets, valid_mask):
        b, l, d_local = hidden.shape
        v_local = w_head.shape[1]
        rows, chunk, block = b * l, 256, 512
        n_chunks = rows // chunk
        any_spec = pl.BlockSpec(memory_space=pl.ANY)
        f32 = jnp.float32
        dma = pltpu.SemaphoreType.DMA
        token = pl.pallas_call(
            functools.partial(head_kernel, (d_local, v_local, rows, chunk, block)),
            out_shape=jax.ShapeDtypeStruct((b, l), f32),
            in_specs=[any_spec] * 4,
            out_specs=pl.BlockSpec(memory_space=pltpu.VMEM),
            scratch_shapes=[
                pltpu.VMEM((v_local, 4 * d_local), jnp.bfloat16),
                pltpu.VMEM((n_chunks, 4 * d_local, chunk), jnp.bfloat16),
                pltpu.VMEM((4, 1, d_local), f32),
                pltpu.VMEM((b, l), jnp.int32),
                pltpu.VMEM((4 * d_local, LANES), f32),
                pltpu.VMEM((2, 4 * d_local, chunk), jnp.bfloat16),
                pltpu.VMEM((2, block, chunk), f32),
                pltpu.VMEM((n_chunks, 8, chunk), f32),
                pltpu.VMEM((3, n_chunks, 8, chunk), f32),
                dma,
                dma((n_chunks,)),
                dma((2,)),
                dma((n_chunks,)), dma((n_chunks,)),
                dma((n_chunks,)), dma((n_chunks,)),
                dma((n_chunks,)), dma((n_chunks,)),
                dma((3,)), dma((3,)),
                dma((3, n_chunks)), dma((3, n_chunks)),
            ],
            compiler_params=pltpu.CompilerParams(
                collective_id=0, has_side_effects=True, vmem_limit_bytes=62 * 1024 * 1024
            ),
        )(hidden.transpose(0, 2, 1), ln_scale.reshape(1, d_local), w_head.T, targets)
        token_logp = valid_mask.astype(f32) * token
        return token_logp, jnp.sum(token_logp, axis=1)

    return jax.shard_map(
        local_score,
        mesh=mesh,
        in_specs=(P("dp", None, "tp"), P("tp"), P(None, "tp"), P("dp", None), P("dp", None)),
        out_specs=(P("dp", None), P("dp")),
        check_vma=False,
    )
```

```python
import functools

import jax
import jax.numpy as jnp
from jax import lax
from jax.experimental import pallas as pl
from jax.experimental.pallas import tpu as pltpu
from jax.sharding import PartitionSpec as P

NORM_EPS = 1e-6
LOG2E = 1.4426950408889634
MESH = pl.DeviceIdType.MESH
LANES = 128


def head_kernel(
    cfg, h_ref, g_ref, w_ref, tgt_ref, out_ref,
    wbuf, hrx, grx, tbuf, gcol, xbuf, zbuf, stx, srx,
    w_sem, own_sem, small_sem, psend, precv, xsend, xrecv, fsend, frecv, gsend, grecv, ssend, srecv,
):
    d_local, v_local, rows, chunk, block = cfg
    n_chunks = rows // chunk
    d_full = 4 * d_local
    per_seq = h_ref.shape[2]
    per_chunk = per_seq // chunk
    starts = list(range(0, v_local, block))
    n_blocks = len(starts)

    me = lax.axis_index("tp")
    peer = me + 1 - 2 * lax.rem(me, 2)
    cross = lax.rem(me + 2, 4)
    diag = lax.rem(peer + 2, 4)
    others = (peer, cross, diag)

    def piece(owner, k):
        return hrx.at[k, pl.ds(pl.multiple_of(owner * d_local, d_local), d_local)]

    own = [
        pltpu.make_async_copy(
            h_ref.at[k // per_chunk, :, pl.ds((k % per_chunk) * chunk, chunk)], piece(me, k), own_sem.at[k]
        )
        for k in range(n_chunks)
    ]
    own_g = pltpu.make_async_copy(g_ref, grx.at[me], small_sem.at[0])
    own_t = pltpu.make_async_copy(tgt_ref, tbuf, small_sem.at[1])
    load_w = pltpu.make_async_copy(w_ref, wbuf, w_sem)
    own_g.start()
    for k in range(n_chunks):
        own[k].start()
    own_t.start()
    load_w.start()

    barrier = pltpu.get_barrier_semaphore()
    for other in others:
        pl.semaphore_signal(barrier, inc=1, device_id={"tp": other}, device_id_type=MESH)
    pl.semaphore_wait(barrier, 3)

    def remote(src, dst, send, recv, dev):
        return pltpu.make_async_remote_copy(
            src_ref=src, dst_ref=dst, send_sem=send, recv_sem=recv, device_id={"tp": dev}, device_id_type=MESH
        )

    def cross_copy(k):
        return remote(piece(me, k), piece(me, k), xsend.at[k], xrecv.at[k], cross)

    def peer_copy(k):
        return remote(piece(me, k), piece(me, k), psend.at[k], precv.at[k], peer)

    def forward_copy(k):
        return remote(piece(cross, k), piece(cross, k), fsend.at[k], frecv.at[k], peer)

    def gain_copy(n):
        return remote(grx.at[me], grx.at[me], gsend.at[n], grecv.at[n], others[n])

    def stat_copy(n, k):
        return remote(stx.at[k], srx.at[n, k], ssend.at[n, k], srecv.at[n, k], others[n])

    own_g.wait()
    for n in range(3):
        gain_copy(n).start()
    for k in range(n_chunks):
        own[k].wait()
        cross_copy(k).start()
        peer_copy(k).start()
    own_t.wait()

    for n in range(3):
        gain_copy(n).wait_recv()
    for s in range(4):
        for lo in range(0, d_local, LANES):
            size = min(LANES, d_local - lo)
            row = grx[s, :, lo : lo + size]
            row = jnp.concatenate([row] * (LANES // size), axis=-1)
            gcol[s * d_local + lo : s * d_local + lo + size, :] = jnp.broadcast_to(row, (LANES, LANES)).T[0:size]

    group = 32

    def normalise(k, slot):
        def square(i, acc):
            at = pl.ds(pl.multiple_of(i * group, group), group)
            part = hrx[k, at, :].astype(jnp.float32)
            return acc + part * part

        sq = lax.fori_loop(0, d_full // group, square, jnp.zeros((group, chunk), jnp.float32), unroll=True)
        inv = lax.rsqrt(jnp.sum(sq, axis=0, keepdims=True) / d_full + NORM_EPS)

        def scale(i, carry):
            at = pl.ds(pl.multiple_of(i * group, group), group)
            gain = gcol[at, :]
            part = hrx[k, at, :].astype(jnp.float32)
            gains = jnp.concatenate([gain] * (chunk // LANES), axis=-1)
            xbuf[slot, at, :] = (part * inv * gains).astype(jnp.bfloat16)
            return carry

        lax.fori_loop(0, d_full // group, scale, 0, unroll=True)

    sub = lax.broadcasted_iota(jnp.int32, (8, chunk), 0)

    def logits(j, xslot, zslot):
        lo = starts[j]
        size = min(block, v_local - lo)
        z = jnp.dot(wbuf[lo : lo + size, :], xbuf[xslot], preferred_element_type=jnp.float32)
        zbuf[zslot, 0:size, :] = z

    def epilogue(j, zslot, want, state):
        lo = starts[j]
        size = min(block, v_local - lo)

        def tile(i):
            return zbuf[zslot, pl.ds(pl.multiple_of(i * 8, 8), 8), :]

        top = lax.fori_loop(1, size // 8, lambda i, t: jnp.maximum(t, tile(i)), tile(0), unroll=True)
        if state is None:
            total = jnp.zeros((8, chunk), jnp.float32)
            pick = total
        else:
            old, total, pick = state
            top = jnp.maximum(top, old)
            total = total * jnp.exp2((old - top) * LOG2E)

        def add(i, carry):
            total, pick = carry
            z = tile(i)
            total = total + jnp.exp2((z - top) * LOG2E)
            pick = jnp.where(want == lo + i * 8, z, pick)
            return total, pick

        total, pick = lax.fori_loop(0, size // 8, add, (total, pick), unroll=True)
        return top, total, pick

    def finish_chunk(k, state):
        m, total, pick = state
        top = jnp.max(m, axis=0, keepdims=True)
        stx[k, 0:1, :] = top
        stx[k, 1:2, :] = jnp.sum(total * jnp.exp2((m - top) * LOG2E), axis=0, keepdims=True)
        stx[k, 2:3, :] = jnp.sum(pick, axis=0, keepdims=True)

    cross_copy(0).wait_recv()
    forward_copy(0).start()
    peer_copy(0).wait_recv()
    forward_copy(0).wait_recv()
    normalise(0, 0)
    load_w.wait()

    half = n_blocks // 2

    def step(k, carry):
        xslot = lax.rem(k, 2)
        row = tbuf[pl.ds(k // per_chunk, 1), pl.ds(pl.multiple_of(lax.rem(k, per_chunk) * chunk, chunk), chunk)]
        local = row - me * v_local
        local = jnp.where((local >= 0) & (local < v_local), local, jnp.int32(-(1 << 20)))
        want = jnp.broadcast_to(local, (8, chunk)) - sub
        state = None
        for j in range(n_blocks):
            if j == half:
                @pl.when(k < n_chunks - 1)
                def _():
                    cross_copy(k + 1).wait_recv()
                    forward_copy(k + 1).start()

            if j == n_blocks - 1:
                @pl.when(k < n_chunks - 1)
                def _():
                    peer_copy(k + 1).wait_recv()
                    forward_copy(k + 1).wait_recv()

            logits(j, xslot, j % 2)
            if j:
                state = epilogue(j - 1, (j - 1) % 2, want, state)
            if j == n_blocks - 1:
                normalise(lax.min(k + 1, n_chunks - 1), 1 - xslot)
        state = epilogue(n_blocks - 1, (n_blocks - 1) % 2, want, state)
        finish_chunk(k, state)
        for n in range(3):
            stat_copy(n, k).start()
        return carry

    lax.fori_loop(0, n_chunks, step, 0)

    for k in range(n_chunks):
        for n in range(3):
            stat_copy(n, k).wait_recv()
        stats = [stx[k]] + [srx[n, k] for n in range(3)]
        top = stats[0][0:1]
        for st in stats[1:]:
            top = jnp.maximum(top, st[0:1])
        total = jnp.zeros_like(top)
        pick = jnp.zeros_like(top)
        for st in stats:
            total = total + st[1:2] * jnp.exp2((st[0:1] - top) * LOG2E)
            pick = pick + st[2:3]
        seq, pos = divmod(k * chunk, per_seq)
        out_ref[seq : seq + 1, pos : pos + chunk] = pick - (top + jnp.log(total))

    for k in range(n_chunks):
        cross_copy(k).wait_send()
        peer_copy(k).wait_send()
        forward_copy(k).wait_send()
        for n in range(3):
            stat_copy(n, k).wait_send()
    for n in range(3):
        gain_copy(n).wait_send()


def solution(mesh):
    def local_score(hidden, ln_scale, w_head, targets, valid_mask):
        b, l, d_local = hidden.shape
        v_local = w_head.shape[1]
        rows, chunk, block = b * l, 256, 512
        n_chunks = rows // chunk
        any_spec = pl.BlockSpec(memory_space=pl.ANY)
        f32 = jnp.float32
        dma = pltpu.SemaphoreType.DMA
        token = pl.pallas_call(
            functools.partial(head_kernel, (d_local, v_local, rows, chunk, block)),
            out_shape=jax.ShapeDtypeStruct((b, l), f32),
            in_specs=[any_spec] * 4,
            out_specs=pl.BlockSpec(memory_space=pltpu.VMEM),
            scratch_shapes=[
                pltpu.VMEM((v_local, 4 * d_local), jnp.bfloat16),
                pltpu.VMEM((n_chunks, 4 * d_local, chunk), jnp.bfloat16),
                pltpu.VMEM((4, 1, d_local), f32),
                pltpu.VMEM((b, l), jnp.int32),
                pltpu.VMEM((4 * d_local, LANES), f32),
                pltpu.VMEM((2, 4 * d_local, chunk), jnp.bfloat16),
                pltpu.VMEM((2, block, chunk), f32),
                pltpu.VMEM((n_chunks, 8, chunk), f32),
                pltpu.VMEM((3, n_chunks, 8, chunk), f32),
                dma,
                dma((n_chunks,)),
                dma((2,)),
                dma((n_chunks,)), dma((n_chunks,)),
                dma((n_chunks,)), dma((n_chunks,)),
                dma((n_chunks,)), dma((n_chunks,)),
                dma((3,)), dma((3,)),
                dma((3, n_chunks)), dma((3, n_chunks)),
            ],
            compiler_params=pltpu.CompilerParams(
                collective_id=0, has_side_effects=True, vmem_limit_bytes=40 * 1024 * 1024
            ),
        )(*[
            pltpu.with_memory_space_constraint(x, pltpu.HBM)
            for x in (hidden.transpose(0, 2, 1), ln_scale.reshape(1, d_local), w_head.T, targets)
        ])
        token_logp = valid_mask.astype(f32) * token
        return token_logp, jnp.sum(token_logp, axis=1)

    return jax.shard_map(
        local_score,
        mesh=mesh,
        in_specs=(P("dp", None, "tp"), P("tp"), P(None, "tp"), P("dp", None), P("dp", None)),
        out_specs=(P("dp", None), P("dp")),
        check_vma=False,
    )
```

```python
import functools

import jax
import jax.numpy as jnp
from jax import lax
from jax.experimental import pallas as pl
from jax.experimental.pallas import tpu as pltpu
from jax.sharding import PartitionSpec as P

NORM_EPS = 1e-6
LOG2E = 1.4426950408889634
MESH = pl.DeviceIdType.MESH
LANES = 128


def head_kernel(
    cfg, h_ref, g_ref, w_ref, tgt_ref, out_ref,
    wbuf, hrx, grx, tbuf, gcol, xbuf, zbuf, stx, srx,
    w_sem, own_sem, small_sem, psend, precv, xsend, xrecv, fsend, frecv, gsend, grecv, ssend, srecv,
):
    d_local, v_local, rows, chunk, block, w_parts = cfg
    n_chunks = rows // chunk
    d_full = 4 * d_local
    per_seq = h_ref.shape[2]
    per_chunk = per_seq // chunk
    starts = list(range(0, v_local, block))
    n_blocks = len(starts)

    me = lax.axis_index("tp")
    peer = me + 1 - 2 * lax.rem(me, 2)
    cross = lax.rem(me + 2, 4)
    diag = lax.rem(peer + 2, 4)
    others = (peer, cross, diag)

    def piece(owner, k):
        return hrx.at[k, pl.ds(pl.multiple_of(owner * d_local, d_local), d_local)]

    own = [
        pltpu.make_async_copy(
            h_ref.at[k // per_chunk, :, pl.ds((k % per_chunk) * chunk, chunk)], piece(me, k), own_sem.at[k]
        )
        for k in range(n_chunks)
    ]
    own_g = pltpu.make_async_copy(g_ref, grx.at[me], small_sem.at[0])
    own_t = pltpu.make_async_copy(tgt_ref, tbuf, small_sem.at[1])
    load_w = [
        pltpu.make_async_copy(w_ref.at[pl.ds(lo, size)], wbuf.at[pl.ds(lo, size)], w_sem.at[n])
        for n, (lo, size) in enumerate(w_parts)
    ]
    own_g.start()
    for k in range(n_chunks):
        own[k].start()
    own_t.start()

    barrier = pltpu.get_barrier_semaphore()
    for other in others:
        pl.semaphore_signal(barrier, inc=1, device_id={"tp": other}, device_id_type=MESH)
    pl.semaphore_wait(barrier, 3)

    def remote(src, dst, send, recv, dev):
        return pltpu.make_async_remote_copy(
            src_ref=src, dst_ref=dst, send_sem=send, recv_sem=recv, device_id={"tp": dev}, device_id_type=MESH
        )

    def cross_copy(k):
        return remote(piece(me, k), piece(me, k), xsend.at[k], xrecv.at[k], cross)

    def peer_copy(k):
        return remote(piece(me, k), piece(me, k), psend.at[k], precv.at[k], peer)

    def forward_copy(k):
        return remote(piece(cross, k), piece(cross, k), fsend.at[k], frecv.at[k], peer)

    def gain_copy(n):
        return remote(grx.at[me], grx.at[me], gsend.at[n], grecv.at[n], others[n])

    def stat_copy(n, k):
        return remote(stx.at[k], srx.at[n, k], ssend.at[n, k], srecv.at[n, k], others[n])

    own_g.wait()
    for n in range(3):
        gain_copy(n).start()
    for k in range(n_chunks):
        own[k].wait()
        cross_copy(k).start()
        peer_copy(k).start()
        if k == 1:
            load_w[0].start()
    for part in load_w[1:]:
        part.start()
    own_t.wait()

    for n in range(3):
        gain_copy(n).wait_recv()
    for s in range(4):
        for lo in range(0, d_local, LANES):
            size = min(LANES, d_local - lo)
            row = grx[s, :, lo : lo + size]
            row = jnp.concatenate([row] * (LANES // size), axis=-1)
            gcol[s * d_local + lo : s * d_local + lo + size, :] = jnp.broadcast_to(row, (LANES, LANES)).T[0:size]

    group = 32

    def normalise(k, slot):
        def square(i, acc):
            at = pl.ds(pl.multiple_of(i * group, group), group)
            part = hrx[k, at, :].astype(jnp.float32)
            return acc + part * part

        sq = lax.fori_loop(0, d_full // group, square, jnp.zeros((group, chunk), jnp.float32), unroll=True)
        inv = lax.rsqrt(jnp.sum(sq, axis=0, keepdims=True) / d_full + NORM_EPS)

        def scale(i, carry):
            at = pl.ds(pl.multiple_of(i * group, group), group)
            gain = gcol[at, :]
            part = hrx[k, at, :].astype(jnp.float32)
            gains = jnp.concatenate([gain] * (chunk // LANES), axis=-1)
            xbuf[slot, at, :] = (part * inv * gains).astype(jnp.bfloat16)
            return carry

        lax.fori_loop(0, d_full // group, scale, 0, unroll=True)

    sub = lax.broadcasted_iota(jnp.int32, (8, chunk), 0)

    def logits(j, xslot, zslot):
        lo = starts[j]
        size = min(block, v_local - lo)
        z = jnp.dot(wbuf[lo : lo + size, :], xbuf[xslot], preferred_element_type=jnp.float32)
        zbuf[zslot, 0:size, :] = z

    def epilogue(j, zslot, want, state):
        lo = starts[j]
        size = min(block, v_local - lo)

        def tile(i):
            return zbuf[zslot, pl.ds(pl.multiple_of(i * 8, 8), 8), :]

        top = lax.fori_loop(1, size // 8, lambda i, t: jnp.maximum(t, tile(i)), tile(0), unroll=True)
        if state is None:
            total = jnp.zeros((8, chunk), jnp.float32)
            pick = total
        else:
            old, total, pick = state
            top = jnp.maximum(top, old)
            total = total * jnp.exp2((old - top) * LOG2E)

        def add(i, carry):
            total, pick = carry
            z = tile(i)
            total = total + jnp.exp2((z - top) * LOG2E)
            pick = jnp.where(want == lo + i * 8, z, pick)
            return total, pick

        total, pick = lax.fori_loop(0, size // 8, add, (total, pick), unroll=True)
        return top, total, pick

    def finish_chunk(k, state):
        m, total, pick = state
        top = jnp.max(m, axis=0, keepdims=True)
        stx[k, 0:1, :] = top
        stx[k, 1:2, :] = jnp.sum(total * jnp.exp2((m - top) * LOG2E), axis=0, keepdims=True)
        stx[k, 2:3, :] = jnp.sum(pick, axis=0, keepdims=True)

    cross_copy(0).wait_recv()
    forward_copy(0).start()
    peer_copy(0).wait_recv()
    forward_copy(0).wait_recv()
    normalise(0, 0)
    for part in load_w:
        part.wait()

    half = n_blocks // 2

    def step(k, carry):
        xslot = lax.rem(k, 2)
        row = tbuf[pl.ds(k // per_chunk, 1), pl.ds(pl.multiple_of(lax.rem(k, per_chunk) * chunk, chunk), chunk)]
        local = row - me * v_local
        local = jnp.where((local >= 0) & (local < v_local), local, jnp.int32(-(1 << 20)))
        want = jnp.broadcast_to(local, (8, chunk)) - sub
        state = None
        for j in range(n_blocks):
            if j == half:
                @pl.when(k < n_chunks - 1)
                def _():
                    cross_copy(k + 1).wait_recv()
                    forward_copy(k + 1).start()

            if j == n_blocks - 1:
                @pl.when(k < n_chunks - 1)
                def _():
                    peer_copy(k + 1).wait_recv()
                    forward_copy(k + 1).wait_recv()

            logits(j, xslot, j % 2)
            if j:
                state = epilogue(j - 1, (j - 1) % 2, want, state)
            if j == n_blocks - 1:
                normalise(lax.min(k + 1, n_chunks - 1), 1 - xslot)
        state = epilogue(n_blocks - 1, (n_blocks - 1) % 2, want, state)
        finish_chunk(k, state)
        for n in range(3):
            stat_copy(n, k).start()
        return carry

    lax.fori_loop(0, n_chunks, step, 0)

    for k in range(n_chunks):
        for n in range(3):
            stat_copy(n, k).wait_recv()
        stats = [stx[k]] + [srx[n, k] for n in range(3)]
        top = stats[0][0:1]
        for st in stats[1:]:
            top = jnp.maximum(top, st[0:1])
        total = jnp.zeros_like(top)
        pick = jnp.zeros_like(top)
        for st in stats:
            total = total + st[1:2] * jnp.exp2((st[0:1] - top) * LOG2E)
            pick = pick + st[2:3]
        seq, pos = divmod(k * chunk, per_seq)
        out_ref[seq : seq + 1, pos : pos + chunk] = pick - (top + jnp.log(total))

    for k in range(n_chunks):
        cross_copy(k).wait_send()
        peer_copy(k).wait_send()
        forward_copy(k).wait_send()
        for n in range(3):
            stat_copy(n, k).wait_send()
    for n in range(3):
        gain_copy(n).wait_send()


def solution(mesh):
    def local_score(hidden, ln_scale, w_head, targets, valid_mask):
        b, l, d_local = hidden.shape
        v_local = w_head.shape[1]
        rows, chunk, block = b * l, 256, 512
        part = 2048
        w_parts = tuple((lo, min(part, v_local - lo)) for lo in range(0, v_local, part))
        n_chunks = rows // chunk
        any_spec = pl.BlockSpec(memory_space=pl.ANY)
        f32 = jnp.float32
        dma = pltpu.SemaphoreType.DMA
        token = pl.pallas_call(
            functools.partial(head_kernel, (d_local, v_local, rows, chunk, block, w_parts)),
            out_shape=jax.ShapeDtypeStruct((b, l), f32),
            in_specs=[any_spec] * 4,
            out_specs=pl.BlockSpec(memory_space=pltpu.VMEM),
            scratch_shapes=[
                pltpu.VMEM((v_local, 4 * d_local), jnp.bfloat16),
                pltpu.VMEM((n_chunks, 4 * d_local, chunk), jnp.bfloat16),
                pltpu.VMEM((4, 1, d_local), f32),
                pltpu.VMEM((b, l), jnp.int32),
                pltpu.VMEM((4 * d_local, LANES), f32),
                pltpu.VMEM((2, 4 * d_local, chunk), jnp.bfloat16),
                pltpu.VMEM((2, block, chunk), f32),
                pltpu.VMEM((n_chunks, 8, chunk), f32),
                pltpu.VMEM((3, n_chunks, 8, chunk), f32),
                dma((len(w_parts),)),
                dma((n_chunks,)),
                dma((2,)),
                dma((n_chunks,)), dma((n_chunks,)),
                dma((n_chunks,)), dma((n_chunks,)),
                dma((n_chunks,)), dma((n_chunks,)),
                dma((3,)), dma((3,)),
                dma((3, n_chunks)), dma((3, n_chunks)),
            ],
            compiler_params=pltpu.CompilerParams(
                collective_id=0, has_side_effects=True, vmem_limit_bytes=40 * 1024 * 1024
            ),
        )(*[
            pltpu.with_memory_space_constraint(x, pltpu.HBM)
            for x in (hidden.transpose(0, 2, 1), ln_scale.reshape(1, d_local), w_head.T, targets)
        ])
        token_logp = valid_mask.astype(f32) * token
        return token_logp, jnp.sum(token_logp, axis=1)

    return jax.shard_map(
        local_score,
        mesh=mesh,
        in_specs=(P("dp", None, "tp"), P("tp"), P(None, "tp"), P("dp", None), P("dp", None)),
        out_specs=(P("dp", None), P("dp")),
        check_vma=False,
    )
```

```python
import functools

import jax
import jax.numpy as jnp
from jax import lax
from jax.experimental import pallas as pl
from jax.experimental.pallas import tpu as pltpu
from jax.sharding import PartitionSpec as P

NORM_EPS = 1e-6
LOG2E = 1.4426950408889634
MESH = pl.DeviceIdType.MESH
LANES = 128


def head_kernel(
    cfg, h_ref, g_ref, w_ref, tgt_ref, out_ref,
    wbuf, hrx, grx, tbuf, gcol, xbuf, zbuf, stx, srx,
    w_sem, own_sem, small_sem, psend, precv, xsend, xrecv, fsend, frecv, gsend, grecv, ssend, srecv,
):
    d_local, v_local, rows, chunk, block, w_parts = cfg
    n_chunks = rows // chunk
    d_full = 4 * d_local
    per_seq = h_ref.shape[2]
    per_chunk = per_seq // chunk
    starts = list(range(0, v_local, block))
    n_blocks = len(starts)

    me = lax.axis_index("tp")
    peer = me + 1 - 2 * lax.rem(me, 2)
    cross = lax.rem(me + 2, 4)
    diag = lax.rem(peer + 2, 4)
    others = (peer, cross, diag)

    def piece(owner, k):
        return hrx.at[k, pl.ds(pl.multiple_of(owner * d_local, d_local), d_local)]

    own = [
        pltpu.make_async_copy(
            h_ref.at[k // per_chunk, :, pl.ds((k % per_chunk) * chunk, chunk)], piece(me, k), own_sem.at[k]
        )
        for k in range(n_chunks)
    ]
    own_g = pltpu.make_async_copy(g_ref, grx.at[me], small_sem.at[0])
    own_t = pltpu.make_async_copy(tgt_ref, tbuf, small_sem.at[1])
    load_w = [
        pltpu.make_async_copy(w_ref.at[pl.ds(lo, size)], wbuf.at[pl.ds(lo, size)], w_sem.at[n])
        for n, (lo, size) in enumerate(w_parts)
    ]
    own_g.start()
    for k in range(n_chunks):
        own[k].start()
    own_t.start()

    barrier = pltpu.get_barrier_semaphore()
    for other in others:
        pl.semaphore_signal(barrier, inc=1, device_id={"tp": other}, device_id_type=MESH)
    pl.semaphore_wait(barrier, 3)

    def remote(src, dst, send, recv, dev):
        return pltpu.make_async_remote_copy(
            src_ref=src, dst_ref=dst, send_sem=send, recv_sem=recv, device_id={"tp": dev}, device_id_type=MESH
        )

    def cross_copy(k):
        return remote(piece(me, k), piece(me, k), xsend.at[k], xrecv.at[k], cross)

    def peer_copy(k):
        return remote(piece(me, k), piece(me, k), psend.at[k], precv.at[k], peer)

    def diag_copy(k):
        return remote(piece(me, k), piece(me, k), fsend.at[k], frecv.at[k], diag)

    def forward_copy():
        return remote(piece(cross, 0), piece(cross, 0), fsend.at[0], frecv.at[0], peer)

    def gain_copy(n):
        return remote(grx.at[me], grx.at[me], gsend.at[n], grecv.at[n], others[n])

    def stat_copy(n, k):
        return remote(stx.at[k], srx.at[n, k], ssend.at[n, k], srecv.at[n, k], others[n])

    ns = jax.named_scope
    with ns("own"):
        own_g.wait()
        for n in range(3):
            gain_copy(n).start()
        for k in range(n_chunks):
            own[k].wait()
            cross_copy(k).start()
            peer_copy(k).start()
            if k:
                diag_copy(k).start()
        for part in load_w:
            part.start()
        own_t.wait()

    for n in range(3):
        gain_copy(n).wait_recv()
    for s in range(4):
        for lo in range(0, d_local, LANES):
            size = min(LANES, d_local - lo)
            row = grx[s, :, lo : lo + size]
            row = jnp.concatenate([row] * (LANES // size), axis=-1)
            gcol[s * d_local + lo : s * d_local + lo + size, :] = jnp.broadcast_to(row, (LANES, LANES)).T[0:size]

    group = 32

    def normalise(k):
        def square(i, acc):
            at = pl.ds(pl.multiple_of(i * group, group), group)
            part = hrx[k, at, :].astype(jnp.float32)
            return acc + part * part

        sq = lax.fori_loop(0, d_full // group, square, jnp.zeros((group, chunk), jnp.float32), unroll=True)
        inv = lax.rsqrt(jnp.sum(sq, axis=0, keepdims=True) / d_full + NORM_EPS)

        def scale(i, carry):
            at = pl.ds(pl.multiple_of(i * group, group), group)
            gain = gcol[at, :]
            part = hrx[k, at, :].astype(jnp.float32)
            gains = jnp.concatenate([gain] * (chunk // LANES), axis=-1)
            xbuf[at, :] = (part * inv * gains).astype(jnp.bfloat16)
            return carry

        lax.fori_loop(0, d_full // group, scale, 0, unroll=True)

    sub = lax.broadcasted_iota(jnp.int32, (8, chunk), 0)

    def logits(j):
        lo = starts[j]
        size = min(block, v_local - lo)
        zbuf[j % 2, 0:size, :] = jnp.dot(wbuf[lo : lo + size, :], xbuf[...], preferred_element_type=jnp.float32)

    def epilogue(j, want, state):
        lo = starts[j]
        size = min(block, v_local - lo)

        def tile(i):
            return zbuf[j % 2, pl.ds(pl.multiple_of(i * 8, 8), 8), :]

        top = lax.fori_loop(1, size // 8, lambda i, t: jnp.maximum(t, tile(i)), tile(0), unroll=True)
        if state is None:
            total = jnp.zeros((8, chunk), jnp.float32)
            pick = total
        else:
            old, total, pick = state
            top = jnp.maximum(top, old)
            total = total * jnp.exp2((old - top) * LOG2E)

        def add(i, carry):
            total, pick = carry
            z = tile(i)
            total = total + jnp.exp2((z - top) * LOG2E)
            pick = jnp.where(want == lo + i * 8, z, pick)
            return total, pick

        total, pick = lax.fori_loop(0, size // 8, add, (total, pick), unroll=True)
        return top, total, pick

    def finish_chunk(k, state):
        m, total, pick = state
        top = jnp.max(m, axis=0, keepdims=True)
        stx[k, 0:1, :] = top
        stx[k, 1:2, :] = jnp.sum(total * jnp.exp2((m - top) * LOG2E), axis=0, keepdims=True)
        stx[k, 2:3, :] = jnp.sum(pick, axis=0, keepdims=True)

    with ns("cross0"):
        cross_copy(0).wait_recv()
    forward_copy().start()
    with ns("fwd0"):
        peer_copy(0).wait_recv()
        forward_copy().wait_recv()
    with ns("wwait"):
        for part in load_w:
            part.wait()

    def targets_of(k):
        row = tbuf[pl.ds(k // per_chunk, 1), pl.ds(pl.multiple_of(lax.rem(k, per_chunk) * chunk, chunk), chunk)]
        local = row - me * v_local
        local = jnp.where((local >= 0) & (local < v_local), local, jnp.int32(-(1 << 20)))
        return jnp.broadcast_to(local, (8, chunk)) - sub

    final = n_blocks - 1

    def send_stats(k):
        for n in range(3):
            stat_copy(n, k).start()

    def step(k, carry):
        @pl.when(k > 0)
        def _():
            with ns("chunkwait"):
                cross_copy(k).wait_recv()
                peer_copy(k).wait_recv()
                diag_copy(k).wait_recv()

        @pl.when(k > 1)
        def _():
            send_stats(k - 2)

        normalise(k)
        last_want, *last_state = carry
        want = targets_of(k)
        state = None
        for j in range(n_blocks):
            logits(j)
            if j:
                state = epilogue(j - 1, want, state)
            else:
                finish_chunk(lax.rem(k + n_chunks, n_chunks + 1), epilogue(final, last_want, last_state))
        return (want, *state)

    blank = jnp.zeros((8, chunk), jnp.float32)
    zbuf[final % 2, 0 : v_local - starts[final], :] = jnp.zeros((v_local - starts[final], chunk), jnp.float32)
    want, *state = lax.fori_loop(0, n_chunks, step, (jnp.full((8, chunk), -1, jnp.int32), blank, blank, blank))
    send_stats(n_chunks - 2)
    with ns("last"):
        finish_chunk(n_chunks - 1, epilogue(final, want, state))
    send_stats(n_chunks - 1)

    for k in range(n_chunks):
        with ns("statwait"):
            for n in range(3):
                stat_copy(n, k).wait_recv()
        stats = [stx[k]] + [srx[n, k] for n in range(3)]
        top = stats[0][0:1]
        for st in stats[1:]:
            top = jnp.maximum(top, st[0:1])
        total = jnp.zeros_like(top)
        pick = jnp.zeros_like(top)
        for st in stats:
            total = total + st[1:2] * jnp.exp2((st[0:1] - top) * LOG2E)
            pick = pick + st[2:3]
        seq, pos = divmod(k * chunk, per_seq)
        out_ref[seq : seq + 1, pos : pos + chunk] = pick - (top + jnp.log(total))

    for k in range(n_chunks):
        cross_copy(k).wait_send()
        peer_copy(k).wait_send()
        if k:
            diag_copy(k).wait_send()
        else:
            forward_copy().wait_send()
        for n in range(3):
            stat_copy(n, k).wait_send()
    for n in range(3):
        gain_copy(n).wait_send()


def solution(mesh):
    def local_score(hidden, ln_scale, w_head, targets, valid_mask):
        b, l, d_local = hidden.shape
        v_local = w_head.shape[1]
        rows, chunk, block = b * l, 256, 512
        part = 2048
        w_parts = tuple((lo, min(part, v_local - lo)) for lo in range(0, v_local, part))
        n_chunks = rows // chunk
        any_spec = pl.BlockSpec(memory_space=pl.ANY)
        f32 = jnp.float32
        dma = pltpu.SemaphoreType.DMA
        token = pl.pallas_call(
            functools.partial(head_kernel, (d_local, v_local, rows, chunk, block, w_parts)),
            out_shape=jax.ShapeDtypeStruct((b, l), f32),
            in_specs=[any_spec] * 4,
            out_specs=pl.BlockSpec(memory_space=pltpu.VMEM),
            scratch_shapes=[
                pltpu.VMEM((v_local, 4 * d_local), jnp.bfloat16),
                pltpu.VMEM((n_chunks, 4 * d_local, chunk), jnp.bfloat16),
                pltpu.VMEM((4, 1, d_local), f32),
                pltpu.VMEM((b, l), jnp.int32),
                pltpu.VMEM((4 * d_local, LANES), f32),
                pltpu.VMEM((4 * d_local, chunk), jnp.bfloat16),
                pltpu.VMEM((2, block, chunk), f32),
                pltpu.VMEM((n_chunks + 1, 8, chunk), f32),
                pltpu.VMEM((3, n_chunks, 8, chunk), f32),
                dma((len(w_parts),)),
                dma((n_chunks,)),
                dma((2,)),
                dma((n_chunks,)), dma((n_chunks,)),
                dma((n_chunks,)), dma((n_chunks,)),
                dma((n_chunks,)), dma((n_chunks,)),
                dma((3,)), dma((3,)),
                dma((3, n_chunks)), dma((3, n_chunks)),
            ],
            compiler_params=pltpu.CompilerParams(
                collective_id=0, has_side_effects=True, vmem_limit_bytes=40 * 1024 * 1024
            ),
        )(*[
            pltpu.with_memory_space_constraint(x, pltpu.HBM)
            for x in (hidden.transpose(0, 2, 1), ln_scale.reshape(1, d_local), w_head.T, targets)
        ])
        token_logp = valid_mask.astype(f32) * token
        return token_logp, jnp.sum(token_logp, axis=1)

    return jax.shard_map(
        local_score,
        mesh=mesh,
        in_specs=(P("dp", None, "tp"), P("tp"), P(None, "tp"), P("dp", None), P("dp", None)),
        out_specs=(P("dp", None), P("dp")),
        check_vma=False,
    )
```

```python
import functools

import jax
import jax.numpy as jnp
from jax import lax
from jax.experimental import pallas as pl
from jax.experimental.pallas import tpu as pltpu
from jax.sharding import PartitionSpec as P

NORM_EPS = 1e-6
LOG2E = 1.4426950408889634
MESH = pl.DeviceIdType.MESH
LANES = 128


def head_kernel(
    cfg, h_ref, g_ref, w_ref, tgt_ref, out_ref,
    wbuf, hrx, grx, tbuf, gcol, xbuf, zbuf, stx, srx,
    w_sem, own_sem, small_sem, psend, precv, xsend, xrecv, fsend, frecv, gsend, grecv, ssend, srecv,
):
    d_local, v_local, rows, chunk, block, w_parts = cfg
    n_chunks = rows // chunk
    d_full = 4 * d_local
    per_seq = h_ref.shape[2]
    per_chunk = per_seq // chunk
    starts = list(range(0, v_local, block))
    n_blocks = len(starts)

    me = lax.axis_index("tp")
    peer = me + 1 - 2 * lax.rem(me, 2)
    cross = lax.rem(me + 2, 4)
    diag = lax.rem(peer + 2, 4)
    others = (peer, cross, diag)

    def piece(owner, k):
        return hrx.at[k, pl.ds(pl.multiple_of(owner * d_local, d_local), d_local)]

    own = [
        pltpu.make_async_copy(
            h_ref.at[k // per_chunk, :, pl.ds((k % per_chunk) * chunk, chunk)], piece(me, k), own_sem.at[k]
        )
        for k in range(n_chunks)
    ]
    own_g = pltpu.make_async_copy(g_ref, grx.at[me], small_sem.at[0])
    own_t = pltpu.make_async_copy(tgt_ref, tbuf, small_sem.at[1])
    load_w = [
        pltpu.make_async_copy(w_ref.at[pl.ds(lo, size)], wbuf.at[pl.ds(lo, size)], w_sem.at[n])
        for n, (lo, size) in enumerate(w_parts)
    ]
    own_g.start()
    for k in range(n_chunks):
        own[k].start()
    own_t.start()

    ns = jax.named_scope
    barrier = pltpu.get_barrier_semaphore()
    for other in others:
        pl.semaphore_signal(barrier, inc=1, device_id={"tp": other}, device_id_type=MESH)
    with ns("own"):
        own_g.wait()
        for k in range(n_chunks):
            own[k].wait()
        own_t.wait()
        for part in load_w:
            part.start()
    with ns("barrier"):
        pl.semaphore_wait(barrier, 3)

    def remote(src, dst, send, recv, dev):
        return pltpu.make_async_remote_copy(
            src_ref=src, dst_ref=dst, send_sem=send, recv_sem=recv, device_id={"tp": dev}, device_id_type=MESH
        )

    def part_of(owner, k, h):
        if h is None:
            return piece(owner, k)
        return hrx.at[k, pl.ds(pl.multiple_of(owner * d_local, d_local), d_local), pl.ds(h * LANES, LANES)]

    def cross_copy(k, h):
        slot = 0 if h is None else h
        return remote(part_of(me, k, h), part_of(me, k, h), xsend.at[slot, k], xrecv.at[slot, k], cross)

    def peer_copy(k):
        return remote(piece(me, k), piece(me, k), psend.at[k], precv.at[k], peer)

    def diag_copy(k):
        return remote(part_of(me, k, 1), part_of(me, k, 1), fsend.at[1, k], frecv.at[1, k], diag)

    def forward_copy(k, h):
        return remote(part_of(cross, k, h), part_of(cross, k, h), fsend.at[0, k], frecv.at[0, k], peer)

    def gain_copy(n):
        return remote(grx.at[me], grx.at[me], gsend.at[n], grecv.at[n], others[n])

    def stat_copy(n, k):
        return remote(stx.at[k], srx.at[n, k], ssend.at[n, k], srecv.at[n, k], others[n])

    for n in range(3):
        gain_copy(n).start()
    cross_copy(0, None).start()
    for k in range(n_chunks):
        peer_copy(k).start()
    with ns("peer0"):
        peer_copy(0).wait_recv()
    for k in range(1, n_chunks):
        cross_copy(k, 0).start()
        cross_copy(k, 1).start()
        diag_copy(k).start()

    for n in range(3):
        gain_copy(n).wait_recv()
    for s in range(4):
        for lo in range(0, d_local, LANES):
            size = min(LANES, d_local - lo)
            row = grx[s, :, lo : lo + size]
            row = jnp.concatenate([row] * (LANES // size), axis=-1)
            gcol[s * d_local + lo : s * d_local + lo + size, :] = jnp.broadcast_to(row, (LANES, LANES)).T[0:size]

    group = 32

    def normalise(k):
        def square(i, acc):
            at = pl.ds(pl.multiple_of(i * group, group), group)
            part = hrx[k, at, :].astype(jnp.float32)
            return acc + part * part

        sq = lax.fori_loop(0, d_full // group, square, jnp.zeros((group, chunk), jnp.float32), unroll=True)
        inv = lax.rsqrt(jnp.sum(sq, axis=0, keepdims=True) / d_full + NORM_EPS)

        def scale(i, carry):
            at = pl.ds(pl.multiple_of(i * group, group), group)
            gain = gcol[at, :]
            part = hrx[k, at, :].astype(jnp.float32)
            gains = jnp.concatenate([gain] * (chunk // LANES), axis=-1)
            xbuf[at, :] = (part * inv * gains).astype(jnp.bfloat16)
            return carry

        lax.fori_loop(0, d_full // group, scale, 0, unroll=True)

    sub = lax.broadcasted_iota(jnp.int32, (8, chunk), 0)

    def slot_of(j):
        return j % 2 if j < n_blocks - 2 else 2 + j % 2

    def logits(j):
        lo = starts[j]
        size = min(block, v_local - lo)
        zbuf[slot_of(j), 0:size, :] = jnp.dot(wbuf[lo : lo + size, :], xbuf[...], preferred_element_type=jnp.float32)

    def epilogue(j, want, state):
        lo = starts[j]
        size = min(block, v_local - lo)

        def tile(i):
            return zbuf[slot_of(j), pl.ds(pl.multiple_of(i * 8, 8), 8), :]

        top = lax.fori_loop(1, size // 8, lambda i, t: jnp.maximum(t, tile(i)), tile(0), unroll=True)
        if state is None:
            total = jnp.zeros((8, chunk), jnp.float32)
            pick = total
        else:
            old, total, pick = state
            top = jnp.maximum(top, old)
            total = total * jnp.exp2((old - top) * LOG2E)

        def add(i, carry):
            total, pick = carry
            z = tile(i)
            total = total + jnp.exp2((z - top) * LOG2E)
            pick = jnp.where(want == lo + i * 8, z, pick)
            return total, pick

        total, pick = lax.fori_loop(0, size // 8, add, (total, pick), unroll=True)
        return top, total, pick

    def finish_chunk(k, state):
        m, total, pick = state
        top = jnp.max(m, axis=0, keepdims=True)
        stx[k, 0:1, :] = top
        stx[k, 1:2, :] = jnp.sum(total * jnp.exp2((m - top) * LOG2E), axis=0, keepdims=True)
        stx[k, 2:3, :] = jnp.sum(pick, axis=0, keepdims=True)

    with ns("cross0"):
        cross_copy(0, None).wait_recv()
    forward_copy(0, None).start()
    with ns("fwd0"):
        forward_copy(0, None).wait_recv()
    with ns("wwait"):
        for part in load_w:
            part.wait()

    def targets_of(k):
        row = tbuf[pl.ds(k // per_chunk, 1), pl.ds(pl.multiple_of(lax.rem(k, per_chunk) * chunk, chunk), chunk)]
        local = row - me * v_local
        local = jnp.where((local >= 0) & (local < v_local), local, jnp.int32(-(1 << 20)))
        return jnp.broadcast_to(local, (8, chunk)) - sub

    final = n_blocks - 1

    def send_stats(k):
        for n in range(3):
            stat_copy(n, k).start()

    def step(k, carry):
        @pl.when(k > 0)
        def _():
            with ns("chunkwait"):
                forward_copy(k, 0).wait_recv()
                cross_copy(k, 1).wait_recv()
                peer_copy(k).wait_recv()
                diag_copy(k).wait_recv()

        @pl.when(k < n_chunks - 1)
        def _():
            with ns("halfwait"):
                cross_copy(k + 1, 0).wait_recv()
            forward_copy(k + 1, 0).start()

        @pl.when(k > 1)
        def _():
            send_stats(k - 2)

        normalise(k)
        last_want, *last_state = carry
        want = targets_of(k)
        state = None
        for j in range(n_blocks):
            logits(j)
            if j == 0:
                last_state = epilogue(final - 1, last_want, last_state)
                finish_chunk(lax.rem(k + n_chunks, n_chunks + 1), epilogue(final, last_want, last_state))
            elif j < final:
                state = epilogue(j - 1, want, state)
        return (want, *state)

    blank = jnp.zeros((8, chunk), jnp.float32)
    for j in (final - 1, final):
        zbuf[slot_of(j), 0 : min(block, v_local - starts[j]), :] = jnp.zeros((min(block, v_local - starts[j]), chunk), jnp.float32)
    want, *state = lax.fori_loop(0, n_chunks, step, (jnp.full((8, chunk), -1, jnp.int32), blank, blank, blank))
    send_stats(n_chunks - 2)
    with ns("last"):
        finish_chunk(n_chunks - 1, epilogue(final, want, epilogue(final - 1, want, state)))
    send_stats(n_chunks - 1)

    for k in range(n_chunks):
        with ns("statwait"):
            for n in range(3):
                stat_copy(n, k).wait_recv()
        stats = [stx[k]] + [srx[n, k] for n in range(3)]
        top = stats[0][0:1]
        for st in stats[1:]:
            top = jnp.maximum(top, st[0:1])
        total = jnp.zeros_like(top)
        pick = jnp.zeros_like(top)
        for st in stats:
            total = total + st[1:2] * jnp.exp2((st[0:1] - top) * LOG2E)
            pick = pick + st[2:3]
        seq, pos = divmod(k * chunk, per_seq)
        out_ref[seq : seq + 1, pos : pos + chunk] = pick - (top + jnp.log(total))

    for k in range(n_chunks):
        peer_copy(k).wait_send()
        forward_copy(k, 0 if k else None).wait_send()
        cross_copy(k, 0 if k else None).wait_send()
        if k:
            cross_copy(k, 1).wait_send()
            diag_copy(k).wait_send()
        for n in range(3):
            stat_copy(n, k).wait_send()
    for n in range(3):
        gain_copy(n).wait_send()


def solution(mesh):
    def local_score(hidden, ln_scale, w_head, targets, valid_mask):
        b, l, d_local = hidden.shape
        v_local = w_head.shape[1]
        rows, chunk, block = b * l, 256, 512
        part = 2048
        w_parts = tuple((lo, min(part, v_local - lo)) for lo in range(0, v_local, part))
        n_chunks = rows // chunk
        any_spec = pl.BlockSpec(memory_space=pl.ANY)
        f32 = jnp.float32
        dma = pltpu.SemaphoreType.DMA
        token = pl.pallas_call(
            functools.partial(head_kernel, (d_local, v_local, rows, chunk, block, w_parts)),
            out_shape=jax.ShapeDtypeStruct((b, l), f32),
            in_specs=[any_spec] * 4,
            out_specs=pl.BlockSpec(memory_space=pltpu.VMEM),
            scratch_shapes=[
                pltpu.VMEM((v_local, 4 * d_local), jnp.bfloat16),
                pltpu.VMEM((n_chunks, 4 * d_local, chunk), jnp.bfloat16),
                pltpu.VMEM((4, 1, d_local), f32),
                pltpu.VMEM((b, l), jnp.int32),
                pltpu.VMEM((4 * d_local, LANES), f32),
                pltpu.VMEM((4 * d_local, chunk), jnp.bfloat16),
                pltpu.VMEM((4, block, chunk), f32),
                pltpu.VMEM((n_chunks + 1, 8, chunk), f32),
                pltpu.VMEM((3, n_chunks, 8, chunk), f32),
                dma((len(w_parts),)),
                dma((n_chunks,)),
                dma((2,)),
                dma((n_chunks,)), dma((n_chunks,)),
                dma((2, n_chunks)), dma((2, n_chunks)),
                dma((2, n_chunks)), dma((2, n_chunks)),
                dma((3,)), dma((3,)),
                dma((3, n_chunks)), dma((3, n_chunks)),
            ],
            compiler_params=pltpu.CompilerParams(
                collective_id=0, has_side_effects=True, vmem_limit_bytes=40 * 1024 * 1024
            ),
        )(*[
            pltpu.with_memory_space_constraint(x, pltpu.HBM)
            for x in (hidden.transpose(0, 2, 1), ln_scale.reshape(1, d_local), w_head.T, targets)
        ])
        token_logp = valid_mask.astype(f32) * token
        return token_logp, jnp.sum(token_logp, axis=1)

    return jax.shard_map(
        local_score,
        mesh=mesh,
        in_specs=(P("dp", None, "tp"), P("tp"), P(None, "tp"), P("dp", None), P("dp", None)),
        out_specs=(P("dp", None), P("dp")),
        check_vma=False,
    )
```

```python
import functools

import jax
import jax.numpy as jnp
from jax import lax
from jax.experimental import pallas as pl
from jax.experimental.pallas import tpu as pltpu
from jax.sharding import PartitionSpec as P

NORM_EPS = 1e-6
LOG2E = 1.4426950408889634
MESH = pl.DeviceIdType.MESH
LANES = 128


def head_kernel(
    cfg, h_ref, g_ref, w_ref, tgt_ref, out_ref,
    wbuf, hrx, grx, tbuf, gcol, xbuf, zbuf, stx, srx,
    w_sem, own_sem, small_sem, psend, precv, osend, orecv, fsend, frecv, xsend, xrecv, dsend, drecv, gsend, grecv, ssend, srecv,
):
    d_local, v_local, rows, chunk, blocks, carried, w_parts = cfg
    n_chunks = rows // chunk
    d_full = 4 * d_local
    per_seq = h_ref.shape[2]
    per_chunk = per_seq // chunk
    starts = [sum(blocks[:j]) for j in range(len(blocks))]
    n_blocks = len(blocks)
    held = n_blocks - carried

    me = lax.axis_index("tp")
    peer = me + 1 - 2 * lax.rem(me, 2)
    cross = lax.rem(me + 2, 4)
    diag = lax.rem(peer + 2, 4)
    others = (peer, cross, diag)

    def piece(owner, k):
        return hrx.at[k, pl.ds(pl.multiple_of(owner * d_local, d_local), d_local)]

    own = [
        pltpu.make_async_copy(
            h_ref.at[k // per_chunk, :, pl.ds((k % per_chunk) * chunk, chunk)], piece(me, k), own_sem.at[k]
        )
        for k in range(n_chunks)
    ]
    own_g = pltpu.make_async_copy(g_ref, grx.at[me], small_sem.at[0])
    own_t = pltpu.make_async_copy(tgt_ref, tbuf, small_sem.at[1])
    load_w = [
        pltpu.make_async_copy(w_ref.at[pl.ds(lo, size)], wbuf.at[pl.ds(lo, size)], w_sem.at[n])
        for n, (lo, size) in enumerate(w_parts)
    ]
    own_g.start()
    for k in range(n_chunks):
        own[k].start()
    own_t.start()

    ns = jax.named_scope
    barrier = pltpu.get_barrier_semaphore()
    for other in others:
        pl.semaphore_signal(barrier, inc=1, device_id={"tp": other}, device_id_type=MESH)
    with ns("own"):
        own_g.wait()
        for k in range(n_chunks):
            own[k].wait()
        own_t.wait()
        for part in load_w:
            part.start()
    with ns("barrier"):
        pl.semaphore_wait(barrier, 3)

    def remote(src, dst, send, recv, dev):
        return pltpu.make_async_remote_copy(
            src_ref=src, dst_ref=dst, send_sem=send, recv_sem=recv, device_id={"tp": dev}, device_id_type=MESH
        )

    once_rows = d_local * 3 // 4 // 16 * 16

    def rows_of(owner, lo, size):
        return pl.ds(pl.multiple_of(owner * d_local + lo, 16), size)

    def once(owner, k, first):
        if first:
            return hrx.at[k, rows_of(owner, 0, once_rows)]
        return hrx.at[k, rows_of(owner, 0, d_local), pl.ds(0, LANES)]

    def direct(owner, k, first):
        if first:
            return hrx.at[k, rows_of(owner, once_rows, d_local - once_rows)]
        return hrx.at[k, rows_of(owner, 0, d_local), pl.ds(LANES, chunk - LANES)]

    def once_copy(k, first):
        part = once(me, k, first)
        return remote(part, part, osend.at[k], orecv.at[k], diag)

    def forward_copy(k, first):
        part = once(diag, k, first)
        return remote(part, part, fsend.at[k], frecv.at[k], peer)

    def cross_copy(k, first):
        part = direct(me, k, first)
        return remote(part, part, xsend.at[k], xrecv.at[k], cross)

    def diag_copy(k, first):
        part = direct(me, k, first)
        return remote(part, part, dsend.at[k], drecv.at[k], diag)

    def peer_copy(k):
        return remote(piece(me, k), piece(me, k), psend.at[k], precv.at[k], peer)

    def gain_copy(n):
        return remote(grx.at[me], grx.at[me], gsend.at[n], grecv.at[n], others[n])

    def stat_copy(n, k):
        return remote(stx.at[k], srx.at[n, k], ssend.at[n, k], srecv.at[n, k], others[n])

    for n in range(3):
        gain_copy(n).start()
    once_copy(0, True).start()
    cross_copy(0, True).start()
    diag_copy(0, True).start()
    for k in range(n_chunks):
        peer_copy(k).start()

    with ns("gainwait"):
        for n in range(3):
            gain_copy(n).wait_recv()
    for k in range(1, n_chunks):
        once_copy(k, False).start()
        cross_copy(k, False).start()
        diag_copy(k, False).start()

    for s in range(4):
        for lo in range(0, d_local, LANES):
            size = min(LANES, d_local - lo)
            row = grx[s, :, lo : lo + size]
            row = jnp.concatenate([row] * (LANES // size), axis=-1)
            gcol[s * d_local + lo : s * d_local + lo + size, :] = jnp.broadcast_to(row, (LANES, LANES)).T[0:size]

    group = 32

    def normalise(k):
        def square(i, acc):
            at = pl.ds(pl.multiple_of(i * group, group), group)
            part = hrx[k, at, :].astype(jnp.float32)
            return acc + part * part

        sq = lax.fori_loop(0, d_full // group, square, jnp.zeros((group, chunk), jnp.float32), unroll=True)
        inv = lax.rsqrt(jnp.sum(sq, axis=0, keepdims=True) / d_full + NORM_EPS)

        def scale(i, carry):
            at = pl.ds(pl.multiple_of(i * group, group), group)
            gain = gcol[at, :]
            part = hrx[k, at, :].astype(jnp.float32)
            gains = jnp.concatenate([gain] * (chunk // LANES), axis=-1)
            xbuf[at, :] = (part * inv * gains).astype(jnp.bfloat16)
            return carry

        lax.fori_loop(0, d_full // group, scale, 0, unroll=True)

    sub = lax.broadcasted_iota(jnp.int32, (8, chunk), 0)

    def slot_of(j):
        return j % 2 if j < held else 2 + j - held

    def logits(j):
        lo = starts[j]
        size = blocks[j]
        zbuf[slot_of(j), 0:size, :] = jnp.dot(wbuf[lo : lo + size, :], xbuf[...], preferred_element_type=jnp.float32)

    def epilogue(j, want, state):
        lo = starts[j]
        size = blocks[j]

        def tile(i):
            return zbuf[slot_of(j), pl.ds(pl.multiple_of(i * 8, 8), 8), :]

        top = lax.fori_loop(1, size // 8, lambda i, t: jnp.maximum(t, tile(i)), tile(0), unroll=True)
        if state is None:
            total = jnp.zeros((8, chunk), jnp.float32)
            pick = total
        else:
            old, total, pick = state
            top = jnp.maximum(top, old)
            total = total * jnp.exp2((old - top) * LOG2E)

        def add(i, carry):
            total, pick = carry
            z = tile(i)
            total = total + jnp.exp2((z - top) * LOG2E)
            pick = jnp.where(want == lo + i * 8, z, pick)
            return total, pick

        total, pick = lax.fori_loop(0, size // 8, add, (total, pick), unroll=True)
        return top, total, pick

    def finish_chunk(k, state):
        m, total, pick = state
        top = jnp.max(m, axis=0, keepdims=True)
        total = jnp.sum(total * jnp.exp2((m - top) * LOG2E), axis=0, keepdims=True)
        pick = jnp.sum(pick, axis=0, keepdims=True)
        for n, stat in enumerate((top, total, pick)):
            for q in range(chunk // LANES):
                row = n * (chunk // LANES) + q
                stx[k, row : row + 1, :] = stat[:, q * LANES : (q + 1) * LANES]

    with ns("once0"):
        once_copy(0, True).wait_recv()
    forward_copy(0, True).start()
    with ns("peer0"):
        peer_copy(0).wait_recv()
        cross_copy(0, True).wait_recv()
        diag_copy(0, True).wait_recv()
    with ns("fwd0"):
        forward_copy(0, True).wait_recv()
    with ns("wwait"):
        for part in load_w:
            part.wait()

    def targets_of(k):
        row = tbuf[pl.ds(k // per_chunk, 1), pl.ds(pl.multiple_of(lax.rem(k, per_chunk) * chunk, chunk), chunk)]
        local = row - me * v_local
        local = jnp.where((local >= 0) & (local < v_local), local, jnp.int32(-(1 << 20)))
        return jnp.broadcast_to(local, (8, chunk)) - sub

    def send_stats(k):
        for n in range(3):
            stat_copy(n, k).start()

    def step(k, carry):
        @pl.when(k > 0)
        def _():
            with ns("chunkwait"):
                forward_copy(k, False).wait_recv()
                cross_copy(k, False).wait_recv()
                diag_copy(k, False).wait_recv()
                peer_copy(k).wait_recv()

        @pl.when(k < n_chunks - 1)
        def _():
            with ns("halfwait"):
                once_copy(k + 1, False).wait_recv()
            forward_copy(k + 1, False).start()

        @pl.when(k > 1)
        def _():
            send_stats(k - 2)

        normalise(k)
        last_want, *last_state = carry
        want = targets_of(k)
        state = None
        for j in range(n_blocks):
            logits(j)
            if j == 0:
                for i in range(held, n_blocks):
                    last_state = epilogue(i, last_want, last_state)
                finish_chunk(lax.rem(k + n_chunks, n_chunks + 1), last_state)
            elif j <= held:
                state = epilogue(j - 1, want, state)
        if held == n_blocks:
            state = epilogue(held - 1, want, state)
        return (want, *state)

    blank = jnp.zeros((8, chunk), jnp.float32)
    for j in range(held, n_blocks):
        zbuf[slot_of(j), 0 : blocks[j], :] = jnp.zeros((blocks[j], chunk), jnp.float32)
    want, *state = lax.fori_loop(0, n_chunks, step, (jnp.full((8, chunk), -1, jnp.int32), blank, blank, blank))
    send_stats(n_chunks - 2)
    with ns("last"):
        for j in range(held, n_blocks):
            state = epilogue(j, want, state)
        finish_chunk(n_chunks - 1, state)
    send_stats(n_chunks - 1)

    per = chunk // LANES
    for k in range(n_chunks):
        with ns("statwait"):
            for n in range(3):
                stat_copy(n, k).wait_recv()
        stats = [stx[k]] + [srx[n, k] for n in range(3)]
        top = stats[0][0:per]
        for st in stats[1:]:
            top = jnp.maximum(top, st[0:per])
        total = jnp.zeros_like(top)
        pick = jnp.zeros_like(top)
        for st in stats:
            total = total + st[per : 2 * per] * jnp.exp2((st[0:per] - top) * LOG2E)
            pick = pick + st[2 * per : 3 * per]
        logp = pick - (top + jnp.log(total))
        seq, pos = divmod(k * chunk, per_seq)
        for q in range(per):
            out_ref[seq : seq + 1, pos + q * LANES : pos + (q + 1) * LANES] = logp[q : q + 1]

    with ns("sendwait"):
        for k in range(n_chunks):
            peer_copy(k).wait_send()
            for copy in (once_copy, forward_copy, cross_copy, diag_copy):
                copy(k, k == 0).wait_send()
            for n in range(3):
                stat_copy(n, k).wait_send()
    for n in range(3):
        gain_copy(n).wait_send()


def solution(mesh):
    def local_score(hidden, ln_scale, w_head, targets, valid_mask):
        b, l, d_local = hidden.shape
        v_local = w_head.shape[1]
        rows, chunk, block, carried = b * l, 256, 224, 2
        blocks = (block,) * (v_local // block) + ((v_local % block,) if v_local % block else ())
        part = 2048
        w_parts = tuple((lo, min(part, v_local - lo)) for lo in range(0, v_local, part))
        n_chunks = rows // chunk
        any_spec = pl.BlockSpec(memory_space=pl.ANY)
        f32 = jnp.float32
        dma = pltpu.SemaphoreType.DMA
        token = pl.pallas_call(
            functools.partial(head_kernel, (d_local, v_local, rows, chunk, blocks, carried, w_parts)),
            out_shape=jax.ShapeDtypeStruct((b, l), f32),
            in_specs=[any_spec] * 4,
            out_specs=pl.BlockSpec(memory_space=pltpu.VMEM),
            scratch_shapes=[
                pltpu.VMEM((v_local, 4 * d_local), jnp.bfloat16),
                pltpu.VMEM((n_chunks, 4 * d_local, chunk), jnp.bfloat16),
                pltpu.VMEM((4, 1, d_local), f32),
                pltpu.VMEM((b, l), jnp.int32),
                pltpu.VMEM((4 * d_local, LANES), f32),
                pltpu.VMEM((4 * d_local, chunk), jnp.bfloat16),
                pltpu.VMEM((2 + carried, block, chunk), f32),
                pltpu.VMEM((n_chunks + 1, 8, LANES), f32),
                pltpu.VMEM((3, n_chunks, 8, LANES), f32),
                dma((len(w_parts),)),
                dma((n_chunks,)),
                dma((2,)),
                dma((n_chunks,)), dma((n_chunks,)),
                dma((n_chunks,)), dma((n_chunks,)),
                dma((n_chunks,)), dma((n_chunks,)),
                dma((n_chunks,)), dma((n_chunks,)),
                dma((n_chunks,)), dma((n_chunks,)),
                dma((3,)), dma((3,)),
                dma((3, n_chunks)), dma((3, n_chunks)),
            ],
            compiler_params=pltpu.CompilerParams(
                collective_id=0,
                has_side_effects=True,
                vmem_limit_bytes=40 * 1024 * 1024,
            ),
        )(*[
            pltpu.with_memory_space_constraint(x, pltpu.HBM)
            for x in (hidden.transpose(0, 2, 1), ln_scale.reshape(1, d_local), w_head.T, targets)
        ])
        token_logp = valid_mask.astype(f32) * token
        return token_logp, jnp.sum(token_logp, axis=1)

    return jax.shard_map(
        local_score,
        mesh=mesh,
        in_specs=(P("dp", None, "tp"), P("tp"), P(None, "tp"), P("dp", None), P("dp", None)),
        out_specs=(P("dp", None), P("dp")),
        check_vma=False,
    )
```

```python
import functools

import jax
import jax.numpy as jnp
from jax import lax
from jax.experimental import pallas as pl
from jax.experimental.pallas import tpu as pltpu
from jax.sharding import PartitionSpec as P

NORM_EPS = 1e-6
LOG2E = 1.4426950408889634
MESH = pl.DeviceIdType.MESH
LANES = 128


def head_kernel(
    cfg, h_ref, g_ref, w_ref, tgt_ref, out_ref,
    wbuf, hrx, grx, tbuf, gcol, xbuf, zbuf, stx, srx,
    w_sem, own_sem, small_sem, hsend, precv, orecv, arecv, gsend, grecv, ssend, srecv,
):
    d_local, v_local, rows, chunk, blocks, carried, w_parts = cfg
    n_chunks = rows // chunk
    d_full = 4 * d_local
    per_seq = h_ref.shape[2]
    per_chunk = per_seq // chunk
    starts = [sum(blocks[:j]) for j in range(len(blocks))]
    n_blocks = len(blocks)
    held = n_blocks - carried

    me = lax.axis_index("tp")
    peer = me + 1 - 2 * lax.rem(me, 2)
    cross = lax.rem(me + 2, 4)
    diag = lax.rem(peer + 2, 4)
    others = (peer, cross, diag)

    def piece(owner, k):
        return hrx.at[k, pl.ds(pl.multiple_of(owner * d_local, d_local), d_local)]

    own_rows = hrx.at[:, pl.ds(pl.multiple_of(me * d_local, d_local), d_local)]

    own = [
        pltpu.make_async_copy(
            h_ref.at[k // per_chunk, :, pl.ds((k % per_chunk) * chunk, chunk)], piece(me, k), own_sem
        )
        for k in range(n_chunks)
    ]
    own_g = pltpu.make_async_copy(g_ref, grx.at[me], small_sem.at[0])
    own_t = pltpu.make_async_copy(tgt_ref, tbuf, small_sem.at[1])
    load_w = [
        pltpu.make_async_copy(w_ref.at[pl.ds(lo, size)], wbuf.at[pl.ds(lo, size)], w_sem)
        for lo, size in w_parts
    ]
    own_g.start()
    for k in range(n_chunks):
        own[k].start()
    own_t.start()

    ns = jax.named_scope
    barrier = pltpu.get_barrier_semaphore()
    for other in others:
        pl.semaphore_signal(barrier, inc=1, device_id={"tp": other}, device_id_type=MESH)
    with ns("own"):
        own_g.wait()
        pltpu.make_async_copy(own_rows, own_rows, own_sem).wait()
        own_t.wait()
        for part in load_w:
            part.start()
    with ns("barrier"):
        pl.semaphore_wait(barrier, 3)

    def remote(src, dst, send, recv, dev):
        return pltpu.make_async_remote_copy(
            src_ref=src, dst_ref=dst, send_sem=send, recv_sem=recv, device_id={"tp": dev}, device_id_type=MESH
        )

    def once_rows(first):
        return (d_local * 3 // 4 if first else d_local // 3) // 16 * 16

    def once(owner, k, first):
        return hrx.at[k, pl.ds(pl.multiple_of(owner * d_local, 16), once_rows(first))]

    def direct(owner, k, first):
        n = once_rows(first)
        return hrx.at[k, pl.ds(pl.multiple_of(owner * d_local + n, 16), d_local - n)]

    def once_copy(k, first):
        return remote(once(me, k, first), once(me, k, first), hsend, orecv.at[k], diag)

    def forward_copy(k, first):
        return remote(once(diag, k, first), once(diag, k, first), hsend, arecv.at[k], peer)

    def cross_copy(k, first):
        return remote(direct(me, k, first), direct(me, k, first), hsend, arecv.at[k], cross)

    def diag_copy(k, first):
        return remote(direct(me, k, first), direct(me, k, first), hsend, arecv.at[k], diag)

    def arrivals(k, first):
        got = hrx.at[k, pl.ds(0, 2 * d_local - once_rows(first))]
        return remote(got, got, hsend, arecv.at[k], peer)

    peer_copy = remote(own_rows, own_rows, hsend, precv, peer)
    all_sent = remote(hrx.at[pl.ds(0, 3)], hrx.at[pl.ds(0, 3)], hsend, precv, peer)

    def gain_copy(n):
        return remote(grx.at[me], grx.at[me], gsend, grecv, others[n])

    all_gains = remote(grx.at[pl.ds(0, 3)], grx.at[pl.ds(0, 3)], gsend, grecv, peer)
    early = n_chunks - 1

    def stat_copy(n, k, sem):
        return remote(stx.at[k], srx.at[k, n], ssend, srecv.at[sem], others[n])

    early_stats = remote(srx.at[pl.ds(0, early)], srx.at[pl.ds(0, early)], ssend, srecv.at[0], peer)
    late_stats = remote(srx.at[early], srx.at[early], ssend, srecv.at[1], peer)
    all_stats = remote(srx, srx, ssend, srecv.at[1], peer)

    for n in range(3):
        gain_copy(n).start()
    once_copy(0, True).start()
    cross_copy(0, True).start()
    diag_copy(0, True).start()
    peer_copy.start()

    with ns("gainwait"):
        all_gains.wait_recv()
    for k in range(1, n_chunks):
        once_copy(k, False).start()
        cross_copy(k, False).start()
        diag_copy(k, False).start()

    for s in range(4):
        for lo in range(0, d_local, LANES):
            size = min(LANES, d_local - lo)
            row = grx[s, :, lo : lo + size]
            row = jnp.concatenate([row] * (LANES // size), axis=-1)
            gcol[s * d_local + lo : s * d_local + lo + size, :] = jnp.broadcast_to(row, (LANES, LANES)).T[0:size]

    group = 32

    def normalise(k):
        def square(i, acc):
            at = pl.ds(pl.multiple_of(i * group, group), group)
            part = hrx[k, at, :].astype(jnp.float32)
            return acc + part * part

        sq = lax.fori_loop(0, d_full // group, square, jnp.zeros((group, chunk), jnp.float32), unroll=True)
        inv = lax.rsqrt(jnp.sum(sq, axis=0, keepdims=True) / d_full + NORM_EPS)

        def scale(i, carry):
            at = pl.ds(pl.multiple_of(i * group, group), group)
            gain = gcol[at, :]
            part = hrx[k, at, :].astype(jnp.float32)
            gains = jnp.concatenate([gain] * (chunk // LANES), axis=-1)
            xbuf[at, :] = (part * inv * gains).astype(jnp.bfloat16)
            return carry

        lax.fori_loop(0, d_full // group, scale, 0, unroll=True)

    sub = lax.broadcasted_iota(jnp.int32, (8, chunk), 0)

    def slot_of(j):
        return j % 2 if j < held else 2 + j - held

    def logits(j):
        lo = starts[j]
        size = blocks[j]
        zbuf[slot_of(j), 0:size, :] = jnp.dot(wbuf[lo : lo + size, :], xbuf[...], preferred_element_type=jnp.float32)

    def epilogue(j, want, state):
        lo = starts[j]
        size = blocks[j]

        def tile(i):
            return zbuf[slot_of(j), pl.ds(pl.multiple_of(i * 8, 8), 8), :]

        top = lax.fori_loop(1, size // 8, lambda i, t: jnp.maximum(t, tile(i)), tile(0), unroll=True)
        if state is None:
            total = jnp.zeros((8, chunk), jnp.float32)
            pick = total
        else:
            old, total, pick = state
            top = jnp.maximum(top, old)
            total = total * jnp.exp2((old - top) * LOG2E)

        def add(i, carry):
            total, pick = carry
            z = tile(i)
            total = total + jnp.exp2((z - top) * LOG2E)
            pick = jnp.where(want == lo + i * 8, z, pick)
            return total, pick

        total, pick = lax.fori_loop(0, size // 8, add, (total, pick), unroll=True)
        return top, total, pick

    def finish_chunk(k, state):
        m, total, pick = state
        top = jnp.max(m, axis=0, keepdims=True)
        total = jnp.sum(total * jnp.exp2((m - top) * LOG2E), axis=0, keepdims=True)
        pick = jnp.sum(pick, axis=0, keepdims=True)
        for n, stat in enumerate((top, total, pick)):
            for q in range(chunk // LANES):
                row = n * (chunk // LANES) + q
                stx[k, row : row + 1, :] = stat[:, q * LANES : (q + 1) * LANES]

    with ns("once0"):
        once_copy(0, True).wait_recv()
    forward_copy(0, True).start()
    with ns("peer0"):
        peer_copy.wait_recv()
    with ns("fwd0"):
        arrivals(0, True).wait_recv()
    with ns("wwait"):
        pltpu.make_async_copy(w_ref, wbuf, w_sem).wait()

    def targets_of(k):
        row = tbuf[pl.ds(k // per_chunk, 1), pl.ds(pl.multiple_of(lax.rem(k, per_chunk) * chunk, chunk), chunk)]
        local = row - me * v_local
        local = jnp.where((local >= 0) & (local < v_local), local, jnp.int32(-(1 << 20)))
        return jnp.broadcast_to(local, (8, chunk)) - sub

    def send_stats(k, sem):
        for n in range(3):
            stat_copy(n, k, sem).start()

    def step(k, carry):
        @pl.when(k > 0)
        def _():
            with ns("chunkwait"):
                arrivals(k, False).wait_recv()

        @pl.when(k < n_chunks - 1)
        def _():
            with ns("halfwait"):
                once_copy(k + 1, False).wait_recv()
            forward_copy(k + 1, False).start()

        @pl.when(k > 1)
        def _():
            send_stats(k - 2, 0)

        normalise(k)
        last_want, *last_state = carry
        want = targets_of(k)
        state = None
        for j in range(n_blocks):
            logits(j)
            if j == 0:
                for i in range(held, n_blocks):
                    last_state = epilogue(i, last_want, last_state)
                finish_chunk(lax.rem(k + n_chunks, n_chunks + 1), last_state)
            elif j <= held:
                state = epilogue(j - 1, want, state)
        if held == n_blocks:
            state = epilogue(held - 1, want, state)
        return (want, *state)

    blank = jnp.zeros((8, chunk), jnp.float32)
    for j in range(held, n_blocks):
        zbuf[slot_of(j), 0 : blocks[j], :] = jnp.zeros((blocks[j], chunk), jnp.float32)
    want, *state = lax.fori_loop(0, n_chunks, step, (jnp.full((8, chunk), -1, jnp.int32), blank, blank, blank))
    send_stats(n_chunks - 2, 0)
    with ns("last"):
        for j in range(held, n_blocks):
            state = epilogue(j, want, state)
        finish_chunk(n_chunks - 1, state)
    send_stats(n_chunks - 1, 1)

    per = chunk // LANES
    for k in range(n_chunks):
        with ns("statwait"):
            if k == 0:
                early_stats.wait_recv()
            if k == early:
                late_stats.wait_recv()
        stats = [stx[k]] + [srx[k, n] for n in range(3)]
        top = stats[0][0:per]
        for st in stats[1:]:
            top = jnp.maximum(top, st[0:per])
        total = jnp.zeros_like(top)
        pick = jnp.zeros_like(top)
        for st in stats:
            total = total + st[per : 2 * per] * jnp.exp2((st[0:per] - top) * LOG2E)
            pick = pick + st[2 * per : 3 * per]
        logp = pick - (top + jnp.log(total))
        seq, pos = divmod(k * chunk, per_seq)
        for q in range(per):
            out_ref[seq : seq + 1, pos + q * LANES : pos + (q + 1) * LANES] = logp[q : q + 1]

    with ns("sendwait"):
        all_sent.wait_send()
        all_gains.wait_send()
        all_stats.wait_send()


def solution(mesh):
    def local_score(hidden, ln_scale, w_head, targets, valid_mask):
        b, l, d_local = hidden.shape
        v_local = w_head.shape[1]
        rows, chunk, block, carried = b * l, 256, 224, 2
        blocks = (block,) * (v_local // block) + ((v_local % block,) if v_local % block else ())
        part = 2048
        w_parts = tuple((lo, min(part, v_local - lo)) for lo in range(0, v_local, part))
        n_chunks = rows // chunk
        any_spec = pl.BlockSpec(memory_space=pl.ANY)
        f32 = jnp.float32
        dma = pltpu.SemaphoreType.DMA
        token = pl.pallas_call(
            functools.partial(head_kernel, (d_local, v_local, rows, chunk, blocks, carried, w_parts)),
            out_shape=jax.ShapeDtypeStruct((b, l), f32),
            in_specs=[any_spec] * 4,
            out_specs=pl.BlockSpec(memory_space=pltpu.VMEM),
            scratch_shapes=[
                pltpu.VMEM((v_local, 4 * d_local), jnp.bfloat16),
                pltpu.VMEM((n_chunks, 4 * d_local, chunk), jnp.bfloat16),
                pltpu.VMEM((4, 1, d_local), f32),
                pltpu.VMEM((b, l), jnp.int32),
                pltpu.VMEM((4 * d_local, LANES), f32),
                pltpu.VMEM((4 * d_local, chunk), jnp.bfloat16),
                pltpu.VMEM((2 + carried, block, chunk), f32),
                pltpu.VMEM((n_chunks + 1, 8, LANES), f32),
                pltpu.VMEM((n_chunks, 3, 8, LANES), f32),
                dma, dma, dma((2,)),
                dma, dma, dma((n_chunks,)), dma((n_chunks,)),
                dma, dma, dma, dma((2,)),
            ],
            compiler_params=pltpu.CompilerParams(
                collective_id=0,
                has_side_effects=True,
                vmem_limit_bytes=40 * 1024 * 1024,
            ),
        )(*[
            pltpu.with_memory_space_constraint(x, pltpu.HBM)
            for x in (hidden.transpose(0, 2, 1), ln_scale.reshape(1, d_local), w_head.T, targets)
        ])
        token_logp = valid_mask.astype(f32) * token
        return token_logp, jnp.sum(token_logp, axis=1)

    return jax.shard_map(
        local_score,
        mesh=mesh,
        in_specs=(P("dp", None, "tp"), P("tp"), P(None, "tp"), P("dp", None), P("dp", None)),
        out_specs=(P("dp", None), P("dp")),
        check_vma=False,
    )
```

```python
import functools

import jax
import jax.numpy as jnp
from jax import lax
from jax.experimental import pallas as pl
from jax.experimental.pallas import tpu as pltpu
from jax.sharding import PartitionSpec as P

NORM_EPS = 1e-6
LOG2E = 1.4426950408889634
MESH = pl.DeviceIdType.MESH
LANES = 128


def head_kernel(
    cfg, h_ref, g_ref, w_ref, tgt_ref, out_ref,
    wbuf, hrx, grx, tbuf, gcol, xbuf, zbuf, stx, srx,
    w_sem, own_sem, small_sem, hsend, precv, orecv, arecv, gsend, grecv, ssend, srecv,
):
    d_local, v_local, rows, chunk, blocks, carried, w_parts = cfg
    n_chunks = rows // chunk
    d_full = 4 * d_local
    per_seq = h_ref.shape[2]
    per_chunk = per_seq // chunk
    starts = [sum(blocks[:j]) for j in range(len(blocks))]
    n_blocks = len(blocks)
    held = n_blocks - carried

    me = lax.axis_index("tp")
    peer = me + 1 - 2 * lax.rem(me, 2)
    cross = lax.rem(me + 2, 4)
    diag = lax.rem(peer + 2, 4)
    others = (peer, cross, diag)

    def piece(owner, k):
        return hrx.at[k, pl.ds(pl.multiple_of(owner * d_local, d_local), d_local)]

    own_rows = hrx.at[:, pl.ds(pl.multiple_of(me * d_local, d_local), d_local)]

    own = [
        pltpu.make_async_copy(
            h_ref.at[k // per_chunk, :, pl.ds((k % per_chunk) * chunk, chunk)], piece(me, k), own_sem
        )
        for k in range(n_chunks)
    ]
    own_g = pltpu.make_async_copy(g_ref, grx.at[me], small_sem.at[0])
    own_t = pltpu.make_async_copy(tgt_ref, tbuf, small_sem.at[1])
    load_w = [
        pltpu.make_async_copy(w_ref.at[pl.ds(lo, size)], wbuf.at[pl.ds(lo, size)], w_sem)
        for lo, size in w_parts
    ]
    own_g.start()
    for k in range(n_chunks):
        own[k].start()
    own_t.start()

    ns = jax.named_scope
    barrier = pltpu.get_barrier_semaphore()
    for other in others:
        pl.semaphore_signal(barrier, inc=1, device_id={"tp": other}, device_id_type=MESH)
    with ns("own"):
        own_g.wait()
        pltpu.make_async_copy(own_rows, own_rows, own_sem).wait()
        own_t.wait()
        for part in load_w:
            part.start()
    with ns("barrier"):
        pl.semaphore_wait(barrier, 3)

    def remote(src, dst, send, recv, dev):
        return pltpu.make_async_remote_copy(
            src_ref=src, dst_ref=dst, send_sem=send, recv_sem=recv, device_id={"tp": dev}, device_id_type=MESH
        )

    def once_rows(first):
        return (d_local * 2 // 3 if first else d_local // 4) // 16 * 16

    def once(owner, k, first):
        return hrx.at[k, pl.ds(pl.multiple_of(owner * d_local, 16), once_rows(first))]

    def direct(owner, k, first):
        n = once_rows(first)
        return hrx.at[k, pl.ds(pl.multiple_of(owner * d_local + n, 16), d_local - n)]

    def once_copy(k, first):
        return remote(once(me, k, first), once(me, k, first), hsend, orecv.at[k], diag)

    def forward_copy(k, first):
        return remote(once(diag, k, first), once(diag, k, first), hsend, arecv.at[k], peer)

    def cross_copy(k, first):
        return remote(direct(me, k, first), direct(me, k, first), hsend, arecv.at[k], cross)

    def diag_copy(k, first):
        return remote(direct(me, k, first), direct(me, k, first), hsend, arecv.at[k], diag)

    def arrivals(k, first):
        got = hrx.at[k, pl.ds(0, 2 * d_local - once_rows(first))]
        return remote(got, got, hsend, arecv.at[k], peer)

    peer_copy = remote(own_rows, own_rows, hsend, precv, peer)
    all_sent = remote(hrx.at[pl.ds(0, 3)], hrx.at[pl.ds(0, 3)], hsend, precv, peer)

    def gain_copy(n):
        return remote(grx.at[me], grx.at[me], gsend, grecv, others[n])

    all_gains = remote(grx.at[pl.ds(0, 3)], grx.at[pl.ds(0, 3)], gsend, grecv, peer)
    early = n_chunks - 1

    def stat_copy(n, k, sem):
        return remote(stx.at[k], srx.at[k, n], ssend, srecv.at[sem], others[n])

    early_stats = remote(srx.at[pl.ds(0, early)], srx.at[pl.ds(0, early)], ssend, srecv.at[0], peer)
    late_stats = remote(srx.at[early], srx.at[early], ssend, srecv.at[1], peer)
    all_stats = remote(srx, srx, ssend, srecv.at[1], peer)

    for n in range(3):
        gain_copy(n).start()
    once_copy(0, True).start()
    cross_copy(0, True).start()
    diag_copy(0, True).start()
    peer_copy.start()

    with ns("gainwait"):
        all_gains.wait_recv()
    for k in range(1, n_chunks):
        once_copy(k, False).start()
        cross_copy(k, False).start()
        diag_copy(k, False).start()

    for s in range(4):
        for lo in range(0, d_local, LANES):
            size = min(LANES, d_local - lo)
            row = grx[s, :, lo : lo + size]
            row = jnp.concatenate([row] * (LANES // size), axis=-1)
            gcol[s * d_local + lo : s * d_local + lo + size, :] = jnp.broadcast_to(row, (LANES, LANES)).T[0:size]

    group = 32

    def normalise(k):
        def square(i, acc):
            at = pl.ds(pl.multiple_of(i * group, group), group)
            part = hrx[k, at, :].astype(jnp.float32)
            return acc + part * part

        sq = lax.fori_loop(0, d_full // group, square, jnp.zeros((group, chunk), jnp.float32), unroll=True)
        inv = lax.rsqrt(jnp.sum(sq, axis=0, keepdims=True) / d_full + NORM_EPS)

        def scale(i, carry):
            at = pl.ds(pl.multiple_of(i * group, group), group)
            gain = gcol[at, :]
            part = hrx[k, at, :].astype(jnp.float32)
            gains = jnp.concatenate([gain] * (chunk // LANES), axis=-1)
            xbuf[at, :] = (part * inv * gains).astype(jnp.bfloat16)
            return carry

        lax.fori_loop(0, d_full // group, scale, 0, unroll=True)

    sub = lax.broadcasted_iota(jnp.int32, (8, chunk), 0)

    def slot_of(j):
        return j % 2 if j < held else 2 + j - held

    def logits(j):
        lo = starts[j]
        size = blocks[j]
        zbuf[slot_of(j), 0:size, :] = jnp.dot(wbuf[lo : lo + size, :], xbuf[...], preferred_element_type=jnp.float32)

    def epilogue(j, want, state):
        lo = starts[j]
        size = blocks[j]

        def tile(i):
            return zbuf[slot_of(j), pl.ds(pl.multiple_of(i * 8, 8), 8), :]

        top = lax.fori_loop(1, size // 8, lambda i, t: jnp.maximum(t, tile(i)), tile(0), unroll=True)
        if state is None:
            total = jnp.zeros((8, chunk), jnp.float32)
            pick = total
        else:
            old, total, pick = state
            top = jnp.maximum(top, old)
            total = total * jnp.exp2((old - top) * LOG2E)

        def add(i, carry):
            total, pick = carry
            z = tile(i)
            total = total + jnp.exp2((z - top) * LOG2E)
            pick = jnp.where(want == lo + i * 8, z, pick)
            return total, pick

        total, pick = lax.fori_loop(0, size // 8, add, (total, pick), unroll=True)
        return top, total, pick

    def finish_chunk(k, state):
        m, total, pick = state
        top = jnp.max(m, axis=0, keepdims=True)
        total = jnp.sum(total * jnp.exp2((m - top) * LOG2E), axis=0, keepdims=True)
        pick = jnp.sum(pick, axis=0, keepdims=True)
        for n, stat in enumerate((top, total, pick)):
            for q in range(chunk // LANES):
                row = n * (chunk // LANES) + q
                stx[k, row : row + 1, :] = stat[:, q * LANES : (q + 1) * LANES]

    with ns("once0"):
        once_copy(0, True).wait_recv()
    forward_copy(0, True).start()
    with ns("peer0"):
        peer_copy.wait_recv()
    with ns("fwd0"):
        arrivals(0, True).wait_recv()
    with ns("wwait"):
        pltpu.make_async_copy(w_ref, wbuf, w_sem).wait()

    def targets_of(k):
        row = tbuf[pl.ds(k // per_chunk, 1), pl.ds(pl.multiple_of(lax.rem(k, per_chunk) * chunk, chunk), chunk)]
        local = row - me * v_local
        local = jnp.where((local >= 0) & (local < v_local), local, jnp.int32(-(1 << 20)))
        return jnp.broadcast_to(local, (8, chunk)) - sub

    def send_stats(k, sem):
        for n in range(3):
            stat_copy(n, k, sem).start()

    def step(k, carry):
        @pl.when(k > 0)
        def _():
            with ns("chunkwait"):
                arrivals(k, False).wait_recv()

        @pl.when(k < n_chunks - 1)
        def _():
            with ns("halfwait"):
                once_copy(k + 1, False).wait_recv()
            forward_copy(k + 1, False).start()

        @pl.when(k > 1)
        def _():
            send_stats(k - 2, 0)

        normalise(k)
        last_want, *last_state = carry
        want = targets_of(k)
        state = None
        for j in range(n_blocks):
            logits(j)
            if j == 0:
                for i in range(held, n_blocks):
                    last_state = epilogue(i, last_want, last_state)
                finish_chunk(lax.rem(k + n_chunks, n_chunks + 1), last_state)
            elif j <= held:
                state = epilogue(j - 1, want, state)
        if held == n_blocks:
            state = epilogue(held - 1, want, state)
        return (want, *state)

    blank = jnp.zeros((8, chunk), jnp.float32)
    for j in range(held, n_blocks):
        zbuf[slot_of(j), 0 : blocks[j], :] = jnp.zeros((blocks[j], chunk), jnp.float32)
    want, *state = lax.fori_loop(0, n_chunks, step, (jnp.full((8, chunk), -1, jnp.int32), blank, blank, blank))
    send_stats(n_chunks - 2, 0)
    with ns("last"):
        for j in range(held, n_blocks):
            state = epilogue(j, want, state)
        finish_chunk(n_chunks - 1, state)
    send_stats(n_chunks - 1, 1)

    per = chunk // LANES
    for k in range(n_chunks):
        with ns("statwait"):
            if k == 0:
                early_stats.wait_recv()
            if k == early:
                late_stats.wait_recv()
        stats = [stx[k]] + [srx[k, n] for n in range(3)]
        top = stats[0][0:per]
        for st in stats[1:]:
            top = jnp.maximum(top, st[0:per])
        total = jnp.zeros_like(top)
        pick = jnp.zeros_like(top)
        for st in stats:
            total = total + st[per : 2 * per] * jnp.exp2((st[0:per] - top) * LOG2E)
            pick = pick + st[2 * per : 3 * per]
        logp = pick - (top + jnp.log(total))
        seq, pos = divmod(k * chunk, per_seq)
        for q in range(per):
            out_ref[seq : seq + 1, pos + q * LANES : pos + (q + 1) * LANES] = logp[q : q + 1]

    with ns("sendwait"):
        all_sent.wait_send()
        all_gains.wait_send()
        all_stats.wait_send()


def solution(mesh):
    def local_score(hidden, ln_scale, w_head, targets, valid_mask):
        b, l, d_local = hidden.shape
        v_local = w_head.shape[1]
        rows, chunk, block, carried = b * l, 256, 224, 2
        blocks = (block,) * (v_local // block) + ((v_local % block,) if v_local % block else ())
        part = 2048
        w_parts = tuple((lo, min(part, v_local - lo)) for lo in range(0, v_local, part))
        n_chunks = rows // chunk
        any_spec = pl.BlockSpec(memory_space=pl.ANY)
        f32 = jnp.float32
        dma = pltpu.SemaphoreType.DMA
        token = pl.pallas_call(
            functools.partial(head_kernel, (d_local, v_local, rows, chunk, blocks, carried, w_parts)),
            out_shape=jax.ShapeDtypeStruct((b, l), f32),
            in_specs=[any_spec] * 4,
            out_specs=pl.BlockSpec(memory_space=pltpu.VMEM),
            scratch_shapes=[
                pltpu.VMEM((v_local, 4 * d_local), jnp.bfloat16),
                pltpu.VMEM((n_chunks, 4 * d_local, chunk), jnp.bfloat16),
                pltpu.VMEM((4, 1, d_local), f32),
                pltpu.VMEM((b, l), jnp.int32),
                pltpu.VMEM((4 * d_local, LANES), f32),
                pltpu.VMEM((4 * d_local, chunk), jnp.bfloat16),
                pltpu.VMEM((2 + carried, block, chunk), f32),
                pltpu.VMEM((n_chunks + 1, 8, LANES), f32),
                pltpu.VMEM((n_chunks, 3, 8, LANES), f32),
                dma, dma, dma((2,)),
                dma, dma, dma((n_chunks,)), dma((n_chunks,)),
                dma, dma, dma, dma((2,)),
            ],
            compiler_params=pltpu.CompilerParams(
                collective_id=0,
                has_side_effects=True,
                vmem_limit_bytes=40 * 1024 * 1024,
            ),
        )(*[
            pltpu.with_memory_space_constraint(x, pltpu.HBM)
            for x in (hidden.transpose(0, 2, 1), ln_scale.reshape(1, d_local), w_head.T, targets)
        ])
        token_logp = valid_mask.astype(f32) * token
        return token_logp, jnp.sum(token_logp, axis=1)

    return jax.shard_map(
        local_score,
        mesh=mesh,
        in_specs=(P("dp", None, "tp"), P("tp"), P(None, "tp"), P("dp", None), P("dp", None)),
        out_specs=(P("dp", None), P("dp")),
        check_vma=False,
    )
```

```python
import functools

import jax
import jax.numpy as jnp
from jax import lax
from jax.experimental import pallas as pl
from jax.experimental.pallas import tpu as pltpu
from jax.sharding import PartitionSpec as P

NORM_EPS = 1e-6
LOG2E = 1.4426950408889634
MESH = pl.DeviceIdType.MESH
LANES = 128


def head_kernel(
    cfg, h_ref, g_ref, w_ref, tgt_ref, out_ref,
    wbuf, hrx, grx, tbuf, gcol, xbuf, zbuf, stx, srx,
    w_sem, own_sem, small_sem, hsend, precv, orecv, arecv, gsend, grecv, ssend, srecv,
):
    d_local, v_local, rows, chunk, blocks, carried, w_parts = cfg
    n_chunks = rows // chunk
    d_full = 4 * d_local
    per_seq = h_ref.shape[2]
    per_chunk = per_seq // chunk
    starts = [sum(blocks[:j]) for j in range(len(blocks))]
    n_blocks = len(blocks)
    held = n_blocks - carried

    me = lax.axis_index("tp")
    peer = me + 1 - 2 * lax.rem(me, 2)
    cross = lax.rem(me + 2, 4)
    diag = lax.rem(peer + 2, 4)
    others = (peer, cross, diag)

    def piece(owner, k):
        return hrx.at[k, pl.ds(pl.multiple_of(owner * d_local, d_local), d_local)]

    own_rows = hrx.at[:, pl.ds(pl.multiple_of(me * d_local, d_local), d_local)]

    own = [
        pltpu.make_async_copy(
            h_ref.at[k // per_chunk, :, pl.ds((k % per_chunk) * chunk, chunk)], piece(me, k), own_sem
        )
        for k in range(n_chunks)
    ]
    own_g = pltpu.make_async_copy(g_ref, grx.at[me], small_sem.at[0])
    own_t = pltpu.make_async_copy(tgt_ref, tbuf, small_sem.at[1])
    load_w = [
        pltpu.make_async_copy(w_ref.at[pl.ds(lo, size)], wbuf.at[pl.ds(lo, size)], w_sem)
        for lo, size in w_parts
    ]
    own_g.start()
    for k in range(n_chunks):
        own[k].start()
    own_t.start()

    ns = jax.named_scope
    barrier = pltpu.get_barrier_semaphore()
    for other in others:
        pl.semaphore_signal(barrier, inc=1, device_id={"tp": other}, device_id_type=MESH)
    with ns("own"):
        own_g.wait()
        pltpu.make_async_copy(own_rows, own_rows, own_sem).wait()
        own_t.wait()
        for part in load_w:
            part.start()
    with ns("barrier"):
        pl.semaphore_wait(barrier, 3)

    def remote(src, dst, send, recv, dev):
        return pltpu.make_async_remote_copy(
            src_ref=src, dst_ref=dst, send_sem=send, recv_sem=recv, device_id={"tp": dev}, device_id_type=MESH
        )

    def once_rows(first):
        return (d_local * 2 // 3 if first else d_local // 4) // 16 * 16

    def once(owner, k, first):
        return hrx.at[k, pl.ds(pl.multiple_of(owner * d_local, 16), once_rows(first))]

    def direct(owner, k, first):
        n = once_rows(first)
        return hrx.at[k, pl.ds(pl.multiple_of(owner * d_local + n, 16), d_local - n)]

    def once_copy(k, first):
        return remote(once(me, k, first), once(me, k, first), hsend, orecv.at[k], diag)

    def forward_copy(k, first):
        return remote(once(diag, k, first), once(diag, k, first), hsend, arecv.at[k], peer)

    def cross_copy(k, first):
        return remote(direct(me, k, first), direct(me, k, first), hsend, arecv.at[k], cross)

    def diag_copy(k, first):
        return remote(direct(me, k, first), direct(me, k, first), hsend, arecv.at[k], diag)

    def arrivals(k, first):
        got = hrx.at[k, pl.ds(0, 2 * d_local - once_rows(first))]
        return remote(got, got, hsend, arecv.at[k], peer)

    peer_copy = remote(own_rows, own_rows, hsend, precv, peer)
    all_sent = remote(hrx.at[pl.ds(0, 3)], hrx.at[pl.ds(0, 3)], hsend, precv, peer)

    def gain_copy(n):
        return remote(grx.at[me], grx.at[me], gsend, grecv, others[n])

    all_gains = remote(grx.at[pl.ds(0, 3)], grx.at[pl.ds(0, 3)], gsend, grecv, peer)
    early = n_chunks - 1

    def stat_copy(n, k, sem):
        return remote(stx.at[k], srx.at[k, n], ssend, srecv.at[sem], others[n])

    early_stats = remote(srx.at[pl.ds(0, early)], srx.at[pl.ds(0, early)], ssend, srecv.at[0], peer)
    late_stats = remote(srx.at[early], srx.at[early], ssend, srecv.at[1], peer)
    all_stats = remote(srx, srx, ssend, srecv.at[1], peer)

    for n in range(3):
        gain_copy(n).start()
    once_copy(0, True).start()
    cross_copy(0, True).start()
    diag_copy(0, True).start()
    peer_copy.start()

    with ns("gainwait"):
        all_gains.wait_recv()
    for k in range(1, n_chunks):
        once_copy(k, False).start()
        cross_copy(k, False).start()
        diag_copy(k, False).start()

    for s in range(4):
        for lo in range(0, d_local, LANES):
            size = min(LANES, d_local - lo)
            row = grx[s, :, lo : lo + size]
            row = jnp.concatenate([row] * (LANES // size), axis=-1)
            gcol[s * d_local + lo : s * d_local + lo + size, :] = jnp.broadcast_to(row, (LANES, LANES)).T[0:size]

    group = 32

    def normalise(k):
        def square(i, acc):
            at = pl.ds(pl.multiple_of(i * group, group), group)
            part = hrx[k, at, :].astype(jnp.float32)
            return acc + part * part

        sq = lax.fori_loop(0, d_full // group, square, jnp.zeros((group, chunk), jnp.float32), unroll=True)
        inv = lax.rsqrt(jnp.sum(sq, axis=0, keepdims=True) / d_full + NORM_EPS)

        def scale(i, carry):
            at = pl.ds(pl.multiple_of(i * group, group), group)
            gain = gcol[at, :]
            part = hrx[k, at, :].astype(jnp.float32)
            gains = jnp.concatenate([gain] * (chunk // LANES), axis=-1)
            xbuf[at, :] = (part * inv * gains).astype(jnp.bfloat16)
            return carry

        lax.fori_loop(0, d_full // group, scale, 0, unroll=True)

    sub = lax.broadcasted_iota(jnp.int32, (8, chunk), 0)

    def slot_of(j):
        return j % 2 if j < held else 2 + j - held

    def logits(j):
        lo = starts[j]
        size = blocks[j]
        zbuf[slot_of(j), 0:size, :] = jnp.dot(wbuf[lo : lo + size, :], xbuf[...], preferred_element_type=jnp.float32)

    def epilogue(j, want, state):
        lo = starts[j]
        size = blocks[j]

        def tile(i):
            return zbuf[slot_of(j), pl.ds(pl.multiple_of(i * 8, 8), 8), :]

        top = lax.fori_loop(1, size // 8, lambda i, t: jnp.maximum(t, tile(i)), tile(0), unroll=True)
        if state is None:
            total = jnp.zeros((8, chunk), jnp.float32)
            pick = total
        else:
            old, total, pick = state
            top = jnp.maximum(top, old)
            total = total * jnp.exp2((old - top) * LOG2E)

        def add(i, carry):
            total, pick = carry
            z = tile(i)
            total = total + jnp.exp2((z - top) * LOG2E)
            pick = jnp.where(want == lo + i * 8, z, pick)
            return total, pick

        total, pick = lax.fori_loop(0, size // 8, add, (total, pick), unroll=True)
        return top, total, pick

    def finish_chunk(k, state):
        m, total, pick = state
        top = jnp.max(m, axis=0, keepdims=True)
        total = jnp.sum(total * jnp.exp2((m - top) * LOG2E), axis=0, keepdims=True)
        pick = jnp.sum(pick, axis=0, keepdims=True)
        for n, stat in enumerate((top, total, pick)):
            for q in range(chunk // LANES):
                row = n * (chunk // LANES) + q
                stx[k, row : row + 1, :] = stat[:, q * LANES : (q + 1) * LANES]

    with ns("once0"):
        once_copy(0, True).wait_recv()
    forward_copy(0, True).start()
    with ns("peer0"):
        peer_copy.wait_recv()
    with ns("fwd0"):
        arrivals(0, True).wait_recv()
    with ns("wwait"):
        pltpu.make_async_copy(w_ref, wbuf, w_sem).wait()

    def targets_of(k):
        row = tbuf[pl.ds(k // per_chunk, 1), pl.ds(pl.multiple_of(lax.rem(k, per_chunk) * chunk, chunk), chunk)]
        local = row - me * v_local
        local = jnp.where((local >= 0) & (local < v_local), local, jnp.int32(-(1 << 20)))
        return jnp.broadcast_to(local, (8, chunk)) - sub

    def send_stats(k, sem):
        for n in range(3):
            stat_copy(n, k, sem).start()

    def step(k, carry):
        @pl.when(k > 0)
        def _():
            with ns("chunkwait"):
                arrivals(k, False).wait_recv()

        @pl.when(k < n_chunks - 1)
        def _():
            with ns("halfwait"):
                once_copy(k + 1, False).wait_recv()
            forward_copy(k + 1, False).start()

        @pl.when(k > 1)
        def _():
            send_stats(k - 2, 0)

        normalise(k)
        last_want, *last_state = carry
        want = targets_of(k)
        state = None
        for j in range(n_blocks):
            logits(j)
            if j == 0:
                for i in range(held, n_blocks):
                    last_state = epilogue(i, last_want, last_state)
                finish_chunk(lax.rem(k + n_chunks, n_chunks + 1), last_state)
            elif j <= held:
                state = epilogue(j - 1, want, state)
        if held == n_blocks:
            state = epilogue(held - 1, want, state)
        return (want, *state)

    blank = jnp.zeros((8, chunk), jnp.float32)
    for j in range(held, n_blocks):
        zbuf[slot_of(j), 0 : blocks[j], :] = jnp.zeros((blocks[j], chunk), jnp.float32)
    want, *state = lax.fori_loop(0, n_chunks, step, (jnp.full((8, chunk), -1, jnp.int32), blank, blank, blank))
    send_stats(n_chunks - 2, 0)
    with ns("last"):
        for j in range(held, n_blocks):
            state = epilogue(j, want, state)
        finish_chunk(n_chunks - 1, state)
    send_stats(n_chunks - 1, 1)

    per = chunk // LANES
    for k in range(n_chunks):
        with ns("statwait"):
            if k == 0:
                early_stats.wait_recv()
            if k == early:
                late_stats.wait_recv()
        stats = [stx[k]] + [srx[k, n] for n in range(3)]
        top = stats[0][0:per]
        for st in stats[1:]:
            top = jnp.maximum(top, st[0:per])
        total = jnp.zeros_like(top)
        pick = jnp.zeros_like(top)
        for st in stats:
            total = total + st[per : 2 * per] * jnp.exp2((st[0:per] - top) * LOG2E)
            pick = pick + st[2 * per : 3 * per]
        logp = pick - (top + jnp.log(total))
        seq, pos = divmod(k * chunk, per_seq)
        for q in range(per):
            out_ref[seq : seq + 1, pos + q * LANES : pos + (q + 1) * LANES] = logp[q : q + 1]

    with ns("sendwait"):
        all_sent.wait_send()
        all_gains.wait_send()
        all_stats.wait_send()


def solution(mesh):
    def local_score(hidden, ln_scale, w_head, targets, valid_mask):
        b, l, d_local = hidden.shape
        v_local = w_head.shape[1]
        rows, chunk, block, carried = b * l, 256, 128, 2
        blocks = (block,) * (v_local // block) + ((v_local % block,) if v_local % block else ())
        part = 2048
        w_parts = tuple((lo, min(part, v_local - lo)) for lo in range(0, v_local, part))
        n_chunks = rows // chunk
        any_spec = pl.BlockSpec(memory_space=pl.ANY)
        f32 = jnp.float32
        dma = pltpu.SemaphoreType.DMA
        token = pl.pallas_call(
            functools.partial(head_kernel, (d_local, v_local, rows, chunk, blocks, carried, w_parts)),
            out_shape=jax.ShapeDtypeStruct((b, l), f32),
            in_specs=[any_spec] * 4,
            out_specs=pl.BlockSpec(memory_space=pltpu.VMEM),
            scratch_shapes=[
                pltpu.VMEM((v_local, 4 * d_local), jnp.bfloat16),
                pltpu.VMEM((n_chunks, 4 * d_local, chunk), jnp.bfloat16),
                pltpu.VMEM((4, 1, d_local), f32),
                pltpu.VMEM((b, l), jnp.int32),
                pltpu.VMEM((4 * d_local, LANES), f32),
                pltpu.VMEM((4 * d_local, chunk), jnp.bfloat16),
                pltpu.VMEM((2 + carried, block, chunk), f32),
                pltpu.VMEM((n_chunks + 1, 8, LANES), f32),
                pltpu.VMEM((n_chunks, 3, 8, LANES), f32),
                dma, dma, dma((2,)),
                dma, dma, dma((n_chunks,)), dma((n_chunks,)),
                dma, dma, dma, dma((2,)),
            ],
            compiler_params=pltpu.CompilerParams(
                collective_id=0,
                has_side_effects=True,
                vmem_limit_bytes=40 * 1024 * 1024,
            ),
        )(*[
            pltpu.with_memory_space_constraint(x, pltpu.HBM)
            for x in (hidden.transpose(0, 2, 1), ln_scale.reshape(1, d_local), w_head.T, targets)
        ])
        token_logp = valid_mask.astype(f32) * token
        return token_logp, jnp.sum(token_logp, axis=1)

    return jax.shard_map(
        local_score,
        mesh=mesh,
        in_specs=(P("dp", None, "tp"), P("tp"), P(None, "tp"), P("dp", None), P("dp", None)),
        out_specs=(P("dp", None), P("dp")),
        check_vma=False,
    )
```

```python
import functools

import jax
import jax.numpy as jnp
from jax import lax
from jax.experimental import pallas as pl
from jax.experimental.pallas import tpu as pltpu
from jax.sharding import PartitionSpec as P

NORM_EPS = 1e-6
LOG2E = 1.4426950408889634
MESH = pl.DeviceIdType.MESH
LANES = 128


def head_kernel(
    cfg, h_ref, g_ref, w_ref, tgt_ref, out_ref,
    wbuf, hrx, grx, tbuf, gcol, xbuf, zbuf, stx, srx,
    w_sem, own_sem, small_sem, hsend, precv, orecv, arecv, gsend, grecv, ssend, srecv,
):
    d_local, v_local, rows, chunk, blocks, carried, w_parts = cfg
    n_chunks = rows // chunk
    d_full = 4 * d_local
    per_seq = h_ref.shape[2]
    per_chunk = per_seq // chunk
    starts = [sum(blocks[:j]) for j in range(len(blocks))]
    n_blocks = len(blocks)
    held = n_blocks - carried

    me = lax.axis_index("tp")
    peer = me + 1 - 2 * lax.rem(me, 2)
    cross = lax.rem(me + 2, 4)
    diag = lax.rem(peer + 2, 4)
    others = (peer, cross, diag)

    def piece(owner, k):
        return hrx.at[k, pl.ds(pl.multiple_of(owner * d_local, d_local), d_local)]

    own_rows = hrx.at[:, pl.ds(pl.multiple_of(me * d_local, d_local), d_local)]

    own = [
        pltpu.make_async_copy(
            h_ref.at[k // per_chunk, :, pl.ds((k % per_chunk) * chunk, chunk)], piece(me, k), own_sem
        )
        for k in range(n_chunks)
    ]
    own_g = pltpu.make_async_copy(g_ref, grx.at[me], small_sem.at[0])
    own_t = pltpu.make_async_copy(tgt_ref, tbuf, small_sem.at[1])
    load_w = [
        pltpu.make_async_copy(w_ref.at[pl.ds(lo, size)], wbuf.at[pl.ds(lo, size)], w_sem)
        for lo, size in w_parts
    ]
    own_g.start()
    for k in range(n_chunks):
        own[k].start()
    own_t.start()

    ns = jax.named_scope
    barrier = pltpu.get_barrier_semaphore()
    for other in others:
        pl.semaphore_signal(barrier, inc=1, device_id={"tp": other}, device_id_type=MESH)
    with ns("own"):
        own_g.wait()
        pltpu.make_async_copy(own_rows, own_rows, own_sem).wait()
        own_t.wait()
        for part in load_w:
            part.start()
    with ns("barrier"):
        pl.semaphore_wait(barrier, 3)

    def remote(src, dst, send, recv, dev):
        return pltpu.make_async_remote_copy(
            src_ref=src, dst_ref=dst, send_sem=send, recv_sem=recv, device_id={"tp": dev}, device_id_type=MESH
        )

    def once_rows(first):
        return (d_local * 3 // 4 if first else d_local // 3) // 16 * 16

    def once(owner, k, first):
        return hrx.at[k, pl.ds(pl.multiple_of(owner * d_local, 16), once_rows(first))]

    def direct(owner, k, first):
        n = once_rows(first)
        return hrx.at[k, pl.ds(pl.multiple_of(owner * d_local + n, 16), d_local - n)]

    def once_copy(k, first):
        return remote(once(me, k, first), once(me, k, first), hsend, orecv.at[k], diag)

    def forward_copy(k, first):
        return remote(once(diag, k, first), once(diag, k, first), hsend, arecv.at[k], peer)

    def cross_copy(k, first):
        return remote(direct(me, k, first), direct(me, k, first), hsend, arecv.at[k], cross)

    def diag_copy(k, first):
        return remote(direct(me, k, first), direct(me, k, first), hsend, arecv.at[k], diag)

    def arrivals(k, first):
        got = hrx.at[k, pl.ds(0, 2 * d_local - once_rows(first))]
        return remote(got, got, hsend, arecv.at[k], peer)

    peer_copy = remote(own_rows, own_rows, hsend, precv, peer)
    all_sent = remote(hrx.at[pl.ds(0, 3)], hrx.at[pl.ds(0, 3)], hsend, precv, peer)

    def gain_copy(n):
        return remote(grx.at[me], grx.at[me], gsend, grecv.at[n], others[n])

    all_gains = remote(grx.at[pl.ds(0, 3)], grx.at[pl.ds(0, 3)], gsend, grecv.at[0], peer)
    early = n_chunks - 1

    def stat_copy(n, k, sem):
        return remote(stx.at[k], srx.at[k, n], ssend, srecv.at[sem], others[n])

    early_stats = remote(srx.at[pl.ds(0, early)], srx.at[pl.ds(0, early)], ssend, srecv.at[0], peer)
    late_stats = remote(srx.at[early], srx.at[early], ssend, srecv.at[1], peer)
    all_stats = remote(srx, srx, ssend, srecv.at[1], peer)

    for n in range(3):
        gain_copy(n).start()
    once_copy(0, True).start()
    cross_copy(0, True).start()
    diag_copy(0, True).start()
    peer_copy.start()

    with ns("gainwait"):
        gain_copy(2).wait_recv()
    for k in range(1, n_chunks):
        once_copy(k, False).start()
        cross_copy(k, False).start()
        diag_copy(k, False).start()

    for n in range(2):
        gain_copy(n).wait_recv()
    for s in range(4):
        for lo in range(0, d_local, LANES):
            size = min(LANES, d_local - lo)
            row = grx[s, :, lo : lo + size]
            row = jnp.concatenate([row] * (LANES // size), axis=-1)
            gcol[s * d_local + lo : s * d_local + lo + size, :] = jnp.broadcast_to(row, (LANES, LANES)).T[0:size]

    group = 32

    def normalise(k):
        def square(i, acc):
            at = pl.ds(pl.multiple_of(i * group, group), group)
            part = hrx[k, at, :].astype(jnp.float32)
            return acc + part * part

        sq = lax.fori_loop(0, d_full // group, square, jnp.zeros((group, chunk), jnp.float32), unroll=True)
        inv = lax.rsqrt(jnp.sum(sq, axis=0, keepdims=True) / d_full + NORM_EPS)

        def scale(i, carry):
            at = pl.ds(pl.multiple_of(i * group, group), group)
            gain = gcol[at, :]
            part = hrx[k, at, :].astype(jnp.float32)
            gains = jnp.concatenate([gain] * (chunk // LANES), axis=-1)
            xbuf[at, :] = (part * inv * gains).astype(jnp.bfloat16)
            return carry

        lax.fori_loop(0, d_full // group, scale, 0, unroll=True)

    sub = lax.broadcasted_iota(jnp.int32, (8, chunk), 0)

    def slot_of(j):
        return j % 2 if j < held else 2 + j - held

    def logits(j):
        lo = starts[j]
        size = blocks[j]
        zbuf[slot_of(j), 0:size, :] = jnp.dot(wbuf[lo : lo + size, :], xbuf[...], preferred_element_type=jnp.float32)

    def epilogue(j, want, state):
        lo = starts[j]
        size = blocks[j]

        def tile(i):
            return zbuf[slot_of(j), pl.ds(pl.multiple_of(i * 8, 8), 8), :]

        top = lax.fori_loop(1, size // 8, lambda i, t: jnp.maximum(t, tile(i)), tile(0), unroll=True)
        if state is None:
            total = jnp.zeros((8, chunk), jnp.float32)
            pick = total
        else:
            old, total, pick = state
            top = jnp.maximum(top, old)
            total = total * jnp.exp2((old - top) * LOG2E)

        def add(i, carry):
            total, pick = carry
            z = tile(i)
            total = total + jnp.exp2((z - top) * LOG2E)
            pick = jnp.where(want == lo + i * 8, z, pick)
            return total, pick

        total, pick = lax.fori_loop(0, size // 8, add, (total, pick), unroll=True)
        return top, total, pick

    def finish_chunk(k, state):
        m, total, pick = state
        top = jnp.max(m, axis=0, keepdims=True)
        total = jnp.sum(total * jnp.exp2((m - top) * LOG2E), axis=0, keepdims=True)
        pick = jnp.sum(pick, axis=0, keepdims=True)
        for n, stat in enumerate((top, total, pick)):
            for q in range(chunk // LANES):
                row = n * (chunk // LANES) + q
                stx[k, row : row + 1, :] = stat[:, q * LANES : (q + 1) * LANES]

    with ns("once0"):
        once_copy(0, True).wait_recv()
    forward_copy(0, True).start()
    with ns("peer0"):
        peer_copy.wait_recv()
    with ns("fwd0"):
        arrivals(0, True).wait_recv()
    with ns("wwait"):
        pltpu.make_async_copy(w_ref, wbuf, w_sem).wait()

    def targets_of(k):
        row = tbuf[pl.ds(k // per_chunk, 1), pl.ds(pl.multiple_of(lax.rem(k, per_chunk) * chunk, chunk), chunk)]
        local = row - me * v_local
        local = jnp.where((local >= 0) & (local < v_local), local, jnp.int32(-(1 << 20)))
        return jnp.broadcast_to(local, (8, chunk)) - sub

    def send_stats(k, sem):
        for n in range(3):
            stat_copy(n, k, sem).start()

    def step(k, carry):
        @pl.when(k > 0)
        def _():
            with ns("chunkwait"):
                arrivals(k, False).wait_recv()

        @pl.when(k < n_chunks - 1)
        def _():
            with ns("halfwait"):
                once_copy(k + 1, False).wait_recv()
            forward_copy(k + 1, False).start()

        @pl.when(k > 1)
        def _():
            send_stats(k - 2, 0)

        normalise(k)
        last_want, *last_state = carry
        want = targets_of(k)
        state = None
        for j in range(n_blocks):
            logits(j)
            if j == 0:
                for i in range(held, n_blocks):
                    last_state = epilogue(i, last_want, last_state)
                finish_chunk(lax.rem(k + n_chunks, n_chunks + 1), last_state)
            elif j <= held:
                state = epilogue(j - 1, want, state)
        if held == n_blocks:
            state = epilogue(held - 1, want, state)
        return (want, *state)

    blank = jnp.zeros((8, chunk), jnp.float32)
    for j in range(held, n_blocks):
        zbuf[slot_of(j), 0 : blocks[j], :] = jnp.zeros((blocks[j], chunk), jnp.float32)
    want, *state = lax.fori_loop(0, n_chunks, step, (jnp.full((8, chunk), -1, jnp.int32), blank, blank, blank))
    send_stats(n_chunks - 2, 0)
    with ns("last"):
        for j in range(held, n_blocks):
            state = epilogue(j, want, state)
        finish_chunk(n_chunks - 1, state)
    send_stats(n_chunks - 1, 1)

    per = chunk // LANES
    for k in range(n_chunks):
        with ns("statwait"):
            if k == 0:
                early_stats.wait_recv()
            if k == early:
                late_stats.wait_recv()
        stats = [stx[k]] + [srx[k, n] for n in range(3)]
        top = stats[0][0:per]
        for st in stats[1:]:
            top = jnp.maximum(top, st[0:per])
        total = jnp.zeros_like(top)
        pick = jnp.zeros_like(top)
        for st in stats:
            total = total + st[per : 2 * per] * jnp.exp2((st[0:per] - top) * LOG2E)
            pick = pick + st[2 * per : 3 * per]
        logp = pick - (top + jnp.log(total))
        seq, pos = divmod(k * chunk, per_seq)
        for q in range(per):
            out_ref[seq : seq + 1, pos + q * LANES : pos + (q + 1) * LANES] = logp[q : q + 1]

    with ns("sendwait"):
        all_sent.wait_send()
        all_gains.wait_send()
        all_stats.wait_send()


def solution(mesh):
    def local_score(hidden, ln_scale, w_head, targets, valid_mask):
        b, l, d_local = hidden.shape
        v_local = w_head.shape[1]
        rows, chunk, block, carried = b * l, 256, 224, 2
        blocks = (block,) * (v_local // block) + ((v_local % block,) if v_local % block else ())
        part = 2048
        w_parts = tuple((lo, min(part, v_local - lo)) for lo in range(0, v_local, part))
        n_chunks = rows // chunk
        any_spec = pl.BlockSpec(memory_space=pl.ANY)
        f32 = jnp.float32
        dma = pltpu.SemaphoreType.DMA
        token = pl.pallas_call(
            functools.partial(head_kernel, (d_local, v_local, rows, chunk, blocks, carried, w_parts)),
            out_shape=jax.ShapeDtypeStruct((b, l), f32),
            in_specs=[any_spec] * 4,
            out_specs=pl.BlockSpec(memory_space=pltpu.VMEM),
            scratch_shapes=[
                pltpu.VMEM((v_local, 4 * d_local), jnp.bfloat16),
                pltpu.VMEM((n_chunks, 4 * d_local, chunk), jnp.bfloat16),
                pltpu.VMEM((4, 1, d_local), f32),
                pltpu.VMEM((b, l), jnp.int32),
                pltpu.VMEM((4 * d_local, LANES), f32),
                pltpu.VMEM((4 * d_local, chunk), jnp.bfloat16),
                pltpu.VMEM((2 + carried, block, chunk), f32),
                pltpu.VMEM((n_chunks + 1, 8, LANES), f32),
                pltpu.VMEM((n_chunks, 3, 8, LANES), f32),
                dma, dma, dma((2,)),
                dma, dma, dma((n_chunks,)), dma((n_chunks,)),
                dma, dma((3,)), dma, dma((2,)),
            ],
            compiler_params=pltpu.CompilerParams(
                collective_id=0,
                has_side_effects=True,
                vmem_limit_bytes=40 * 1024 * 1024,
            ),
        )(*[
            pltpu.with_memory_space_constraint(x, pltpu.HBM)
            for x in (hidden.transpose(0, 2, 1), ln_scale.reshape(1, d_local), w_head.T, targets)
        ])
        token_logp = valid_mask.astype(f32) * token
        return token_logp, jnp.sum(token_logp, axis=1)

    return jax.shard_map(
        local_score,
        mesh=mesh,
        in_specs=(P("dp", None, "tp"), P("tp"), P(None, "tp"), P("dp", None), P("dp", None)),
        out_specs=(P("dp", None), P("dp")),
        check_vma=False,
    )
```

```python
import functools

import jax
import jax.numpy as jnp
from jax import lax
from jax.experimental import pallas as pl
from jax.experimental.pallas import tpu as pltpu
from jax.sharding import PartitionSpec as P

NORM_EPS = 1e-6
LOG2E = 1.4426950408889634
MESH = pl.DeviceIdType.MESH
LANES = 128


def head_kernel(
    cfg, h_ref, g_ref, w_ref, tgt_ref, out_ref,
    wbuf, hrx, grx, tbuf, gcol, xbuf, zbuf, stx, srx,
    w_sem, own_sem, small_sem, hsend, precv, orecv, arecv, gsend, grecv, ssend, srecv,
):
    d_local, v_local, rows, chunk, blocks, carried, w_parts, once_rows = cfg
    n_chunks = rows // chunk
    d_full = 4 * d_local
    per_seq = h_ref.shape[2]
    per_chunk = per_seq // chunk
    starts = [sum(blocks[:j]) for j in range(len(blocks))]
    n_blocks = len(blocks)
    held = n_blocks - carried

    me = lax.axis_index("tp")
    peer = me + 1 - 2 * lax.rem(me, 2)
    cross = lax.rem(me + 2, 4)
    diag = lax.rem(peer + 2, 4)
    others = (peer, cross, diag)

    def piece(owner, k):
        return hrx.at[k, pl.ds(pl.multiple_of(owner * d_local, d_local), d_local)]

    own_rows = hrx.at[:, pl.ds(pl.multiple_of(me * d_local, d_local), d_local)]

    own = [
        pltpu.make_async_copy(
            h_ref.at[k // per_chunk, :, pl.ds((k % per_chunk) * chunk, chunk)], piece(me, k), own_sem
        )
        for k in range(n_chunks)
    ]
    own_g = pltpu.make_async_copy(g_ref, grx.at[me], small_sem.at[0])
    own_t = pltpu.make_async_copy(tgt_ref, tbuf, small_sem.at[1])
    load_w = [
        pltpu.make_async_copy(w_ref.at[pl.ds(lo, size)], wbuf.at[pl.ds(lo, size)], w_sem)
        for lo, size in w_parts
    ]
    own_g.start()
    for k in range(n_chunks):
        own[k].start()
    own_t.start()

    ns = jax.named_scope
    barrier = pltpu.get_barrier_semaphore()
    for other in others:
        pl.semaphore_signal(barrier, inc=1, device_id={"tp": other}, device_id_type=MESH)
    with ns("own"):
        own_g.wait()
        pltpu.make_async_copy(own_rows, own_rows, own_sem).wait()
        own_t.wait()
        for part in load_w:
            part.start()
    with ns("barrier"):
        pl.semaphore_wait(barrier, 3)

    def remote(src, dst, send, recv, dev):
        return pltpu.make_async_remote_copy(
            src_ref=src, dst_ref=dst, send_sem=send, recv_sem=recv, device_id={"tp": dev}, device_id_type=MESH
        )

    def once(owner, k):
        return hrx.at[k, pl.ds(pl.multiple_of(owner * d_local, 16), once_rows[k])]

    def direct(owner, k):
        n = once_rows[k]
        return hrx.at[k, pl.ds(pl.multiple_of(owner * d_local + n, 16), d_local - n)]

    def once_copy(k):
        return remote(once(me, k), once(me, k), hsend, orecv.at[k], diag)

    def forward_copy(k):
        return remote(once(diag, k), once(diag, k), hsend, arecv.at[k], peer)

    def cross_copy(k):
        return remote(direct(me, k), direct(me, k), hsend, arecv.at[k], cross)

    def diag_copy(k):
        return remote(direct(me, k), direct(me, k), hsend, arecv.at[k], diag)

    def arrivals(k):
        got = hrx.at[k, pl.ds(0, 2 * d_local - once_rows[k])]
        return remote(got, got, hsend, arecv.at[k], peer)

    peer_copy = remote(own_rows, own_rows, hsend, precv, peer)
    all_sent = remote(hrx.at[pl.ds(0, 3)], hrx.at[pl.ds(0, 3)], hsend, precv, peer)

    def gain_copy(n):
        return remote(grx.at[me], grx.at[me], gsend, grecv, others[n])

    all_gains = remote(grx.at[pl.ds(0, 3)], grx.at[pl.ds(0, 3)], gsend, grecv, peer)
    early = n_chunks - 1

    def stat_copy(n, k, sem):
        return remote(stx.at[k], srx.at[k, n], ssend, srecv.at[sem], others[n])

    early_stats = remote(srx.at[pl.ds(0, early)], srx.at[pl.ds(0, early)], ssend, srecv.at[0], peer)
    late_stats = remote(srx.at[early], srx.at[early], ssend, srecv.at[1], peer)
    all_stats = remote(srx, srx, ssend, srecv.at[1], peer)

    for n in range(3):
        gain_copy(n).start()
    once_copy(0).start()
    cross_copy(0).start()
    diag_copy(0).start()
    peer_copy.start()

    with ns("gainwait"):
        all_gains.wait_recv()
    for k in range(1, n_chunks):
        once_copy(k).start()
        cross_copy(k).start()
        diag_copy(k).start()

    for s in range(4):
        for lo in range(0, d_local, LANES):
            size = min(LANES, d_local - lo)
            row = grx[s, :, lo : lo + size]
            row = jnp.concatenate([row] * (LANES // size), axis=-1)
            gcol[s * d_local + lo : s * d_local + lo + size, :] = jnp.broadcast_to(row, (LANES, LANES)).T[0:size]

    group = 32

    def normalise(k):
        def square(i, acc):
            at = pl.ds(pl.multiple_of(i * group, group), group)
            part = hrx[k, at, :].astype(jnp.float32)
            return acc + part * part

        sq = lax.fori_loop(0, d_full // group, square, jnp.zeros((group, chunk), jnp.float32), unroll=True)
        inv = lax.rsqrt(jnp.sum(sq, axis=0, keepdims=True) / d_full + NORM_EPS)

        def scale(i, carry):
            at = pl.ds(pl.multiple_of(i * group, group), group)
            gain = gcol[at, :]
            part = hrx[k, at, :].astype(jnp.float32)
            gains = jnp.concatenate([gain] * (chunk // LANES), axis=-1)
            xbuf[at, :] = (part * inv * gains).astype(jnp.bfloat16)
            return carry

        lax.fori_loop(0, d_full // group, scale, 0, unroll=True)

    sub = lax.broadcasted_iota(jnp.int32, (8, chunk), 0)

    def slot_of(j):
        return j % 2 if j < held else 2 + j - held

    def logits(j):
        lo = starts[j]
        size = blocks[j]
        zbuf[slot_of(j), 0:size, :] = jnp.dot(wbuf[lo : lo + size, :], xbuf[...], preferred_element_type=jnp.float32)

    def epilogue(j, want, state):
        lo = starts[j]
        size = blocks[j]

        def tile(i):
            return zbuf[slot_of(j), pl.ds(pl.multiple_of(i * 8, 8), 8), :]

        top = lax.fori_loop(1, size // 8, lambda i, t: jnp.maximum(t, tile(i)), tile(0), unroll=True)
        if state is None:
            total = jnp.zeros((8, chunk), jnp.float32)
            pick = total
        else:
            old, total, pick = state
            top = jnp.maximum(top, old)
            total = total * jnp.exp2((old - top) * LOG2E)

        def add(i, carry):
            total, pick = carry
            z = tile(i)
            total = total + jnp.exp2((z - top) * LOG2E)
            pick = jnp.where(want == lo + i * 8, z, pick)
            return total, pick

        total, pick = lax.fori_loop(0, size // 8, add, (total, pick), unroll=True)
        return top, total, pick

    def finish_chunk(k, state):
        m, total, pick = state
        top = jnp.max(m, axis=0, keepdims=True)
        total = jnp.sum(total * jnp.exp2((m - top) * LOG2E), axis=0, keepdims=True)
        pick = jnp.sum(pick, axis=0, keepdims=True)
        for n, stat in enumerate((top, total, pick)):
            for q in range(chunk // LANES):
                row = n * (chunk // LANES) + q
                stx[k, row : row + 1, :] = stat[:, q * LANES : (q + 1) * LANES]

    with ns("once0"):
        once_copy(0).wait_recv()
    forward_copy(0).start()
    with ns("peer0"):
        peer_copy.wait_recv()
    with ns("fwd0"):
        arrivals(0).wait_recv()
    with ns("wwait"):
        pltpu.make_async_copy(w_ref, wbuf, w_sem).wait()

    def targets_of(k):
        row = tbuf[pl.ds(k // per_chunk, 1), pl.ds(pl.multiple_of(lax.rem(k, per_chunk) * chunk, chunk), chunk)]
        local = row - me * v_local
        local = jnp.where((local >= 0) & (local < v_local), local, jnp.int32(-(1 << 20)))
        return jnp.broadcast_to(local, (8, chunk)) - sub

    def send_stats(k, sem):
        for n in range(3):
            stat_copy(n, k, sem).start()

    def step(k, carry):
        for n in range(n_chunks):
            @pl.when(k == n)
            def _():
                if n:
                    with ns("chunkwait"):
                        arrivals(n).wait_recv()
                if n + 1 < n_chunks:
                    with ns("oncewait"):
                        once_copy(n + 1).wait_recv()
                    forward_copy(n + 1).start()

        @pl.when(k > 1)
        def _():
            send_stats(k - 2, 0)

        normalise(k)
        last_want, *last_state = carry
        want = targets_of(k)
        state = None
        for j in range(n_blocks):
            logits(j)
            if j == 0:
                for i in range(held, n_blocks):
                    last_state = epilogue(i, last_want, last_state)
                finish_chunk(lax.rem(k + n_chunks, n_chunks + 1), last_state)
            elif j <= held:
                state = epilogue(j - 1, want, state)
        if held == n_blocks:
            state = epilogue(held - 1, want, state)
        return (want, *state)

    blank = jnp.zeros((8, chunk), jnp.float32)
    for j in range(held, n_blocks):
        zbuf[slot_of(j), 0 : blocks[j], :] = jnp.zeros((blocks[j], chunk), jnp.float32)
    want, *state = lax.fori_loop(0, n_chunks, step, (jnp.full((8, chunk), -1, jnp.int32), blank, blank, blank))
    send_stats(n_chunks - 2, 0)
    with ns("last"):
        for j in range(held, n_blocks):
            state = epilogue(j, want, state)
        finish_chunk(n_chunks - 1, state)
    send_stats(n_chunks - 1, 1)

    per = chunk // LANES
    for k in range(n_chunks):
        with ns("statwait"):
            if k == 0:
                early_stats.wait_recv()
            if k == early:
                late_stats.wait_recv()
        stats = [stx[k]] + [srx[k, n] for n in range(3)]
        top = stats[0][0:per]
        for st in stats[1:]:
            top = jnp.maximum(top, st[0:per])
        total = jnp.zeros_like(top)
        pick = jnp.zeros_like(top)
        for st in stats:
            total = total + st[per : 2 * per] * jnp.exp2((st[0:per] - top) * LOG2E)
            pick = pick + st[2 * per : 3 * per]
        logp = pick - (top + jnp.log(total))
        seq, pos = divmod(k * chunk, per_seq)
        for q in range(per):
            out_ref[seq : seq + 1, pos + q * LANES : pos + (q + 1) * LANES] = logp[q : q + 1]

    with ns("sendwait"):
        all_sent.wait_send()
        all_gains.wait_send()
        all_stats.wait_send()


def solution(mesh):
    def local_score(hidden, ln_scale, w_head, targets, valid_mask):
        b, l, d_local = hidden.shape
        v_local = w_head.shape[1]
        rows, chunk, block, carried = b * l, 256, 224, 2
        blocks = (block,) * (v_local // block) + ((v_local % block,) if v_local % block else ())
        part = 2048
        w_parts = tuple((lo, min(part, v_local - lo)) for lo in range(0, v_local, part))
        n_chunks = rows // chunk
        once_rows = (d_local * 3 // 4 // 16 * 16, d_local // 6 // 16 * 16) + (d_local // 3 // 16 * 16,) * (n_chunks - 2)
        any_spec = pl.BlockSpec(memory_space=pl.ANY)
        f32 = jnp.float32
        dma = pltpu.SemaphoreType.DMA
        token = pl.pallas_call(
            functools.partial(head_kernel, (d_local, v_local, rows, chunk, blocks, carried, w_parts, once_rows)),
            out_shape=jax.ShapeDtypeStruct((b, l), f32),
            in_specs=[any_spec] * 4,
            out_specs=pl.BlockSpec(memory_space=pltpu.VMEM),
            scratch_shapes=[
                pltpu.VMEM((v_local, 4 * d_local), jnp.bfloat16),
                pltpu.VMEM((n_chunks, 4 * d_local, chunk), jnp.bfloat16),
                pltpu.VMEM((4, 1, d_local), f32),
                pltpu.VMEM((b, l), jnp.int32),
                pltpu.VMEM((4 * d_local, LANES), f32),
                pltpu.VMEM((4 * d_local, chunk), jnp.bfloat16),
                pltpu.VMEM((2 + carried, block, chunk), f32),
                pltpu.VMEM((n_chunks + 1, 8, LANES), f32),
                pltpu.VMEM((n_chunks, 3, 8, LANES), f32),
                dma, dma, dma((2,)),
                dma, dma, dma((n_chunks,)), dma((n_chunks,)),
                dma, dma, dma, dma((2,)),
            ],
            compiler_params=pltpu.CompilerParams(
                collective_id=0,
                has_side_effects=True,
                vmem_limit_bytes=40 * 1024 * 1024,
            ),
        )(*[
            pltpu.with_memory_space_constraint(x, pltpu.HBM)
            for x in (hidden.transpose(0, 2, 1), ln_scale.reshape(1, d_local), w_head.T, targets)
        ])
        token_logp = valid_mask.astype(f32) * token
        return token_logp, jnp.sum(token_logp, axis=1)

    return jax.shard_map(
        local_score,
        mesh=mesh,
        in_specs=(P("dp", None, "tp"), P("tp"), P(None, "tp"), P("dp", None), P("dp", None)),
        out_specs=(P("dp", None), P("dp")),
        check_vma=False,
    )
```

```python
import functools

import jax
import jax.numpy as jnp
from jax import lax
from jax.experimental import pallas as pl
from jax.experimental.pallas import tpu as pltpu
from jax.sharding import PartitionSpec as P

NORM_EPS = 1e-6
LOG2E = 1.4426950408889634
MESH = pl.DeviceIdType.MESH
LANES = 128


def head_kernel(
    cfg, h_ref, g_ref, w_ref, tgt_ref, out_ref,
    wbuf, hrx, grx, tbuf, gcol, xbuf, zbuf, stx, srx,
    w_sem, own_sem, small_sem, hsend, precv, orecv, arecv, gsend, grecv, ssend, srecv,
):
    d_local, v_local, rows, chunk, blocks, carried, w_parts, once_rows = cfg
    n_chunks = rows // chunk
    d_full = 4 * d_local
    per_seq = h_ref.shape[2]
    per_chunk = per_seq // chunk
    starts = [sum(blocks[:j]) for j in range(len(blocks))]
    n_blocks = len(blocks)
    held = n_blocks - carried

    me = lax.axis_index("tp")
    peer = me + 1 - 2 * lax.rem(me, 2)
    cross = lax.rem(me + 2, 4)
    diag = lax.rem(peer + 2, 4)
    others = (peer, cross, diag)

    def piece(owner, k):
        return hrx.at[k, pl.ds(pl.multiple_of(owner * d_local, d_local), d_local)]

    own_rows = hrx.at[:, pl.ds(pl.multiple_of(me * d_local, d_local), d_local)]

    own = [
        pltpu.make_async_copy(
            h_ref.at[k // per_chunk, :, pl.ds((k % per_chunk) * chunk, chunk)], piece(me, k), own_sem
        )
        for k in range(n_chunks)
    ]
    own_g = pltpu.make_async_copy(g_ref, grx.at[me], small_sem.at[0])
    own_t = pltpu.make_async_copy(tgt_ref, tbuf, small_sem.at[1])
    load_w = [
        pltpu.make_async_copy(w_ref.at[pl.ds(lo, size)], wbuf.at[pl.ds(lo, size)], w_sem)
        for lo, size in w_parts
    ]
    own_g.start()
    for k in range(n_chunks):
        own[k].start()
    own_t.start()

    ns = jax.named_scope
    barrier = pltpu.get_barrier_semaphore()
    for other in others:
        pl.semaphore_signal(barrier, inc=1, device_id={"tp": other}, device_id_type=MESH)
    with ns("own"):
        own_g.wait()
        pltpu.make_async_copy(own_rows, own_rows, own_sem).wait()
        own_t.wait()
        for part in load_w:
            part.start()
    with ns("barrier"):
        pl.semaphore_wait(barrier, 3)

    def remote(src, dst, send, recv, dev):
        return pltpu.make_async_remote_copy(
            src_ref=src, dst_ref=dst, send_sem=send, recv_sem=recv, device_id={"tp": dev}, device_id_type=MESH
        )

    def once(owner, k):
        return hrx.at[k, pl.ds(pl.multiple_of(owner * d_local, 16), once_rows[k])]

    def direct(owner, k):
        n = once_rows[k]
        return hrx.at[k, pl.ds(pl.multiple_of(owner * d_local + n, 16), d_local - n)]

    def once_copy(k):
        return remote(once(me, k), once(me, k), hsend, orecv.at[k], diag)

    def forward_copy(k):
        return remote(once(diag, k), once(diag, k), hsend, arecv.at[k], peer)

    def cross_copy(k):
        return remote(direct(me, k), direct(me, k), hsend, arecv.at[k], cross)

    def diag_copy(k):
        return remote(direct(me, k), direct(me, k), hsend, arecv.at[k], diag)

    def arrivals(k):
        got = hrx.at[k, pl.ds(0, 2 * d_local - once_rows[k])]
        return remote(got, got, hsend, arecv.at[k], peer)

    peer_copy = remote(own_rows, own_rows, hsend, precv, peer)
    all_sent = remote(hrx.at[pl.ds(0, 3)], hrx.at[pl.ds(0, 3)], hsend, precv, peer)

    def gain_copy(n):
        return remote(grx.at[me], grx.at[me], gsend, grecv, others[n])

    all_gains = remote(grx.at[pl.ds(0, 3)], grx.at[pl.ds(0, 3)], gsend, grecv, peer)
    early = n_chunks - 1

    def stat_copy(n, k, sem):
        return remote(stx.at[k], srx.at[k, n], ssend, srecv.at[sem], others[n])

    early_stats = remote(srx.at[pl.ds(0, early)], srx.at[pl.ds(0, early)], ssend, srecv.at[0], peer)
    late_stats = remote(srx.at[early], srx.at[early], ssend, srecv.at[1], peer)
    all_stats = remote(srx, srx, ssend, srecv.at[1], peer)

    for n in range(3):
        gain_copy(n).start()
    once_copy(0).start()
    cross_copy(0).start()
    diag_copy(0).start()
    peer_copy.start()

    with ns("gainwait"):
        all_gains.wait_recv()
    for k in range(1, n_chunks):
        once_copy(k).start()
        cross_copy(k).start()
        diag_copy(k).start()

    for s in range(4):
        for lo in range(0, d_local, LANES):
            size = min(LANES, d_local - lo)
            row = grx[s, :, lo : lo + size]
            row = jnp.concatenate([row] * (LANES // size), axis=-1)
            gcol[s * d_local + lo : s * d_local + lo + size, :] = jnp.broadcast_to(row, (LANES, LANES)).T[0:size]

    group = 32

    def normalise(k):
        def square(i, acc):
            at = pl.ds(pl.multiple_of(i * group, group), group)
            part = hrx[k, at, :].astype(jnp.float32)
            return acc + part * part

        sq = lax.fori_loop(0, d_full // group, square, jnp.zeros((group, chunk), jnp.float32), unroll=True)
        inv = lax.rsqrt(jnp.sum(sq, axis=0, keepdims=True) / d_full + NORM_EPS)

        def scale(i, carry):
            at = pl.ds(pl.multiple_of(i * group, group), group)
            gain = gcol[at, :]
            part = hrx[k, at, :].astype(jnp.float32)
            gains = jnp.concatenate([gain] * (chunk // LANES), axis=-1)
            xbuf[at, :] = (part * inv * gains).astype(jnp.bfloat16)
            return carry

        lax.fori_loop(0, d_full // group, scale, 0, unroll=True)

    sub = lax.broadcasted_iota(jnp.int32, (8, chunk), 0)

    def slot_of(j):
        return j % 2 if j < held else 2 + j - held

    def logits(j):
        lo = starts[j]
        size = blocks[j]
        zbuf[slot_of(j), 0:size, :] = jnp.dot(wbuf[lo : lo + size, :], xbuf[...], preferred_element_type=jnp.float32)

    def epilogue(j, want, state):
        lo = starts[j]
        size = blocks[j]

        def tile(i):
            return zbuf[slot_of(j), pl.ds(pl.multiple_of(i * 8, 8), 8), :]

        top = lax.fori_loop(1, size // 8, lambda i, t: jnp.maximum(t, tile(i)), tile(0), unroll=True)
        if state is None:
            total = jnp.zeros((8, chunk), jnp.float32)
            pick = total
        else:
            old, total, pick = state
            top = jnp.maximum(top, old)
            total = total * jnp.exp2((old - top) * LOG2E)

        def add(i, carry):
            total, pick = carry
            z = tile(i)
            total = total + jnp.exp2((z - top) * LOG2E)
            pick = jnp.where(want == lo + i * 8, z, pick)
            return total, pick

        total, pick = lax.fori_loop(0, size // 8, add, (total, pick), unroll=True)
        return top, total, pick

    def finish_chunk(k, state):
        m, total, pick = state
        top = jnp.max(m, axis=0, keepdims=True)
        total = jnp.sum(total * jnp.exp2((m - top) * LOG2E), axis=0, keepdims=True)
        pick = jnp.sum(pick, axis=0, keepdims=True)
        for n, stat in enumerate((top, total, pick)):
            for q in range(chunk // LANES):
                row = n * (chunk // LANES) + q
                stx[k, row : row + 1, :] = stat[:, q * LANES : (q + 1) * LANES]

    with ns("once0"):
        once_copy(0).wait_recv()
    forward_copy(0).start()
    with ns("peer0"):
        peer_copy.wait_recv()
    with ns("fwd0"):
        arrivals(0).wait_recv()
    with ns("wwait"):
        pltpu.make_async_copy(w_ref, wbuf, w_sem).wait()

    def targets_of(k):
        row = tbuf[pl.ds(k // per_chunk, 1), pl.ds(pl.multiple_of(lax.rem(k, per_chunk) * chunk, chunk), chunk)]
        local = row - me * v_local
        local = jnp.where((local >= 0) & (local < v_local), local, jnp.int32(-(1 << 20)))
        return jnp.broadcast_to(local, (8, chunk)) - sub

    def send_stats(k, sem):
        for n in range(3):
            stat_copy(n, k, sem).start()

    def step(k, carry):
        for n in range(n_chunks):
            @pl.when(k == n)
            def _():
                if n:
                    with ns("chunkwait"):
                        arrivals(n).wait_recv()
                if n + 1 < n_chunks:
                    with ns("oncewait"):
                        once_copy(n + 1).wait_recv()
                    forward_copy(n + 1).start()

        @pl.when(k > 1)
        def _():
            send_stats(k - 2, 0)

        normalise(k)
        last_want, *last_state = carry
        want = targets_of(k)
        state = None
        for j in range(n_blocks):
            logits(j)
            if j == 0:
                for i in range(held, n_blocks):
                    last_state = epilogue(i, last_want, last_state)
                finish_chunk(lax.rem(k + n_chunks, n_chunks + 1), last_state)
            elif j <= held:
                state = epilogue(j - 1, want, state)
        if held == n_blocks:
            state = epilogue(held - 1, want, state)
        return (want, *state)

    blank = jnp.zeros((8, chunk), jnp.float32)
    for j in range(held, n_blocks):
        zbuf[slot_of(j), 0 : blocks[j], :] = jnp.zeros((blocks[j], chunk), jnp.float32)
    want, *state = lax.fori_loop(0, n_chunks, step, (jnp.full((8, chunk), -1, jnp.int32), blank, blank, blank))
    send_stats(n_chunks - 2, 0)
    with ns("last"):
        for j in range(held, n_blocks):
            state = epilogue(j, want, state)
        finish_chunk(n_chunks - 1, state)
    send_stats(n_chunks - 1, 1)

    per = chunk // LANES
    for k in range(n_chunks):
        with ns("statwait"):
            if k == 0:
                early_stats.wait_recv()
            if k == early:
                late_stats.wait_recv()
        stats = [stx[k]] + [srx[k, n] for n in range(3)]
        top = stats[0][0:per]
        for st in stats[1:]:
            top = jnp.maximum(top, st[0:per])
        total = jnp.zeros_like(top)
        pick = jnp.zeros_like(top)
        for st in stats:
            total = total + st[per : 2 * per] * jnp.exp2((st[0:per] - top) * LOG2E)
            pick = pick + st[2 * per : 3 * per]
        logp = pick - (top + jnp.log(total))
        seq, pos = divmod(k * chunk, per_seq)
        for q in range(per):
            out_ref[seq : seq + 1, pos + q * LANES : pos + (q + 1) * LANES] = logp[q : q + 1]

    with ns("sendwait"):
        all_sent.wait_send()
        all_gains.wait_send()
        all_stats.wait_send()


def solution(mesh):
    def local_score(hidden, ln_scale, w_head, targets, valid_mask):
        b, l, d_local = hidden.shape
        v_local = w_head.shape[1]
        rows, chunk, block, carried = b * l, 256, 224, 2
        blocks = (block,) * (v_local // block) + ((v_local % block,) if v_local % block else ())
        part = 2048
        w_parts = tuple((lo, min(part, v_local - lo)) for lo in range(0, v_local, part))
        n_chunks = rows // chunk
        once_rows = (d_local * 5 // 6 // 16 * 16, d_local // 4 // 16 * 16) + (d_local // 3 // 16 * 16,) * (n_chunks - 2)
        any_spec = pl.BlockSpec(memory_space=pl.ANY)
        f32 = jnp.float32
        dma = pltpu.SemaphoreType.DMA
        token = pl.pallas_call(
            functools.partial(head_kernel, (d_local, v_local, rows, chunk, blocks, carried, w_parts, once_rows)),
            out_shape=jax.ShapeDtypeStruct((b, l), f32),
            in_specs=[any_spec] * 4,
            out_specs=pl.BlockSpec(memory_space=pltpu.VMEM),
            scratch_shapes=[
                pltpu.VMEM((v_local, 4 * d_local), jnp.bfloat16),
                pltpu.VMEM((n_chunks, 4 * d_local, chunk), jnp.bfloat16),
                pltpu.VMEM((4, 1, d_local), f32),
                pltpu.VMEM((b, l), jnp.int32),
                pltpu.VMEM((4 * d_local, LANES), f32),
                pltpu.VMEM((4 * d_local, chunk), jnp.bfloat16),
                pltpu.VMEM((2 + carried, block, chunk), f32),
                pltpu.VMEM((n_chunks + 1, 8, LANES), f32),
                pltpu.VMEM((n_chunks, 3, 8, LANES), f32),
                dma, dma, dma((2,)),
                dma, dma, dma((n_chunks,)), dma((n_chunks,)),
                dma, dma, dma, dma((2,)),
            ],
            compiler_params=pltpu.CompilerParams(
                collective_id=0,
                has_side_effects=True,
                vmem_limit_bytes=40 * 1024 * 1024,
            ),
        )(*[
            pltpu.with_memory_space_constraint(x, pltpu.HBM)
            for x in (hidden.transpose(0, 2, 1), ln_scale.reshape(1, d_local), w_head.T, targets)
        ])
        token_logp = valid_mask.astype(f32) * token
        return token_logp, jnp.sum(token_logp, axis=1)

    return jax.shard_map(
        local_score,
        mesh=mesh,
        in_specs=(P("dp", None, "tp"), P("tp"), P(None, "tp"), P("dp", None), P("dp", None)),
        out_specs=(P("dp", None), P("dp")),
        check_vma=False,
    )
```

```python
import functools

import jax
import jax.numpy as jnp
from jax import lax
from jax.experimental import pallas as pl
from jax.experimental.pallas import tpu as pltpu
from jax.sharding import PartitionSpec as P

NORM_EPS = 1e-6
LOG2E = 1.4426950408889634
MESH = pl.DeviceIdType.MESH
LANES = 128


def head_kernel(
    cfg, h_ref, g_ref, w_ref, tgt_ref, out_ref,
    wbuf, hrx, grx, tbuf, gcol, xbuf, zbuf, stx, srx,
    w_sem, own_sem, small_sem, hsend, precv, orecv, arecv, gsend, grecv, ssend, srecv,
):
    d_local, v_local, rows, chunk, blocks, carried, w_parts, once_rows = cfg
    n_chunks = rows // chunk
    d_full = 4 * d_local
    per_seq = h_ref.shape[2]
    per_chunk = per_seq // chunk
    starts = [sum(blocks[:j]) for j in range(len(blocks))]
    n_blocks = len(blocks)
    held = n_blocks - carried

    me = lax.axis_index("tp")
    peer = me + 1 - 2 * lax.rem(me, 2)
    cross = lax.rem(me + 2, 4)
    diag = lax.rem(peer + 2, 4)
    others = (peer, cross, diag)

    def piece(owner, k):
        return hrx.at[k, pl.ds(pl.multiple_of(owner * d_local, d_local), d_local)]

    own_rows = hrx.at[:, pl.ds(pl.multiple_of(me * d_local, d_local), d_local)]

    own = [
        pltpu.make_async_copy(
            h_ref.at[k // per_chunk, :, pl.ds((k % per_chunk) * chunk, chunk)], piece(me, k), own_sem
        )
        for k in range(n_chunks)
    ]
    own_g = pltpu.make_async_copy(g_ref, grx.at[me], small_sem.at[0])
    own_t = pltpu.make_async_copy(tgt_ref, tbuf, small_sem.at[1])
    load_w = [
        pltpu.make_async_copy(w_ref.at[pl.ds(lo, size)], wbuf.at[pl.ds(lo, size)], w_sem)
        for lo, size in w_parts
    ]
    own_g.start()
    for k in range(n_chunks):
        own[k].start()
    own_t.start()

    ns = jax.named_scope
    barrier = pltpu.get_barrier_semaphore()
    for other in others:
        pl.semaphore_signal(barrier, inc=1, device_id={"tp": other}, device_id_type=MESH)
    with ns("own"):
        own_g.wait()
        pltpu.make_async_copy(own_rows, own_rows, own_sem).wait()
        own_t.wait()
        for part in load_w:
            part.start()
    with ns("barrier"):
        pl.semaphore_wait(barrier, 3)

    def remote(src, dst, send, recv, dev):
        return pltpu.make_async_remote_copy(
            src_ref=src, dst_ref=dst, send_sem=send, recv_sem=recv, device_id={"tp": dev}, device_id_type=MESH
        )

    def once(owner, k):
        return hrx.at[k, pl.ds(pl.multiple_of(owner * d_local, 16), once_rows[k])]

    def direct(owner, k):
        n = once_rows[k]
        return hrx.at[k, pl.ds(pl.multiple_of(owner * d_local + n, 16), d_local - n)]

    def once_copy(k):
        return remote(once(me, k), once(me, k), hsend, orecv.at[k], diag)

    def forward_copy(k):
        return remote(once(diag, k), once(diag, k), hsend, arecv.at[k], peer)

    def cross_copy(k):
        return remote(direct(me, k), direct(me, k), hsend, arecv.at[k], cross)

    def diag_copy(k):
        return remote(direct(me, k), direct(me, k), hsend, arecv.at[k], diag)

    def arrivals(k):
        got = hrx.at[k, pl.ds(0, 2 * d_local - once_rows[k])]
        return remote(got, got, hsend, arecv.at[k], peer)

    peer_copy = remote(own_rows, own_rows, hsend, precv, peer)
    all_sent = remote(hrx.at[pl.ds(0, 3)], hrx.at[pl.ds(0, 3)], hsend, precv, peer)

    def gain_copy(n):
        return remote(grx.at[me], grx.at[me], gsend, grecv, others[n])

    all_gains = remote(grx.at[pl.ds(0, 3)], grx.at[pl.ds(0, 3)], gsend, grecv, peer)
    early = n_chunks - 1

    def stat_copy(n, k, sem):
        return remote(stx.at[k], srx.at[k, n], ssend, srecv.at[sem], others[n])

    early_stats = remote(srx.at[pl.ds(0, early)], srx.at[pl.ds(0, early)], ssend, srecv.at[0], peer)
    late_stats = remote(srx.at[early], srx.at[early], ssend, srecv.at[1], peer)
    all_stats = remote(srx, srx, ssend, srecv.at[1], peer)

    for n in range(3):
        gain_copy(n).start()
    once_copy(0).start()
    cross_copy(0).start()
    diag_copy(0).start()
    peer_copy.start()

    with ns("gainwait"):
        all_gains.wait_recv()
    for k in range(1, n_chunks):
        once_copy(k).start()
        cross_copy(k).start()
        diag_copy(k).start()

    for s in range(4):
        for lo in range(0, d_local, LANES):
            size = min(LANES, d_local - lo)
            row = grx[s, :, lo : lo + size]
            row = jnp.concatenate([row] * (LANES // size), axis=-1)
            gcol[s * d_local + lo : s * d_local + lo + size, :] = jnp.broadcast_to(row, (LANES, LANES)).T[0:size]

    group = 32

    def normalise(k):
        def square(i, acc):
            at = pl.ds(pl.multiple_of(i * group, group), group)
            part = hrx[k, at, :].astype(jnp.float32)
            return acc + part * part

        sq = lax.fori_loop(0, d_full // group, square, jnp.zeros((group, chunk), jnp.float32), unroll=True)
        inv = lax.rsqrt(jnp.sum(sq, axis=0, keepdims=True) / d_full + NORM_EPS)

        def scale(i, carry):
            at = pl.ds(pl.multiple_of(i * group, group), group)
            gain = gcol[at, :]
            part = hrx[k, at, :].astype(jnp.float32)
            gains = jnp.concatenate([gain] * (chunk // LANES), axis=-1)
            xbuf[at, :] = (part * inv * gains).astype(jnp.bfloat16)
            return carry

        lax.fori_loop(0, d_full // group, scale, 0, unroll=True)

    sub = lax.broadcasted_iota(jnp.int32, (8, chunk), 0)

    def slot_of(j):
        return j % 2 if j < held else 2 + j - held

    def logits(j):
        lo = starts[j]
        size = blocks[j]
        zbuf[slot_of(j), 0:size, :] = jnp.dot(wbuf[lo : lo + size, :], xbuf[...], preferred_element_type=jnp.float32)

    def epilogue(j, want, state):
        lo = starts[j]
        size = blocks[j]

        def tile(i):
            return zbuf[slot_of(j), pl.ds(pl.multiple_of(i * 8, 8), 8), :]

        top = lax.fori_loop(1, size // 8, lambda i, t: jnp.maximum(t, tile(i)), tile(0), unroll=True)
        if state is None:
            total = jnp.zeros((8, chunk), jnp.float32)
            pick = total
        else:
            old, total, pick = state
            top = jnp.maximum(top, old)
            total = total * jnp.exp2((old - top) * LOG2E)

        def add(i, carry):
            total, pick = carry
            z = tile(i)
            total = total + jnp.exp2((z - top) * LOG2E)
            pick = jnp.where(want == lo + i * 8, z, pick)
            return total, pick

        total, pick = lax.fori_loop(0, size // 8, add, (total, pick), unroll=True)
        return top, total, pick

    def finish_chunk(k, state):
        m, total, pick = state
        top = jnp.max(m, axis=0, keepdims=True)
        total = jnp.sum(total * jnp.exp2((m - top) * LOG2E), axis=0, keepdims=True)
        pick = jnp.sum(pick, axis=0, keepdims=True)
        for n, stat in enumerate((top, total, pick)):
            for q in range(chunk // LANES):
                row = n * (chunk // LANES) + q
                stx[k, row : row + 1, :] = stat[:, q * LANES : (q + 1) * LANES]

    with ns("once0"):
        once_copy(0).wait_recv()
    forward_copy(0).start()
    with ns("peer0"):
        peer_copy.wait_recv()
    with ns("fwd0"):
        arrivals(0).wait_recv()
    with ns("wwait"):
        pltpu.make_async_copy(w_ref, wbuf, w_sem).wait()

    def targets_of(k):
        row = tbuf[pl.ds(k // per_chunk, 1), pl.ds(pl.multiple_of(lax.rem(k, per_chunk) * chunk, chunk), chunk)]
        local = row - me * v_local
        local = jnp.where((local >= 0) & (local < v_local), local, jnp.int32(-(1 << 20)))
        return jnp.broadcast_to(local, (8, chunk)) - sub

    def send_stats(k, sem):
        for n in range(3):
            stat_copy(n, k, sem).start()

    def step(k, carry):
        for n in range(n_chunks):
            @pl.when(k == n)
            def _():
                if n:
                    with ns("chunkwait"):
                        arrivals(n).wait_recv()
                if n + 1 < n_chunks:
                    with ns("oncewait"):
                        once_copy(n + 1).wait_recv()
                    forward_copy(n + 1).start()

        @pl.when(k > 1)
        def _():
            send_stats(k - 2, 0)

        normalise(k)
        last_want, *last_state = carry
        want = targets_of(k)
        state = None
        for j in range(n_blocks):
            logits(j)
            if j == 0:
                for i in range(held, n_blocks):
                    last_state = epilogue(i, last_want, last_state)
                finish_chunk(lax.rem(k + n_chunks, n_chunks + 1), last_state)
            elif j <= held:
                state = epilogue(j - 1, want, state)
        if held == n_blocks:
            state = epilogue(held - 1, want, state)
        return (want, *state)

    blank = jnp.zeros((8, chunk), jnp.float32)
    for j in range(held, n_blocks):
        zbuf[slot_of(j), 0 : blocks[j], :] = jnp.zeros((blocks[j], chunk), jnp.float32)
    want, *state = lax.fori_loop(0, n_chunks, step, (jnp.full((8, chunk), -1, jnp.int32), blank, blank, blank))
    send_stats(n_chunks - 2, 0)
    with ns("last"):
        for j in range(held, n_blocks):
            state = epilogue(j, want, state)
        finish_chunk(n_chunks - 1, state)
    send_stats(n_chunks - 1, 1)

    per = chunk // LANES
    for k in range(n_chunks):
        with ns("statwait"):
            if k == 0:
                early_stats.wait_recv()
            if k == early:
                late_stats.wait_recv()
        stats = [stx[k]] + [srx[k, n] for n in range(3)]
        top = stats[0][0:per]
        for st in stats[1:]:
            top = jnp.maximum(top, st[0:per])
        total = jnp.zeros_like(top)
        pick = jnp.zeros_like(top)
        for st in stats:
            total = total + st[per : 2 * per] * jnp.exp2((st[0:per] - top) * LOG2E)
            pick = pick + st[2 * per : 3 * per]
        logp = pick - (top + jnp.log(total))
        seq, pos = divmod(k * chunk, per_seq)
        for q in range(per):
            out_ref[seq : seq + 1, pos + q * LANES : pos + (q + 1) * LANES] = logp[q : q + 1]

    with ns("sendwait"):
        all_sent.wait_send()
        all_gains.wait_send()
        all_stats.wait_send()


def solution(mesh):
    def local_score(hidden, ln_scale, w_head, targets, valid_mask):
        b, l, d_local = hidden.shape
        v_local = w_head.shape[1]
        rows, chunk, block, carried = b * l, 256, 224, 2
        blocks = (block,) * (v_local // block) + ((v_local % block,) if v_local % block else ())
        part = 2048
        w_parts = tuple((lo, min(part, v_local - lo)) for lo in range(0, v_local, part))
        n_chunks = rows // chunk
        once_rows = (d_local * 11 // 12 // 16 * 16, d_local // 3 // 16 * 16) + (d_local // 3 // 16 * 16,) * (n_chunks - 2)
        any_spec = pl.BlockSpec(memory_space=pl.ANY)
        f32 = jnp.float32
        dma = pltpu.SemaphoreType.DMA
        token = pl.pallas_call(
            functools.partial(head_kernel, (d_local, v_local, rows, chunk, blocks, carried, w_parts, once_rows)),
            out_shape=jax.ShapeDtypeStruct((b, l), f32),
            in_specs=[any_spec] * 4,
            out_specs=pl.BlockSpec(memory_space=pltpu.VMEM),
            scratch_shapes=[
                pltpu.VMEM((v_local, 4 * d_local), jnp.bfloat16),
                pltpu.VMEM((n_chunks, 4 * d_local, chunk), jnp.bfloat16),
                pltpu.VMEM((4, 1, d_local), f32),
                pltpu.VMEM((b, l), jnp.int32),
                pltpu.VMEM((4 * d_local, LANES), f32),
                pltpu.VMEM((4 * d_local, chunk), jnp.bfloat16),
                pltpu.VMEM((2 + carried, block, chunk), f32),
                pltpu.VMEM((n_chunks + 1, 8, LANES), f32),
                pltpu.VMEM((n_chunks, 3, 8, LANES), f32),
                dma, dma, dma((2,)),
                dma, dma, dma((n_chunks,)), dma((n_chunks,)),
                dma, dma, dma, dma((2,)),
            ],
            compiler_params=pltpu.CompilerParams(
                collective_id=0,
                has_side_effects=True,
                vmem_limit_bytes=40 * 1024 * 1024,
            ),
        )(*[
            pltpu.with_memory_space_constraint(x, pltpu.HBM)
            for x in (hidden.transpose(0, 2, 1), ln_scale.reshape(1, d_local), w_head.T, targets)
        ])
        token_logp = valid_mask.astype(f32) * token
        return token_logp, jnp.sum(token_logp, axis=1)

    return jax.shard_map(
        local_score,
        mesh=mesh,
        in_specs=(P("dp", None, "tp"), P("tp"), P(None, "tp"), P("dp", None), P("dp", None)),
        out_specs=(P("dp", None), P("dp")),
        check_vma=False,
    )
```

```python
import functools

import jax
import jax.numpy as jnp
from jax import lax
from jax.experimental import pallas as pl
from jax.experimental.pallas import tpu as pltpu
from jax.sharding import PartitionSpec as P

NORM_EPS = 1e-6
LOG2E = 1.4426950408889634
MESH = pl.DeviceIdType.MESH
LANES = 128


def head_kernel(
    cfg, h_ref, g_ref, w_ref, tgt_ref, out_ref,
    wbuf, hrx, grx, tbuf, gcol, xbuf, zbuf, stx, srx,
    w_sem, own_sem, small_sem, hsend, precv, orecv, arecv, gsend, grecv, ssend, srecv,
):
    d_local, v_local, rows, chunk, blocks, carried, w_parts, once_rows = cfg
    n_chunks = rows // chunk
    d_full = 4 * d_local
    per_seq = h_ref.shape[2]
    per_chunk = per_seq // chunk
    starts = [sum(blocks[:j]) for j in range(len(blocks))]
    n_blocks = len(blocks)
    held = n_blocks - carried

    me = lax.axis_index("tp")
    peer = me + 1 - 2 * lax.rem(me, 2)
    cross = lax.rem(me + 2, 4)
    diag = lax.rem(peer + 2, 4)
    others = (peer, cross, diag)

    def piece(owner, k):
        return hrx.at[k, pl.ds(pl.multiple_of(owner * d_local, d_local), d_local)]

    own_rows = hrx.at[:, pl.ds(pl.multiple_of(me * d_local, d_local), d_local)]

    own = [
        pltpu.make_async_copy(
            h_ref.at[k // per_chunk, :, pl.ds((k % per_chunk) * chunk, chunk)], piece(me, k), own_sem.at[min(k, 1)]
        )
        for k in range(n_chunks)
    ]
    own_g = pltpu.make_async_copy(g_ref, grx.at[me], small_sem.at[0])
    own_t = pltpu.make_async_copy(tgt_ref, tbuf, small_sem.at[1])
    load_w = [
        pltpu.make_async_copy(w_ref.at[pl.ds(lo, size)], wbuf.at[pl.ds(lo, size)], w_sem)
        for lo, size in w_parts
    ]
    own_g.start()
    for k in range(n_chunks):
        own[k].start()
    own_t.start()

    ns = jax.named_scope
    barrier = pltpu.get_barrier_semaphore()
    for other in others:
        pl.semaphore_signal(barrier, inc=1, device_id={"tp": other}, device_id_type=MESH)
    with ns("own"):
        own_g.wait()
        own[0].wait()
    with ns("barrier"):
        pl.semaphore_wait(barrier, 3)

    def remote(src, dst, send, recv, dev):
        return pltpu.make_async_remote_copy(
            src_ref=src, dst_ref=dst, send_sem=send, recv_sem=recv, device_id={"tp": dev}, device_id_type=MESH
        )

    def once(owner, k):
        return hrx.at[k, pl.ds(pl.multiple_of(owner * d_local, 16), once_rows[k])]

    def direct(owner, k):
        n = once_rows[k]
        return hrx.at[k, pl.ds(pl.multiple_of(owner * d_local + n, 16), d_local - n)]

    def once_copy(k):
        return remote(once(me, k), once(me, k), hsend, orecv.at[k], diag)

    def forward_copy(k):
        return remote(once(diag, k), once(diag, k), hsend, arecv.at[k], peer)

    def cross_copy(k):
        return remote(direct(me, k), direct(me, k), hsend, arecv.at[k], cross)

    def diag_copy(k):
        return remote(direct(me, k), direct(me, k), hsend, arecv.at[k], diag)

    def arrivals(k):
        got = hrx.at[k, pl.ds(0, 2 * d_local - once_rows[k])]
        return remote(got, got, hsend, arecv.at[k], peer)

    peer_copy = remote(own_rows, own_rows, hsend, precv, peer)
    all_sent = remote(hrx.at[pl.ds(0, 3)], hrx.at[pl.ds(0, 3)], hsend, precv, peer)

    def gain_copy(n):
        return remote(grx.at[me], grx.at[me], gsend, grecv, others[n])

    all_gains = remote(grx.at[pl.ds(0, 3)], grx.at[pl.ds(0, 3)], gsend, grecv, peer)
    early = n_chunks - 1

    def stat_copy(n, k, sem):
        return remote(stx.at[k], srx.at[k, n], ssend, srecv.at[sem], others[n])

    early_stats = remote(srx.at[pl.ds(0, early)], srx.at[pl.ds(0, early)], ssend, srecv.at[0], peer)
    late_stats = remote(srx.at[early], srx.at[early], ssend, srecv.at[1], peer)
    all_stats = remote(srx, srx, ssend, srecv.at[1], peer)

    for n in range(3):
        gain_copy(n).start()
    once_copy(0).start()
    cross_copy(0).start()
    diag_copy(0).start()
    later_rows = hrx.at[pl.ds(1, n_chunks - 1), pl.ds(pl.multiple_of(me * d_local, d_local), d_local)]
    pltpu.make_async_copy(later_rows, later_rows, own_sem.at[1]).wait()
    peer_copy.start()
    for part in load_w:
        part.start()
    own_t.wait()

    with ns("gainwait"):
        all_gains.wait_recv()
    for k in range(1, n_chunks):
        once_copy(k).start()
        cross_copy(k).start()
        diag_copy(k).start()

    for s in range(4):
        for lo in range(0, d_local, LANES):
            size = min(LANES, d_local - lo)
            row = grx[s, :, lo : lo + size]
            row = jnp.concatenate([row] * (LANES // size), axis=-1)
            gcol[s * d_local + lo : s * d_local + lo + size, :] = jnp.broadcast_to(row, (LANES, LANES)).T[0:size]

    group = 32

    def normalise(k):
        def square(i, acc):
            at = pl.ds(pl.multiple_of(i * group, group), group)
            part = hrx[k, at, :].astype(jnp.float32)
            return acc + part * part

        sq = lax.fori_loop(0, d_full // group, square, jnp.zeros((group, chunk), jnp.float32), unroll=True)
        inv = lax.rsqrt(jnp.sum(sq, axis=0, keepdims=True) / d_full + NORM_EPS)

        def scale(i, carry):
            at = pl.ds(pl.multiple_of(i * group, group), group)
            gain = gcol[at, :]
            part = hrx[k, at, :].astype(jnp.float32)
            gains = jnp.concatenate([gain] * (chunk // LANES), axis=-1)
            xbuf[at, :] = (part * inv * gains).astype(jnp.bfloat16)
            return carry

        lax.fori_loop(0, d_full // group, scale, 0, unroll=True)

    sub = lax.broadcasted_iota(jnp.int32, (8, chunk), 0)

    def slot_of(j):
        return j % 2 if j < held else 2 + j - held

    def logits(j):
        lo = starts[j]
        size = blocks[j]
        zbuf[slot_of(j), 0:size, :] = jnp.dot(wbuf[lo : lo + size, :], xbuf[...], preferred_element_type=jnp.float32)

    def epilogue(j, want, state):
        lo = starts[j]
        size = blocks[j]

        def tile(i):
            return zbuf[slot_of(j), pl.ds(pl.multiple_of(i * 8, 8), 8), :]

        top = lax.fori_loop(1, size // 8, lambda i, t: jnp.maximum(t, tile(i)), tile(0), unroll=True)
        if state is None:
            total = jnp.zeros((8, chunk), jnp.float32)
            pick = total
        else:
            old, total, pick = state
            top = jnp.maximum(top, old)
            total = total * jnp.exp2((old - top) * LOG2E)

        def add(i, carry):
            total, pick = carry
            z = tile(i)
            total = total + jnp.exp2((z - top) * LOG2E)
            pick = jnp.where(want == lo + i * 8, z, pick)
            return total, pick

        total, pick = lax.fori_loop(0, size // 8, add, (total, pick), unroll=True)
        return top, total, pick

    def finish_chunk(k, state):
        m, total, pick = state
        top = jnp.max(m, axis=0, keepdims=True)
        total = jnp.sum(total * jnp.exp2((m - top) * LOG2E), axis=0, keepdims=True)
        pick = jnp.sum(pick, axis=0, keepdims=True)
        for n, stat in enumerate((top, total, pick)):
            for q in range(chunk // LANES):
                row = n * (chunk // LANES) + q
                stx[k, row : row + 1, :] = stat[:, q * LANES : (q + 1) * LANES]

    with ns("once0"):
        once_copy(0).wait_recv()
    forward_copy(0).start()
    with ns("peer0"):
        peer_copy.wait_recv()
    with ns("fwd0"):
        arrivals(0).wait_recv()
    with ns("wwait"):
        pltpu.make_async_copy(w_ref, wbuf, w_sem).wait()

    def targets_of(k):
        row = tbuf[pl.ds(k // per_chunk, 1), pl.ds(pl.multiple_of(lax.rem(k, per_chunk) * chunk, chunk), chunk)]
        local = row - me * v_local
        local = jnp.where((local >= 0) & (local < v_local), local, jnp.int32(-(1 << 20)))
        return jnp.broadcast_to(local, (8, chunk)) - sub

    def send_stats(k, sem):
        for n in range(3):
            stat_copy(n, k, sem).start()

    def step(k, carry):
        for n in range(n_chunks):
            @pl.when(k == n)
            def _():
                if n:
                    with ns("chunkwait"):
                        arrivals(n).wait_recv()
                if n + 1 < n_chunks:
                    with ns("oncewait"):
                        once_copy(n + 1).wait_recv()
                    forward_copy(n + 1).start()

        @pl.when(k > 1)
        def _():
            send_stats(k - 2, 0)

        normalise(k)
        last_want, *last_state = carry
        want = targets_of(k)
        state = None
        for j in range(n_blocks):
            logits(j)
            if j == 0:
                for i in range(held, n_blocks):
                    last_state = epilogue(i, last_want, last_state)
                finish_chunk(lax.rem(k + n_chunks, n_chunks + 1), last_state)
            elif j <= held:
                state = epilogue(j - 1, want, state)
        if held == n_blocks:
            state = epilogue(held - 1, want, state)
        return (want, *state)

    blank = jnp.zeros((8, chunk), jnp.float32)
    for j in range(held, n_blocks):
        zbuf[slot_of(j), 0 : blocks[j], :] = jnp.zeros((blocks[j], chunk), jnp.float32)
    want, *state = lax.fori_loop(0, n_chunks, step, (jnp.full((8, chunk), -1, jnp.int32), blank, blank, blank))
    send_stats(n_chunks - 2, 0)
    with ns("last"):
        for j in range(held, n_blocks):
            state = epilogue(j, want, state)
        finish_chunk(n_chunks - 1, state)
    send_stats(n_chunks - 1, 1)

    per = chunk // LANES
    for k in range(n_chunks):
        with ns("statwait"):
            if k == 0:
                early_stats.wait_recv()
            if k == early:
                late_stats.wait_recv()
        stats = [stx[k]] + [srx[k, n] for n in range(3)]
        top = stats[0][0:per]
        for st in stats[1:]:
            top = jnp.maximum(top, st[0:per])
        total = jnp.zeros_like(top)
        pick = jnp.zeros_like(top)
        for st in stats:
            total = total + st[per : 2 * per] * jnp.exp2((st[0:per] - top) * LOG2E)
            pick = pick + st[2 * per : 3 * per]
        logp = pick - (top + jnp.log(total))
        seq, pos = divmod(k * chunk, per_seq)
        for q in range(per):
            out_ref[seq : seq + 1, pos + q * LANES : pos + (q + 1) * LANES] = logp[q : q + 1]

    with ns("sendwait"):
        all_sent.wait_send()
        all_gains.wait_send()
        all_stats.wait_send()


def solution(mesh):
    def local_score(hidden, ln_scale, w_head, targets, valid_mask):
        b, l, d_local = hidden.shape
        v_local = w_head.shape[1]
        rows, chunk, block, carried = b * l, 256, 224, 2
        blocks = (block,) * (v_local // block) + ((v_local % block,) if v_local % block else ())
        part = 2048
        w_parts = tuple((lo, min(part, v_local - lo)) for lo in range(0, v_local, part))
        n_chunks = rows // chunk
        once_rows = (d_local * 11 // 12 // 16 * 16, d_local // 3 // 16 * 16) + (d_local // 3 // 16 * 16,) * (n_chunks - 2)
        any_spec = pl.BlockSpec(memory_space=pl.ANY)
        f32 = jnp.float32
        dma = pltpu.SemaphoreType.DMA
        token = pl.pallas_call(
            functools.partial(head_kernel, (d_local, v_local, rows, chunk, blocks, carried, w_parts, once_rows)),
            out_shape=jax.ShapeDtypeStruct((b, l), f32),
            in_specs=[any_spec] * 4,
            out_specs=pl.BlockSpec(memory_space=pltpu.VMEM),
            scratch_shapes=[
                pltpu.VMEM((v_local, 4 * d_local), jnp.bfloat16),
                pltpu.VMEM((n_chunks, 4 * d_local, chunk), jnp.bfloat16),
                pltpu.VMEM((4, 1, d_local), f32),
                pltpu.VMEM((b, l), jnp.int32),
                pltpu.VMEM((4 * d_local, LANES), f32),
                pltpu.VMEM((4 * d_local, chunk), jnp.bfloat16),
                pltpu.VMEM((2 + carried, block, chunk), f32),
                pltpu.VMEM((n_chunks + 1, 8, LANES), f32),
                pltpu.VMEM((n_chunks, 3, 8, LANES), f32),
                dma, dma((2,)), dma((2,)),
                dma, dma, dma((n_chunks,)), dma((n_chunks,)),
                dma, dma, dma, dma((2,)),
            ],
            compiler_params=pltpu.CompilerParams(
                collective_id=0,
                has_side_effects=True,
                vmem_limit_bytes=40 * 1024 * 1024,
            ),
        )(*[
            pltpu.with_memory_space_constraint(x, pltpu.HBM)
            for x in (hidden.transpose(0, 2, 1), ln_scale.reshape(1, d_local), w_head.T, targets)
        ])
        token_logp = valid_mask.astype(f32) * token
        return token_logp, jnp.sum(token_logp, axis=1)

    return jax.shard_map(
        local_score,
        mesh=mesh,
        in_specs=(P("dp", None, "tp"), P("tp"), P(None, "tp"), P("dp", None), P("dp", None)),
        out_specs=(P("dp", None), P("dp")),
        check_vma=False,
    )
```

```python
import functools

import jax
import jax.numpy as jnp
from jax import lax
from jax.experimental import pallas as pl
from jax.experimental.pallas import tpu as pltpu
from jax.sharding import PartitionSpec as P

NORM_EPS = 1e-6
LOG2E = 1.4426950408889634
MESH = pl.DeviceIdType.MESH
LANES = 128


def head_kernel(
    cfg, h_ref, g_ref, w_ref, tgt_ref, out_ref,
    wbuf, hrx, grx, tbuf, gcol, xbuf, zbuf, stx, srx,
    w_sem, own_sem, small_sem, hsend, precv, orecv, arecv, gsend, grecv, ssend, srecv,
):
    d_local, v_local, rows, chunk, blocks, carried, w_parts, once_rows = cfg
    n_chunks = rows // chunk
    d_full = 4 * d_local
    per_seq = h_ref.shape[2]
    per_chunk = per_seq // chunk
    starts = [sum(blocks[:j]) for j in range(len(blocks))]
    n_blocks = len(blocks)
    held = n_blocks - carried

    me = lax.axis_index("tp")
    peer = me + 1 - 2 * lax.rem(me, 2)
    cross = lax.rem(me + 2, 4)
    diag = lax.rem(peer + 2, 4)
    others = (peer, cross, diag)

    def piece(owner, k):
        return hrx.at[k, pl.ds(pl.multiple_of(owner * d_local, d_local), d_local)]

    own_rows = hrx.at[:, pl.ds(pl.multiple_of(me * d_local, d_local), d_local)]

    own = [
        pltpu.make_async_copy(
            h_ref.at[k // per_chunk, :, pl.ds((k % per_chunk) * chunk, chunk)], piece(me, k), own_sem.at[min(k, 1)]
        )
        for k in range(n_chunks)
    ]
    own_g = pltpu.make_async_copy(g_ref, grx.at[me], small_sem.at[0])
    own_t = pltpu.make_async_copy(tgt_ref, tbuf, small_sem.at[1])
    load_w = [
        pltpu.make_async_copy(w_ref.at[pl.ds(lo, size)], wbuf.at[pl.ds(lo, size)], w_sem)
        for lo, size in w_parts
    ]
    own_g.start()
    for k in range(n_chunks):
        own[k].start()
    own_t.start()

    ns = jax.named_scope
    barrier = pltpu.get_barrier_semaphore()
    for other in others:
        pl.semaphore_signal(barrier, inc=1, device_id={"tp": other}, device_id_type=MESH)
    with ns("own"):
        own_g.wait()
        own[0].wait()
    with ns("barrier"):
        pl.semaphore_wait(barrier, 3)

    def remote(src, dst, send, recv, dev):
        return pltpu.make_async_remote_copy(
            src_ref=src, dst_ref=dst, send_sem=send, recv_sem=recv, device_id={"tp": dev}, device_id_type=MESH
        )

    def once(owner, k):
        return hrx.at[k, pl.ds(pl.multiple_of(owner * d_local, 16), once_rows[k])]

    def direct(owner, k):
        n = once_rows[k]
        return hrx.at[k, pl.ds(pl.multiple_of(owner * d_local + n, 16), d_local - n)]

    def once_copy(k):
        return remote(once(me, k), once(me, k), hsend, orecv.at[k], diag)

    def forward_copy(k):
        return remote(once(diag, k), once(diag, k), hsend, arecv.at[k], peer)

    def cross_copy(k):
        return remote(direct(me, k), direct(me, k), hsend, arecv.at[k], cross)

    def diag_copy(k):
        return remote(direct(me, k), direct(me, k), hsend, arecv.at[k], diag)

    def arrivals(k):
        got = hrx.at[k, pl.ds(0, 2 * d_local - once_rows[k])]
        return remote(got, got, hsend, arecv.at[k], peer)

    peer_copy = remote(own_rows, own_rows, hsend, precv, peer)
    all_sent = remote(hrx.at[pl.ds(0, 3)], hrx.at[pl.ds(0, 3)], hsend, precv, peer)

    def gain_copy(n):
        return remote(grx.at[me], grx.at[me], gsend, grecv, others[n])

    all_gains = remote(grx.at[pl.ds(0, 3)], grx.at[pl.ds(0, 3)], gsend, grecv, peer)
    early = n_chunks - 1

    def stat_copy(n, k, sem):
        return remote(stx.at[k], srx.at[k, n], ssend, srecv.at[sem], others[n])

    early_stats = remote(srx.at[pl.ds(0, early)], srx.at[pl.ds(0, early)], ssend, srecv.at[0], peer)
    late_stats = remote(srx.at[early], srx.at[early], ssend, srecv.at[1], peer)
    all_stats = remote(srx, srx, ssend, srecv.at[1], peer)

    for n in range(3):
        gain_copy(n).start()
    once_copy(0).start()
    cross_copy(0).start()
    diag_copy(0).start()
    later_rows = hrx.at[pl.ds(1, n_chunks - 1), pl.ds(pl.multiple_of(me * d_local, d_local), d_local)]
    pltpu.make_async_copy(later_rows, later_rows, own_sem.at[1]).wait()
    peer_copy.start()
    for part in load_w:
        part.start()
    own_t.wait()

    with ns("gainwait"):
        all_gains.wait_recv()
    for k in range(1, n_chunks):
        once_copy(k).start()
        cross_copy(k).start()
        diag_copy(k).start()

    for s in range(4):
        for lo in range(0, d_local, LANES):
            size = min(LANES, d_local - lo)
            row = grx[s, :, lo : lo + size]
            row = jnp.concatenate([row] * (LANES // size), axis=-1)
            gcol[s * d_local + lo : s * d_local + lo + size, :] = jnp.broadcast_to(row, (LANES, LANES)).T[0:size]

    group = 32

    def normalise(k):
        def square(i, acc):
            at = pl.ds(pl.multiple_of(i * group, group), group)
            part = hrx[k, at, :].astype(jnp.float32)
            return acc + part * part

        sq = lax.fori_loop(0, d_full // group, square, jnp.zeros((group, chunk), jnp.float32), unroll=True)
        inv = lax.rsqrt(jnp.sum(sq, axis=0, keepdims=True) / d_full + NORM_EPS)

        def scale(i, carry):
            at = pl.ds(pl.multiple_of(i * group, group), group)
            gain = gcol[at, :]
            part = hrx[k, at, :].astype(jnp.float32)
            gains = jnp.concatenate([gain] * (chunk // LANES), axis=-1)
            xbuf[at, :] = (part * inv * gains).astype(jnp.bfloat16)
            return carry

        lax.fori_loop(0, d_full // group, scale, 0, unroll=True)

    sub = lax.broadcasted_iota(jnp.int32, (8, chunk), 0)

    def slot_of(j):
        return j % 2 if j < held else 2 + j - held

    def logits(j):
        lo = starts[j]
        size = blocks[j]
        zbuf[slot_of(j), 0:size, :] = jnp.dot(wbuf[lo : lo + size, :], xbuf[...], preferred_element_type=jnp.float32)

    def epilogue(j, want, state):
        lo = starts[j]
        size = blocks[j]

        def tile(i):
            return zbuf[slot_of(j), pl.ds(pl.multiple_of(i * 8, 8), 8), :]

        top = lax.fori_loop(1, size // 8, lambda i, t: jnp.maximum(t, tile(i)), tile(0), unroll=True)
        if state is None:
            total = jnp.zeros((8, chunk), jnp.float32)
            pick = total
        else:
            old, total, pick = state
            top = jnp.maximum(top, old)
            total = total * jnp.exp2((old - top) * LOG2E)

        def add(i, carry):
            total, pick = carry
            z = tile(i)
            total = total + jnp.exp2((z - top) * LOG2E)
            pick = jnp.where(want == lo + i * 8, z, pick)
            return total, pick

        total, pick = lax.fori_loop(0, size // 8, add, (total, pick), unroll=True)
        return top, total, pick

    def finish_chunk(k, state):
        m, total, pick = state
        top = jnp.max(m, axis=0, keepdims=True)
        total = jnp.sum(total * jnp.exp2((m - top) * LOG2E), axis=0, keepdims=True)
        pick = jnp.sum(pick, axis=0, keepdims=True)
        for n, stat in enumerate((top, total, pick)):
            for q in range(chunk // LANES):
                row = n * (chunk // LANES) + q
                stx[k, row : row + 1, :] = stat[:, q * LANES : (q + 1) * LANES]

    with ns("once0"):
        once_copy(0).wait_recv()
    forward_copy(0).start()
    with ns("peer0"):
        peer_copy.wait_recv()
    with ns("fwd0"):
        arrivals(0).wait_recv()
    with ns("wwait"):
        pltpu.make_async_copy(w_ref, wbuf, w_sem).wait()

    def targets_of(k):
        row = tbuf[pl.ds(k // per_chunk, 1), pl.ds(pl.multiple_of(lax.rem(k, per_chunk) * chunk, chunk), chunk)]
        local = row - me * v_local
        local = jnp.where((local >= 0) & (local < v_local), local, jnp.int32(-(1 << 20)))
        return jnp.broadcast_to(local, (8, chunk)) - sub

    def send_stats(k, sem):
        for n in range(3):
            stat_copy(n, k, sem).start()

    def step(k, carry):
        for n in range(n_chunks):
            @pl.when(k == n)
            def _():
                if n:
                    with ns("chunkwait"):
                        arrivals(n).wait_recv()
                if n + 1 < n_chunks:
                    with ns("oncewait"):
                        once_copy(n + 1).wait_recv()
                    forward_copy(n + 1).start()

        @pl.when(k > 1)
        def _():
            send_stats(k - 2, 0)

        normalise(k)
        last_want, *last_state = carry
        want = targets_of(k)
        state = None
        for j in range(n_blocks):
            logits(j)
            if j == 0:
                for i in range(held, n_blocks):
                    last_state = epilogue(i, last_want, last_state)
                finish_chunk(lax.rem(k + n_chunks, n_chunks + 1), last_state)
            elif j <= held:
                state = epilogue(j - 1, want, state)
        if held == n_blocks:
            state = epilogue(held - 1, want, state)
        return (want, *state)

    blank = jnp.zeros((8, chunk), jnp.float32)
    for j in range(held, n_blocks):
        zbuf[slot_of(j), 0 : blocks[j], :] = jnp.zeros((blocks[j], chunk), jnp.float32)
    want, *state = lax.fori_loop(0, n_chunks, step, (jnp.full((8, chunk), -1, jnp.int32), blank, blank, blank))
    send_stats(n_chunks - 2, 0)
    with ns("last"):
        for j in range(held, n_blocks):
            state = epilogue(j, want, state)
        finish_chunk(n_chunks - 1, state)
    send_stats(n_chunks - 1, 1)

    per = chunk // LANES
    for k in range(n_chunks):
        with ns("statwait"):
            if k == 0:
                early_stats.wait_recv()
            if k == early:
                late_stats.wait_recv()
        stats = [stx[k]] + [srx[k, n] for n in range(3)]
        top = stats[0][0:per]
        for st in stats[1:]:
            top = jnp.maximum(top, st[0:per])
        total = jnp.zeros_like(top)
        pick = jnp.zeros_like(top)
        for st in stats:
            total = total + st[per : 2 * per] * jnp.exp2((st[0:per] - top) * LOG2E)
            pick = pick + st[2 * per : 3 * per]
        logp = pick - (top + jnp.log(total))
        seq, pos = divmod(k * chunk, per_seq)
        for q in range(per):
            out_ref[seq : seq + 1, pos + q * LANES : pos + (q + 1) * LANES] = logp[q : q + 1]

    with ns("sendwait"):
        all_sent.wait_send()
        all_gains.wait_send()
        all_stats.wait_send()


def solution(mesh):
    def local_score(hidden, ln_scale, w_head, targets, valid_mask):
        b, l, d_local = hidden.shape
        v_local = w_head.shape[1]
        rows, chunk, block, carried = b * l, 256, 192, 3
        blocks = (block,) * (v_local // block) + ((v_local % block,) if v_local % block else ())
        part = 2048
        w_parts = tuple((lo, min(part, v_local - lo)) for lo in range(0, v_local, part))
        n_chunks = rows // chunk
        once_rows = (d_local * 11 // 12 // 16 * 16, d_local // 3 // 16 * 16) + (d_local // 3 // 16 * 16,) * (n_chunks - 2)
        any_spec = pl.BlockSpec(memory_space=pl.ANY)
        f32 = jnp.float32
        dma = pltpu.SemaphoreType.DMA
        token = pl.pallas_call(
            functools.partial(head_kernel, (d_local, v_local, rows, chunk, blocks, carried, w_parts, once_rows)),
            out_shape=jax.ShapeDtypeStruct((b, l), f32),
            in_specs=[any_spec] * 4,
            out_specs=pl.BlockSpec(memory_space=pltpu.VMEM),
            scratch_shapes=[
                pltpu.VMEM((v_local, 4 * d_local), jnp.bfloat16),
                pltpu.VMEM((n_chunks, 4 * d_local, chunk), jnp.bfloat16),
                pltpu.VMEM((4, 1, d_local), f32),
                pltpu.VMEM((b, l), jnp.int32),
                pltpu.VMEM((4 * d_local, LANES), f32),
                pltpu.VMEM((4 * d_local, chunk), jnp.bfloat16),
                pltpu.VMEM((2 + carried, block, chunk), f32),
                pltpu.VMEM((n_chunks + 1, 8, LANES), f32),
                pltpu.VMEM((n_chunks, 3, 8, LANES), f32),
                dma, dma((2,)), dma((2,)),
                dma, dma, dma((n_chunks,)), dma((n_chunks,)),
                dma, dma, dma, dma((2,)),
            ],
            compiler_params=pltpu.CompilerParams(
                collective_id=0,
                has_side_effects=True,
                vmem_limit_bytes=40 * 1024 * 1024,
            ),
        )(*[
            pltpu.with_memory_space_constraint(x, pltpu.HBM)
            for x in (hidden.transpose(0, 2, 1), ln_scale.reshape(1, d_local), w_head.T, targets)
        ])
        token_logp = valid_mask.astype(f32) * token
        return token_logp, jnp.sum(token_logp, axis=1)

    return jax.shard_map(
        local_score,
        mesh=mesh,
        in_specs=(P("dp", None, "tp"), P("tp"), P(None, "tp"), P("dp", None), P("dp", None)),
        out_specs=(P("dp", None), P("dp")),
        check_vma=False,
    )
```

```python
import functools

import jax
import jax.numpy as jnp
from jax import lax
from jax.experimental import pallas as pl
from jax.experimental.pallas import tpu as pltpu
from jax.sharding import PartitionSpec as P

NORM_EPS = 1e-6
LOG2E = 1.4426950408889634
MESH = pl.DeviceIdType.MESH
LANES = 128


def head_kernel(
    cfg, h_ref, g_ref, w_ref, tgt_ref, out_ref,
    wbuf, hrx, grx, tbuf, gcol, xbuf, zbuf, stx, srx,
    w_sem, own_sem, small_sem, hsend, precv, orecv, arecv, gsend, grecv, ssend, srecv,
):
    d_local, v_local, rows, chunk, blocks, carried, w_parts, once_rows = cfg
    n_chunks = rows // chunk
    d_full = 4 * d_local
    per_seq = h_ref.shape[2]
    per_chunk = per_seq // chunk
    starts = [sum(blocks[:j]) for j in range(len(blocks))]
    n_blocks = len(blocks)
    held = n_blocks - carried

    me = lax.axis_index("tp")
    peer = me + 1 - 2 * lax.rem(me, 2)
    cross = lax.rem(me + 2, 4)
    diag = lax.rem(peer + 2, 4)
    others = (peer, cross, diag)

    def piece(owner, k):
        return hrx.at[k, pl.ds(pl.multiple_of(owner * d_local, d_local), d_local)]

    own_rows = hrx.at[:, pl.ds(pl.multiple_of(me * d_local, d_local), d_local)]

    own = [
        pltpu.make_async_copy(
            h_ref.at[k // per_chunk, :, pl.ds((k % per_chunk) * chunk, chunk)], piece(me, k), own_sem.at[min(k, 1)]
        )
        for k in range(n_chunks)
    ]
    own_g = pltpu.make_async_copy(g_ref, grx.at[me], small_sem.at[0])
    own_t = pltpu.make_async_copy(tgt_ref, tbuf, small_sem.at[1])
    load_w = [
        pltpu.make_async_copy(w_ref.at[pl.ds(lo, size)], wbuf.at[pl.ds(lo, size)], w_sem)
        for lo, size in w_parts
    ]
    own_g.start()
    for k in range(n_chunks):
        own[k].start()
    own_t.start()

    ns = jax.named_scope
    barrier = pltpu.get_barrier_semaphore()
    for other in others:
        pl.semaphore_signal(barrier, inc=1, device_id={"tp": other}, device_id_type=MESH)
    with ns("own"):
        own_g.wait()
        own[0].wait()
        for part in load_w:
            part.start()
    with ns("barrier"):
        pl.semaphore_wait(barrier, 3)

    def remote(src, dst, send, recv, dev):
        return pltpu.make_async_remote_copy(
            src_ref=src, dst_ref=dst, send_sem=send, recv_sem=recv, device_id={"tp": dev}, device_id_type=MESH
        )

    def once(owner, k):
        return hrx.at[k, pl.ds(pl.multiple_of(owner * d_local, 16), once_rows[k])]

    def direct(owner, k):
        n = once_rows[k]
        return hrx.at[k, pl.ds(pl.multiple_of(owner * d_local + n, 16), d_local - n)]

    def once_copy(k):
        return remote(once(me, k), once(me, k), hsend, orecv.at[k], diag)

    def forward_copy(k):
        return remote(once(diag, k), once(diag, k), hsend, arecv.at[k], peer)

    def cross_copy(k):
        return remote(direct(me, k), direct(me, k), hsend, arecv.at[k], cross)

    def diag_copy(k):
        return remote(direct(me, k), direct(me, k), hsend, arecv.at[k], diag)

    def arrivals(k):
        got = hrx.at[k, pl.ds(0, 2 * d_local - once_rows[k])]
        return remote(got, got, hsend, arecv.at[k], peer)

    peer_copy = remote(own_rows, own_rows, hsend, precv, peer)
    all_sent = remote(hrx.at[pl.ds(0, 3)], hrx.at[pl.ds(0, 3)], hsend, precv, peer)

    def gain_copy(n):
        return remote(grx.at[me], grx.at[me], gsend, grecv.at[n], others[n])

    all_gains = remote(grx.at[pl.ds(0, 3)], grx.at[pl.ds(0, 3)], gsend, grecv.at[0], peer)
    early = n_chunks - 1

    def stat_copy(n, k, sem):
        return remote(stx.at[k], srx.at[k, n], ssend, srecv.at[sem], others[n])

    early_stats = remote(srx.at[pl.ds(0, early)], srx.at[pl.ds(0, early)], ssend, srecv.at[0], peer)
    late_stats = remote(srx.at[early], srx.at[early], ssend, srecv.at[1], peer)
    all_stats = remote(srx, srx, ssend, srecv.at[1], peer)

    for n in range(3):
        gain_copy(n).start()
    once_copy(0).start()
    cross_copy(0).start()
    diag_copy(0).start()
    later_rows = hrx.at[pl.ds(1, n_chunks - 1), pl.ds(pl.multiple_of(me * d_local, d_local), d_local)]
    pltpu.make_async_copy(later_rows, later_rows, own_sem.at[1]).wait()
    peer_copy.start()
    own_t.wait()

    with ns("gainwait"):
        gain_copy(2).wait_recv()
    for k in range(1, n_chunks):
        once_copy(k).start()
        cross_copy(k).start()
        diag_copy(k).start()

    for n in range(2):
        gain_copy(n).wait_recv()
    for s in range(4):
        for lo in range(0, d_local, LANES):
            size = min(LANES, d_local - lo)
            row = grx[s, :, lo : lo + size]
            row = jnp.concatenate([row] * (LANES // size), axis=-1)
            gcol[s * d_local + lo : s * d_local + lo + size, :] = jnp.broadcast_to(row, (LANES, LANES)).T[0:size]

    group = 32

    def normalise(k):
        def square(i, acc):
            at = pl.ds(pl.multiple_of(i * group, group), group)
            part = hrx[k, at, :].astype(jnp.float32)
            return acc + part * part

        sq = lax.fori_loop(0, d_full // group, square, jnp.zeros((group, chunk), jnp.float32), unroll=True)
        inv = lax.rsqrt(jnp.sum(sq, axis=0, keepdims=True) / d_full + NORM_EPS)

        def scale(i, carry):
            at = pl.ds(pl.multiple_of(i * group, group), group)
            gain = gcol[at, :]
            part = hrx[k, at, :].astype(jnp.float32)
            gains = jnp.concatenate([gain] * (chunk // LANES), axis=-1)
            xbuf[at, :] = (part * inv * gains).astype(jnp.bfloat16)
            return carry

        lax.fori_loop(0, d_full // group, scale, 0, unroll=True)

    sub = lax.broadcasted_iota(jnp.int32, (8, chunk), 0)

    def slot_of(j):
        return j % 2 if j < held else 2 + j - held

    def logits(j):
        lo = starts[j]
        size = blocks[j]
        zbuf[slot_of(j), 0:size, :] = jnp.dot(wbuf[lo : lo + size, :], xbuf[...], preferred_element_type=jnp.float32)

    def epilogue(j, want, state):
        lo = starts[j]
        size = blocks[j]

        def tile(i):
            return zbuf[slot_of(j), pl.ds(pl.multiple_of(i * 8, 8), 8), :]

        top = lax.fori_loop(1, size // 8, lambda i, t: jnp.maximum(t, tile(i)), tile(0), unroll=True)
        if state is None:
            total = jnp.zeros((8, chunk), jnp.float32)
            pick = total
        else:
            old, total, pick = state
            top = jnp.maximum(top, old)
            total = total * jnp.exp2((old - top) * LOG2E)

        def add(i, carry):
            total, pick = carry
            z = tile(i)
            total = total + jnp.exp2((z - top) * LOG2E)
            pick = jnp.where(want == lo + i * 8, z, pick)
            return total, pick

        total, pick = lax.fori_loop(0, size // 8, add, (total, pick), unroll=True)
        return top, total, pick

    def finish_chunk(k, state):
        m, total, pick = state
        top = jnp.max(m, axis=0, keepdims=True)
        total = jnp.sum(total * jnp.exp2((m - top) * LOG2E), axis=0, keepdims=True)
        pick = jnp.sum(pick, axis=0, keepdims=True)
        for n, stat in enumerate((top, total, pick)):
            for q in range(chunk // LANES):
                row = n * (chunk // LANES) + q
                stx[k, row : row + 1, :] = stat[:, q * LANES : (q + 1) * LANES]

    with ns("once0"):
        once_copy(0).wait_recv()
    forward_copy(0).start()
    with ns("peer0"):
        peer_copy.wait_recv()
    with ns("fwd0"):
        arrivals(0).wait_recv()
    with ns("wwait"):
        pltpu.make_async_copy(w_ref, wbuf, w_sem).wait()

    def targets_of(k):
        row = tbuf[pl.ds(k // per_chunk, 1), pl.ds(pl.multiple_of(lax.rem(k, per_chunk) * chunk, chunk), chunk)]
        local = row - me * v_local
        local = jnp.where((local >= 0) & (local < v_local), local, jnp.int32(-(1 << 20)))
        return jnp.broadcast_to(local, (8, chunk)) - sub

    def send_stats(k, sem):
        for n in range(3):
            stat_copy(n, k, sem).start()

    def step(k, carry):
        for n in range(n_chunks):
            @pl.when(k == n)
            def _():
                if n:
                    with ns("chunkwait"):
                        arrivals(n).wait_recv()
                if n + 1 < n_chunks:
                    with ns("oncewait"):
                        once_copy(n + 1).wait_recv()
                    forward_copy(n + 1).start()

        @pl.when(k > 1)
        def _():
            send_stats(k - 2, 0)

        normalise(k)
        last_want, *last_state = carry
        want = targets_of(k)
        state = None
        for j in range(n_blocks):
            logits(j)
            if j == 0:
                for i in range(held, n_blocks):
                    last_state = epilogue(i, last_want, last_state)
                finish_chunk(lax.rem(k + n_chunks, n_chunks + 1), last_state)
            elif j <= held:
                state = epilogue(j - 1, want, state)
        if held == n_blocks:
            state = epilogue(held - 1, want, state)
        return (want, *state)

    blank = jnp.zeros((8, chunk), jnp.float32)
    for j in range(held, n_blocks):
        zbuf[slot_of(j), 0 : blocks[j], :] = jnp.zeros((blocks[j], chunk), jnp.float32)
    want, *state = lax.fori_loop(0, n_chunks, step, (jnp.full((8, chunk), -1, jnp.int32), blank, blank, blank))
    send_stats(n_chunks - 2, 0)
    with ns("last"):
        for j in range(held, n_blocks):
            state = epilogue(j, want, state)
        finish_chunk(n_chunks - 1, state)
    send_stats(n_chunks - 1, 1)

    per = chunk // LANES
    for k in range(n_chunks):
        with ns("statwait"):
            if k == 0:
                early_stats.wait_recv()
            if k == early:
                late_stats.wait_recv()
        stats = [stx[k]] + [srx[k, n] for n in range(3)]
        top = stats[0][0:per]
        for st in stats[1:]:
            top = jnp.maximum(top, st[0:per])
        total = jnp.zeros_like(top)
        pick = jnp.zeros_like(top)
        for st in stats:
            total = total + st[per : 2 * per] * jnp.exp2((st[0:per] - top) * LOG2E)
            pick = pick + st[2 * per : 3 * per]
        logp = pick - (top + jnp.log(total))
        seq, pos = divmod(k * chunk, per_seq)
        for q in range(per):
            out_ref[seq : seq + 1, pos + q * LANES : pos + (q + 1) * LANES] = logp[q : q + 1]

    with ns("sendwait"):
        all_sent.wait_send()
        all_gains.wait_send()
        all_stats.wait_send()


def solution(mesh):
    def local_score(hidden, ln_scale, w_head, targets, valid_mask):
        b, l, d_local = hidden.shape
        v_local = w_head.shape[1]
        rows, chunk, block, carried = b * l, 256, 192, 3
        blocks = (block,) * (v_local // block) + ((v_local % block,) if v_local % block else ())
        part = 2048
        w_parts = tuple((lo, min(part, v_local - lo)) for lo in range(0, v_local, part))
        n_chunks = rows // chunk
        once_rows = (d_local * 11 // 12 // 16 * 16, d_local // 3 // 16 * 16) + (d_local // 3 // 16 * 16,) * (n_chunks - 2)
        any_spec = pl.BlockSpec(memory_space=pl.ANY)
        f32 = jnp.float32
        dma = pltpu.SemaphoreType.DMA
        token = pl.pallas_call(
            functools.partial(head_kernel, (d_local, v_local, rows, chunk, blocks, carried, w_parts, once_rows)),
            out_shape=jax.ShapeDtypeStruct((b, l), f32),
            in_specs=[any_spec] * 4,
            out_specs=pl.BlockSpec(memory_space=pltpu.VMEM),
            scratch_shapes=[
                pltpu.VMEM((v_local, 4 * d_local), jnp.bfloat16),
                pltpu.VMEM((n_chunks, 4 * d_local, chunk), jnp.bfloat16),
                pltpu.VMEM((4, 1, d_local), f32),
                pltpu.VMEM((b, l), jnp.int32),
                pltpu.VMEM((4 * d_local, LANES), f32),
                pltpu.VMEM((4 * d_local, chunk), jnp.bfloat16),
                pltpu.VMEM((2 + carried, block, chunk), f32),
                pltpu.VMEM((n_chunks + 1, 8, LANES), f32),
                pltpu.VMEM((n_chunks, 3, 8, LANES), f32),
                dma, dma((2,)), dma((2,)),
                dma, dma, dma((n_chunks,)), dma((n_chunks,)),
                dma, dma((3,)), dma, dma((2,)),
            ],
            compiler_params=pltpu.CompilerParams(
                collective_id=0,
                has_side_effects=True,
                vmem_limit_bytes=40 * 1024 * 1024,
            ),
        )(*[
            pltpu.with_memory_space_constraint(x, pltpu.HBM)
            for x in (hidden.transpose(0, 2, 1), ln_scale.reshape(1, d_local), w_head.T, targets)
        ])
        token_logp = valid_mask.astype(f32) * token
        return token_logp, jnp.sum(token_logp, axis=1)

    return jax.shard_map(
        local_score,
        mesh=mesh,
        in_specs=(P("dp", None, "tp"), P("tp"), P(None, "tp"), P("dp", None), P("dp", None)),
        out_specs=(P("dp", None), P("dp")),
        check_vma=False,
    )
```

```python
import functools

import jax
import jax.numpy as jnp
from jax import lax
from jax.experimental import pallas as pl
from jax.experimental.pallas import tpu as pltpu
from jax.sharding import PartitionSpec as P

NORM_EPS = 1e-6
LOG2E = 1.4426950408889634
MESH = pl.DeviceIdType.MESH
LANES = 128


def head_kernel(
    cfg, h_ref, g_ref, w_ref, tgt_ref, out_ref,
    wbuf, hrx, grx, tbuf, gcol, xbuf, zbuf, stx, srx,
    w_sem, own_sem, small_sem, hsend, precv, orecv, arecv, gsend, grecv, ssend, srecv,
):
    d_local, v_local, rows, chunk, blocks, carried, w_parts, once_rows = cfg
    n_chunks = rows // chunk
    d_full = 4 * d_local
    per_seq = h_ref.shape[2]
    per_chunk = per_seq // chunk
    starts = [sum(blocks[:j]) for j in range(len(blocks))]
    n_blocks = len(blocks)
    held = n_blocks - carried

    me = lax.axis_index("tp")
    peer = me + 1 - 2 * lax.rem(me, 2)
    cross = lax.rem(me + 2, 4)
    diag = lax.rem(peer + 2, 4)
    others = (peer, cross, diag)

    def piece(owner, k):
        return hrx.at[k, pl.ds(pl.multiple_of(owner * d_local, d_local), d_local)]

    own_rows = hrx.at[:, pl.ds(pl.multiple_of(me * d_local, d_local), d_local)]

    own = [
        pltpu.make_async_copy(
            h_ref.at[k // per_chunk, :, pl.ds((k % per_chunk) * chunk, chunk)], piece(me, k), own_sem.at[min(k, 1)]
        )
        for k in range(n_chunks)
    ]
    own_g = pltpu.make_async_copy(g_ref, grx.at[me], small_sem.at[0])
    own_t = pltpu.make_async_copy(tgt_ref, tbuf, small_sem.at[1])
    load_w = [
        pltpu.make_async_copy(w_ref.at[pl.ds(lo, size)], wbuf.at[pl.ds(lo, size)], w_sem)
        for lo, size in w_parts
    ]
    own_g.start()
    for k in range(n_chunks):
        own[k].start()
    own_t.start()

    ns = jax.named_scope
    barrier = pltpu.get_barrier_semaphore()
    for other in others:
        pl.semaphore_signal(barrier, inc=1, device_id={"tp": other}, device_id_type=MESH)
    with ns("own"):
        own_g.wait()
        own[0].wait()
    with ns("barrier"):
        pl.semaphore_wait(barrier, 3)

    def remote(src, dst, send, recv, dev):
        return pltpu.make_async_remote_copy(
            src_ref=src, dst_ref=dst, send_sem=send, recv_sem=recv, device_id={"tp": dev}, device_id_type=MESH
        )

    def once(owner, k):
        return hrx.at[k, pl.ds(pl.multiple_of(owner * d_local, 16), once_rows[k])]

    def direct(owner, k):
        n = once_rows[k]
        return hrx.at[k, pl.ds(pl.multiple_of(owner * d_local + n, 16), d_local - n)]

    def once_copy(k):
        return remote(once(me, k), once(me, k), hsend, orecv.at[k], diag)

    def forward_copy(k):
        return remote(once(diag, k), once(diag, k), hsend, arecv.at[k], peer)

    def cross_copy(k):
        return remote(direct(me, k), direct(me, k), hsend, arecv.at[k], cross)

    def diag_copy(k):
        return remote(direct(me, k), direct(me, k), hsend, arecv.at[k], diag)

    def arrivals(k):
        got = hrx.at[k, pl.ds(0, 2 * d_local - once_rows[k])]
        return remote(got, got, hsend, arecv.at[k], peer)

    peer_copy = remote(own_rows, own_rows, hsend, precv, peer)
    all_sent = remote(hrx.at[pl.ds(0, 3)], hrx.at[pl.ds(0, 3)], hsend, precv, peer)

    def gain_copy(n):
        return remote(grx.at[me], grx.at[me], gsend, grecv.at[n], others[n])

    all_gains = remote(grx.at[pl.ds(0, 3)], grx.at[pl.ds(0, 3)], gsend, grecv.at[0], peer)
    early = n_chunks - 1

    def stat_copy(n, k, sem):
        return remote(stx.at[k], srx.at[k, n], ssend, srecv.at[sem], others[n])

    early_stats = remote(srx.at[pl.ds(0, early)], srx.at[pl.ds(0, early)], ssend, srecv.at[0], peer)
    late_stats = remote(srx.at[early], srx.at[early], ssend, srecv.at[1], peer)
    all_stats = remote(srx, srx, ssend, srecv.at[1], peer)

    for n in range(3):
        gain_copy(n).start()
    once_copy(0).start()
    cross_copy(0).start()
    diag_copy(0).start()
    later_rows = hrx.at[pl.ds(1, n_chunks - 1), pl.ds(pl.multiple_of(me * d_local, d_local), d_local)]
    pltpu.make_async_copy(later_rows, later_rows, own_sem.at[1]).wait()
    peer_copy.start()
    for part in load_w:
        part.start()
    own_t.wait()

    with ns("gainwait"):
        gain_copy(2).wait_recv()
    for k in range(1, n_chunks):
        once_copy(k).start()
        cross_copy(k).start()
        diag_copy(k).start()

    for n in range(2):
        gain_copy(n).wait_recv()
    for s in range(4):
        for lo in range(0, d_local, LANES):
            size = min(LANES, d_local - lo)
            row = grx[s, :, lo : lo + size]
            row = jnp.concatenate([row] * (LANES // size), axis=-1)
            gcol[s * d_local + lo : s * d_local + lo + size, :] = jnp.broadcast_to(row, (LANES, LANES)).T[0:size]

    group = 32

    def normalise(k):
        def square(i, acc):
            at = pl.ds(pl.multiple_of(i * group, group), group)
            part = hrx[k, at, :].astype(jnp.float32)
            return acc + part * part

        sq = lax.fori_loop(0, d_full // group, square, jnp.zeros((group, chunk), jnp.float32), unroll=True)
        inv = lax.rsqrt(jnp.sum(sq, axis=0, keepdims=True) / d_full + NORM_EPS)

        def scale(i, carry):
            at = pl.ds(pl.multiple_of(i * group, group), group)
            gain = gcol[at, :]
            part = hrx[k, at, :].astype(jnp.float32)
            gains = jnp.concatenate([gain] * (chunk // LANES), axis=-1)
            xbuf[at, :] = (part * inv * gains).astype(jnp.bfloat16)
            return carry

        lax.fori_loop(0, d_full // group, scale, 0, unroll=True)

    sub = lax.broadcasted_iota(jnp.int32, (8, chunk), 0)

    def slot_of(j):
        return j % 2 if j < held else 2 + j - held

    def logits(j):
        lo = starts[j]
        size = blocks[j]
        zbuf[slot_of(j), 0:size, :] = jnp.dot(wbuf[lo : lo + size, :], xbuf[...], preferred_element_type=jnp.float32)

    def epilogue(j, want, state):
        lo = starts[j]
        size = blocks[j]

        def tile(i):
            return zbuf[slot_of(j), pl.ds(pl.multiple_of(i * 8, 8), 8), :]

        top = lax.fori_loop(1, size // 8, lambda i, t: jnp.maximum(t, tile(i)), tile(0), unroll=True)
        if state is None:
            total = jnp.zeros((8, chunk), jnp.float32)
            pick = total
        else:
            old, total, pick = state
            top = jnp.maximum(top, old)
            total = total * jnp.exp2((old - top) * LOG2E)

        def add(i, carry):
            total, pick = carry
            z = tile(i)
            total = total + jnp.exp2((z - top) * LOG2E)
            pick = jnp.where(want == lo + i * 8, z, pick)
            return total, pick

        total, pick = lax.fori_loop(0, size // 8, add, (total, pick), unroll=True)
        return top, total, pick

    def finish_chunk(k, state):
        m, total, pick = state
        top = jnp.max(m, axis=0, keepdims=True)
        total = jnp.sum(total * jnp.exp2((m - top) * LOG2E), axis=0, keepdims=True)
        pick = jnp.sum(pick, axis=0, keepdims=True)
        for n, stat in enumerate((top, total, pick)):
            for q in range(chunk // LANES):
                row = n * (chunk // LANES) + q
                stx[k, row : row + 1, :] = stat[:, q * LANES : (q + 1) * LANES]

    with ns("once0"):
        once_copy(0).wait_recv()
    forward_copy(0).start()
    with ns("peer0"):
        peer_copy.wait_recv()
    with ns("fwd0"):
        arrivals(0).wait_recv()
    with ns("wwait"):
        pltpu.make_async_copy(w_ref, wbuf, w_sem).wait()

    def targets_of(k):
        row = tbuf[pl.ds(k // per_chunk, 1), pl.ds(pl.multiple_of(lax.rem(k, per_chunk) * chunk, chunk), chunk)]
        local = row - me * v_local
        local = jnp.where((local >= 0) & (local < v_local), local, jnp.int32(-(1 << 20)))
        return jnp.broadcast_to(local, (8, chunk)) - sub

    def send_stats(k, sem):
        for n in range(3):
            stat_copy(n, k, sem).start()

    def step(k, carry):
        for n in range(n_chunks):
            @pl.when(k == n)
            def _():
                if n:
                    with ns("chunkwait"):
                        arrivals(n).wait_recv()
                if n + 1 < n_chunks:
                    with ns("oncewait"):
                        once_copy(n + 1).wait_recv()
                    forward_copy(n + 1).start()

        @pl.when(k > 1)
        def _():
            send_stats(k - 2, 0)

        normalise(k)
        last_want, *last_state = carry
        want = targets_of(k)
        state = None
        for j in range(n_blocks):
            logits(j)
            if j == 0:
                for i in range(held, n_blocks):
                    last_state = epilogue(i, last_want, last_state)
                finish_chunk(lax.rem(k + n_chunks, n_chunks + 1), last_state)
            elif j <= held:
                state = epilogue(j - 1, want, state)
        if held == n_blocks:
            state = epilogue(held - 1, want, state)
        return (want, *state)

    blank = jnp.zeros((8, chunk), jnp.float32)
    for j in range(held, n_blocks):
        zbuf[slot_of(j), 0 : blocks[j], :] = jnp.zeros((blocks[j], chunk), jnp.float32)
    want, *state = lax.fori_loop(0, n_chunks, step, (jnp.full((8, chunk), -1, jnp.int32), blank, blank, blank))
    send_stats(n_chunks - 2, 0)
    with ns("last"):
        for j in range(held, n_blocks):
            state = epilogue(j, want, state)
        finish_chunk(n_chunks - 1, state)
    send_stats(n_chunks - 1, 1)

    per = chunk // LANES
    for k in range(n_chunks):
        with ns("statwait"):
            if k == 0:
                early_stats.wait_recv()
            if k == early:
                late_stats.wait_recv()
        stats = [stx[k]] + [srx[k, n] for n in range(3)]
        top = stats[0][0:per]
        for st in stats[1:]:
            top = jnp.maximum(top, st[0:per])
        total = jnp.zeros_like(top)
        pick = jnp.zeros_like(top)
        for st in stats:
            total = total + st[per : 2 * per] * jnp.exp2((st[0:per] - top) * LOG2E)
            pick = pick + st[2 * per : 3 * per]
        logp = pick - (top + jnp.log(total))
        seq, pos = divmod(k * chunk, per_seq)
        for q in range(per):
            out_ref[seq : seq + 1, pos + q * LANES : pos + (q + 1) * LANES] = logp[q : q + 1]

    with ns("sendwait"):
        all_sent.wait_send()
        all_gains.wait_send()
        all_stats.wait_send()


def solution(mesh):
    def local_score(hidden, ln_scale, w_head, targets, valid_mask):
        b, l, d_local = hidden.shape
        v_local = w_head.shape[1]
        rows, chunk, block, carried = b * l, 256, 192, 3
        blocks = (block,) * (v_local // block) + ((v_local % block,) if v_local % block else ())
        part = 2048
        w_parts = tuple((lo, min(part, v_local - lo)) for lo in range(0, v_local, part))
        n_chunks = rows // chunk
        once_rows = (d_local * 11 // 12 // 16 * 16, d_local // 3 // 16 * 16) + (d_local // 3 // 16 * 16,) * (n_chunks - 2)
        any_spec = pl.BlockSpec(memory_space=pl.ANY)
        f32 = jnp.float32
        dma = pltpu.SemaphoreType.DMA
        token = pl.pallas_call(
            functools.partial(head_kernel, (d_local, v_local, rows, chunk, blocks, carried, w_parts, once_rows)),
            out_shape=jax.ShapeDtypeStruct((b, l), f32),
            in_specs=[any_spec] * 4,
            out_specs=pl.BlockSpec(memory_space=pltpu.VMEM),
            scratch_shapes=[
                pltpu.VMEM((v_local, 4 * d_local), jnp.bfloat16),
                pltpu.VMEM((n_chunks, 4 * d_local, chunk), jnp.bfloat16),
                pltpu.VMEM((4, 1, d_local), f32),
                pltpu.VMEM((b, l), jnp.int32),
                pltpu.VMEM((4 * d_local, LANES), f32),
                pltpu.VMEM((4 * d_local, chunk), jnp.bfloat16),
                pltpu.VMEM((2 + carried, block, chunk), f32),
                pltpu.VMEM((n_chunks + 1, 8, LANES), f32),
                pltpu.VMEM((n_chunks, 3, 8, LANES), f32),
                dma, dma((2,)), dma((2,)),
                dma, dma, dma((n_chunks,)), dma((n_chunks,)),
                dma, dma((3,)), dma, dma((2,)),
            ],
            compiler_params=pltpu.CompilerParams(
                collective_id=0,
                has_side_effects=True,
                vmem_limit_bytes=40 * 1024 * 1024,
            ),
        )(*[
            pltpu.with_memory_space_constraint(x, pltpu.HBM)
            for x in (hidden.transpose(0, 2, 1), ln_scale.reshape(1, d_local), w_head.T, targets)
        ])
        token_logp = valid_mask.astype(f32) * token
        return token_logp, jnp.sum(token_logp, axis=1)

    return jax.shard_map(
        local_score,
        mesh=mesh,
        in_specs=(P("dp", None, "tp"), P("tp"), P(None, "tp"), P("dp", None), P("dp", None)),
        out_specs=(P("dp", None), P("dp")),
        check_vma=False,
    )
```

```python
import functools

import jax
import jax.numpy as jnp
from jax import lax
from jax.experimental import pallas as pl
from jax.experimental.pallas import tpu as pltpu
from jax.sharding import PartitionSpec as P

NORM_EPS = 1e-6
LOG2E = 1.4426950408889634
MESH = pl.DeviceIdType.MESH
LANES = 128


def head_kernel(
    cfg, h_ref, g_ref, w_ref, tgt_ref, out_ref,
    wbuf, hrx, grx, tbuf, gcol, xbuf, zbuf, stx, srx,
    w_sem, own_sem, small_sem, hsend, precv, orecv, arecv, gsend, grecv, ssend, srecv,
):
    d_local, v_local, rows, chunk, blocks, carried, w_parts, once_rows = cfg
    n_chunks = rows // chunk
    d_full = 4 * d_local
    per_seq = h_ref.shape[2]
    per_chunk = per_seq // chunk
    starts = [sum(blocks[:j]) for j in range(len(blocks))]
    n_blocks = len(blocks)
    held = n_blocks - carried

    me = lax.axis_index("tp")
    peer = me + 1 - 2 * lax.rem(me, 2)
    cross = lax.rem(me + 2, 4)
    diag = lax.rem(peer + 2, 4)
    others = (peer, cross, diag)

    def piece(owner, k):
        return hrx.at[k, pl.ds(pl.multiple_of(owner * d_local, d_local), d_local)]

    own_rows = hrx.at[:, pl.ds(pl.multiple_of(me * d_local, d_local), d_local)]

    own = [
        pltpu.make_async_copy(
            h_ref.at[k // per_chunk, :, pl.ds((k % per_chunk) * chunk, chunk)], piece(me, k), own_sem.at[min(k, 1)]
        )
        for k in range(n_chunks)
    ]
    own_g = pltpu.make_async_copy(g_ref, grx.at[me], small_sem.at[0])
    own_t = pltpu.make_async_copy(tgt_ref, tbuf, small_sem.at[1])
    load_w = [
        pltpu.make_async_copy(w_ref.at[pl.ds(lo, size)], wbuf.at[pl.ds(lo, size)], w_sem)
        for lo, size in w_parts
    ]
    own_g.start()
    for k in range(n_chunks):
        own[k].start()
    own_t.start()

    ns = jax.named_scope
    barrier = pltpu.get_barrier_semaphore()
    for other in others:
        pl.semaphore_signal(barrier, inc=1, device_id={"tp": other}, device_id_type=MESH)
    with ns("own"):
        own_g.wait()
        own[0].wait()
    with ns("barrier"):
        pl.semaphore_wait(barrier, 3)

    def remote(src, dst, send, recv, dev):
        return pltpu.make_async_remote_copy(
            src_ref=src, dst_ref=dst, send_sem=send, recv_sem=recv, device_id={"tp": dev}, device_id_type=MESH
        )

    def once(owner, k):
        return hrx.at[k, pl.ds(pl.multiple_of(owner * d_local, 16), once_rows[k])]

    def direct(owner, k):
        n = once_rows[k]
        return hrx.at[k, pl.ds(pl.multiple_of(owner * d_local + n, 16), d_local - n)]

    def once_copy(k):
        return remote(once(me, k), once(me, k), hsend, orecv.at[k], diag)

    def forward_copy(k):
        return remote(once(diag, k), once(diag, k), hsend, arecv.at[k], peer)

    def cross_copy(k):
        return remote(direct(me, k), direct(me, k), hsend, arecv.at[k], cross)

    def diag_copy(k):
        return remote(direct(me, k), direct(me, k), hsend, arecv.at[k], diag)

    def arrivals(k):
        got = hrx.at[k, pl.ds(0, 2 * d_local - once_rows[k])]
        return remote(got, got, hsend, arecv.at[k], peer)

    peer_copy = remote(own_rows, own_rows, hsend, precv, peer)
    all_sent = remote(hrx.at[pl.ds(0, 3)], hrx.at[pl.ds(0, 3)], hsend, precv, peer)

    def gain_copy(n):
        return remote(grx.at[me], grx.at[me], gsend, grecv.at[n], others[n])

    all_gains = remote(grx.at[pl.ds(0, 3)], grx.at[pl.ds(0, 3)], gsend, grecv.at[0], peer)
    early = n_chunks - 1

    def stat_copy(n, k, sem):
        return remote(stx.at[k], srx.at[k, n], ssend, srecv.at[sem], others[n])

    early_stats = remote(srx.at[pl.ds(0, early)], srx.at[pl.ds(0, early)], ssend, srecv.at[0], peer)
    late_stats = remote(srx.at[early], srx.at[early], ssend, srecv.at[1], peer)
    all_stats = remote(srx, srx, ssend, srecv.at[1], peer)

    for n in range(3):
        gain_copy(n).start()
    once_copy(0).start()
    cross_copy(0).start()
    diag_copy(0).start()
    later_rows = hrx.at[pl.ds(1, n_chunks - 1), pl.ds(pl.multiple_of(me * d_local, d_local), d_local)]
    pltpu.make_async_copy(later_rows, later_rows, own_sem.at[1]).wait()
    peer_copy.start()
    for part in load_w:
        part.start()
    own_t.wait()

    with ns("gainwait"):
        gain_copy(2).wait_recv()
    once_copy(1).start()
    for n in range(2):
        gain_copy(n).wait_recv()
    for k in range(1, n_chunks):
        if k > 1:
            once_copy(k).start()
        cross_copy(k).start()
        diag_copy(k).start()

    for s in range(4):
        for lo in range(0, d_local, LANES):
            size = min(LANES, d_local - lo)
            row = grx[s, :, lo : lo + size]
            row = jnp.concatenate([row] * (LANES // size), axis=-1)
            gcol[s * d_local + lo : s * d_local + lo + size, :] = jnp.broadcast_to(row, (LANES, LANES)).T[0:size]

    group = 32

    def normalise(k):
        def square(i, acc):
            at = pl.ds(pl.multiple_of(i * group, group), group)
            part = hrx[k, at, :].astype(jnp.float32)
            return acc + part * part

        sq = lax.fori_loop(0, d_full // group, square, jnp.zeros((group, chunk), jnp.float32), unroll=True)
        inv = lax.rsqrt(jnp.sum(sq, axis=0, keepdims=True) / d_full + NORM_EPS)

        def scale(i, carry):
            at = pl.ds(pl.multiple_of(i * group, group), group)
            gain = gcol[at, :]
            part = hrx[k, at, :].astype(jnp.float32)
            gains = jnp.concatenate([gain] * (chunk // LANES), axis=-1)
            xbuf[at, :] = (part * inv * gains).astype(jnp.bfloat16)
            return carry

        lax.fori_loop(0, d_full // group, scale, 0, unroll=True)

    sub = lax.broadcasted_iota(jnp.int32, (8, chunk), 0)

    def slot_of(j):
        return j % 2 if j < held else 2 + j - held

    def logits(j):
        lo = starts[j]
        size = blocks[j]
        zbuf[slot_of(j), 0:size, :] = jnp.dot(wbuf[lo : lo + size, :], xbuf[...], preferred_element_type=jnp.float32)

    def epilogue(j, want, state):
        lo = starts[j]
        size = blocks[j]

        def tile(i):
            return zbuf[slot_of(j), pl.ds(pl.multiple_of(i * 8, 8), 8), :]

        top = lax.fori_loop(1, size // 8, lambda i, t: jnp.maximum(t, tile(i)), tile(0), unroll=True)
        if state is None:
            total = jnp.zeros((8, chunk), jnp.float32)
            pick = total
        else:
            old, total, pick = state
            top = jnp.maximum(top, old)
            total = total * jnp.exp2((old - top) * LOG2E)

        def add(i, carry):
            total, pick = carry
            z = tile(i)
            total = total + jnp.exp2((z - top) * LOG2E)
            pick = jnp.where(want == lo + i * 8, z, pick)
            return total, pick

        total, pick = lax.fori_loop(0, size // 8, add, (total, pick), unroll=True)
        return top, total, pick

    def finish_chunk(k, state):
        m, total, pick = state
        top = jnp.max(m, axis=0, keepdims=True)
        total = jnp.sum(total * jnp.exp2((m - top) * LOG2E), axis=0, keepdims=True)
        pick = jnp.sum(pick, axis=0, keepdims=True)
        for n, stat in enumerate((top, total, pick)):
            for q in range(chunk // LANES):
                row = n * (chunk // LANES) + q
                stx[k, row : row + 1, :] = stat[:, q * LANES : (q + 1) * LANES]

    with ns("once0"):
        once_copy(0).wait_recv()
    forward_copy(0).start()
    with ns("peer0"):
        peer_copy.wait_recv()
    with ns("fwd0"):
        arrivals(0).wait_recv()
    with ns("wwait"):
        pltpu.make_async_copy(w_ref, wbuf, w_sem).wait()

    def targets_of(k):
        row = tbuf[pl.ds(k // per_chunk, 1), pl.ds(pl.multiple_of(lax.rem(k, per_chunk) * chunk, chunk), chunk)]
        local = row - me * v_local
        local = jnp.where((local >= 0) & (local < v_local), local, jnp.int32(-(1 << 20)))
        return jnp.broadcast_to(local, (8, chunk)) - sub

    def send_stats(k, sem):
        for n in range(3):
            stat_copy(n, k, sem).start()

    def step(k, carry):
        for n in range(n_chunks):
            @pl.when(k == n)
            def _():
                if n:
                    with ns("chunkwait"):
                        arrivals(n).wait_recv()
                if n + 1 < n_chunks:
                    with ns("oncewait"):
                        once_copy(n + 1).wait_recv()
                    forward_copy(n + 1).start()

        @pl.when(k > 1)
        def _():
            send_stats(k - 2, 0)

        normalise(k)
        last_want, *last_state = carry
        want = targets_of(k)
        state = None
        for j in range(n_blocks):
            logits(j)
            if j == 0:
                for i in range(held, n_blocks):
                    last_state = epilogue(i, last_want, last_state)
                finish_chunk(lax.rem(k + n_chunks, n_chunks + 1), last_state)
            elif j <= held:
                state = epilogue(j - 1, want, state)
        if held == n_blocks:
            state = epilogue(held - 1, want, state)
        return (want, *state)

    blank = jnp.zeros((8, chunk), jnp.float32)
    for j in range(held, n_blocks):
        zbuf[slot_of(j), 0 : blocks[j], :] = jnp.zeros((blocks[j], chunk), jnp.float32)
    want, *state = lax.fori_loop(0, n_chunks, step, (jnp.full((8, chunk), -1, jnp.int32), blank, blank, blank))
    send_stats(n_chunks - 2, 0)
    with ns("last"):
        for j in range(held, n_blocks):
            state = epilogue(j, want, state)
        finish_chunk(n_chunks - 1, state)
    send_stats(n_chunks - 1, 1)

    per = chunk // LANES
    for k in range(n_chunks):
        with ns("statwait"):
            if k == 0:
                early_stats.wait_recv()
            if k == early:
                late_stats.wait_recv()
        stats = [stx[k]] + [srx[k, n] for n in range(3)]
        top = stats[0][0:per]
        for st in stats[1:]:
            top = jnp.maximum(top, st[0:per])
        total = jnp.zeros_like(top)
        pick = jnp.zeros_like(top)
        for st in stats:
            total = total + st[per : 2 * per] * jnp.exp2((st[0:per] - top) * LOG2E)
            pick = pick + st[2 * per : 3 * per]
        logp = pick - (top + jnp.log(total))
        seq, pos = divmod(k * chunk, per_seq)
        for q in range(per):
            out_ref[seq : seq + 1, pos + q * LANES : pos + (q + 1) * LANES] = logp[q : q + 1]

    with ns("sendwait"):
        all_sent.wait_send()
        all_gains.wait_send()
        all_stats.wait_send()


def solution(mesh):
    def local_score(hidden, ln_scale, w_head, targets, valid_mask):
        b, l, d_local = hidden.shape
        v_local = w_head.shape[1]
        rows, chunk, block, carried = b * l, 256, 192, 3
        blocks = (block,) * (v_local // block) + ((v_local % block,) if v_local % block else ())
        part = 2048
        w_parts = tuple((lo, min(part, v_local - lo)) for lo in range(0, v_local, part))
        n_chunks = rows // chunk
        once_rows = (d_local * 11 // 12 // 16 * 16, d_local // 3 // 16 * 16) + (d_local // 3 // 16 * 16,) * (n_chunks - 2)
        any_spec = pl.BlockSpec(memory_space=pl.ANY)
        f32 = jnp.float32
        dma = pltpu.SemaphoreType.DMA
        token = pl.pallas_call(
            functools.partial(head_kernel, (d_local, v_local, rows, chunk, blocks, carried, w_parts, once_rows)),
            out_shape=jax.ShapeDtypeStruct((b, l), f32),
            in_specs=[any_spec] * 4,
            out_specs=pl.BlockSpec(memory_space=pltpu.VMEM),
            scratch_shapes=[
                pltpu.VMEM((v_local, 4 * d_local), jnp.bfloat16),
                pltpu.VMEM((n_chunks, 4 * d_local, chunk), jnp.bfloat16),
                pltpu.VMEM((4, 1, d_local), f32),
                pltpu.VMEM((b, l), jnp.int32),
                pltpu.VMEM((4 * d_local, LANES), f32),
                pltpu.VMEM((4 * d_local, chunk), jnp.bfloat16),
                pltpu.VMEM((2 + carried, block, chunk), f32),
                pltpu.VMEM((n_chunks + 1, 8, LANES), f32),
                pltpu.VMEM((n_chunks, 3, 8, LANES), f32),
                dma, dma((2,)), dma((2,)),
                dma, dma, dma((n_chunks,)), dma((n_chunks,)),
                dma, dma((3,)), dma, dma((2,)),
            ],
            compiler_params=pltpu.CompilerParams(
                collective_id=0,
                has_side_effects=True,
                vmem_limit_bytes=40 * 1024 * 1024,
            ),
        )(*[
            pltpu.with_memory_space_constraint(x, pltpu.HBM)
            for x in (hidden.transpose(0, 2, 1), ln_scale.reshape(1, d_local), w_head.T, targets)
        ])
        token_logp = valid_mask.astype(f32) * token
        return token_logp, jnp.sum(token_logp, axis=1)

    return jax.shard_map(
        local_score,
        mesh=mesh,
        in_specs=(P("dp", None, "tp"), P("tp"), P(None, "tp"), P("dp", None), P("dp", None)),
        out_specs=(P("dp", None), P("dp")),
        check_vma=False,
    )
```

```python
import functools

import jax
import jax.numpy as jnp
from jax import lax
from jax.experimental import pallas as pl
from jax.experimental.pallas import tpu as pltpu
from jax.sharding import PartitionSpec as P

NORM_EPS = 1e-6
LOG2E = 1.4426950408889634
MESH = pl.DeviceIdType.MESH
LANES = 128


def head_kernel(
    cfg, h_ref, g_ref, w_ref, tgt_ref, out_ref,
    wbuf, hrx, grx, tbuf, gcol, xbuf, zbuf, stx, srx,
    w_sem, own_sem, small_sem, hsend, precv, orecv, arecv, gsend, grecv, ssend, srecv,
):
    d_local, v_local, rows, chunk, blocks, carried, w_parts, once_rows = cfg
    n_chunks = rows // chunk
    d_full = 4 * d_local
    per_seq = h_ref.shape[2]
    per_chunk = per_seq // chunk
    starts = [sum(blocks[:j]) for j in range(len(blocks))]
    n_blocks = len(blocks)
    held = n_blocks - carried

    me = lax.axis_index("tp")
    peer = me + 1 - 2 * lax.rem(me, 2)
    cross = lax.rem(me + 2, 4)
    diag = lax.rem(peer + 2, 4)
    others = (peer, cross, diag)

    def piece(owner, k):
        return hrx.at[k, pl.ds(pl.multiple_of(owner * d_local, d_local), d_local)]

    own_rows = hrx.at[:, pl.ds(pl.multiple_of(me * d_local, d_local), d_local)]

    own = [
        pltpu.make_async_copy(
            h_ref.at[k // per_chunk, :, pl.ds((k % per_chunk) * chunk, chunk)], piece(me, k), own_sem.at[min(k, 1)]
        )
        for k in range(n_chunks)
    ]
    own_g = pltpu.make_async_copy(g_ref, grx.at[me], small_sem.at[0])
    own_t = pltpu.make_async_copy(tgt_ref, tbuf, small_sem.at[1])
    load_w = [
        pltpu.make_async_copy(w_ref.at[pl.ds(lo, size)], wbuf.at[pl.ds(lo, size)], w_sem)
        for lo, size in w_parts
    ]
    own_g.start()
    for k in range(n_chunks):
        own[k].start()
    own_t.start()

    ns = jax.named_scope
    barrier = pltpu.get_barrier_semaphore()
    for other in others:
        pl.semaphore_signal(barrier, inc=1, device_id={"tp": other}, device_id_type=MESH)
    with ns("own"):
        own_g.wait()
        own[0].wait()
    with ns("barrier"):
        pl.semaphore_wait(barrier, 3)

    def remote(src, dst, send, recv, dev):
        return pltpu.make_async_remote_copy(
            src_ref=src, dst_ref=dst, send_sem=send, recv_sem=recv, device_id={"tp": dev}, device_id_type=MESH
        )

    def once(owner, k):
        return hrx.at[k, pl.ds(pl.multiple_of(owner * d_local, 16), once_rows[k])]

    def direct(owner, k):
        n = once_rows[k]
        return hrx.at[k, pl.ds(pl.multiple_of(owner * d_local + n, 16), d_local - n)]

    def once_copy(k):
        return remote(once(me, k), once(me, k), hsend, orecv.at[k], diag)

    def forward_copy(k):
        return remote(once(diag, k), once(diag, k), hsend, arecv.at[k], peer)

    def cross_copy(k):
        return remote(direct(me, k), direct(me, k), hsend, arecv.at[k], cross)

    def diag_copy(k):
        return remote(direct(me, k), direct(me, k), hsend, arecv.at[k], diag)

    def arrivals(k):
        got = hrx.at[k, pl.ds(0, 2 * d_local - once_rows[k])]
        return remote(got, got, hsend, arecv.at[k], peer)

    peer_copy = remote(own_rows, own_rows, hsend, precv, peer)
    all_sent = remote(hrx.at[pl.ds(0, 3)], hrx.at[pl.ds(0, 3)], hsend, precv, peer)

    def gain_copy(n):
        return remote(grx.at[me], grx.at[me], gsend, grecv, others[n])

    all_gains = remote(grx.at[pl.ds(0, 3)], grx.at[pl.ds(0, 3)], gsend, grecv, peer)
    early = n_chunks - 1

    def stat_copy(n, k, sem):
        return remote(stx.at[k], srx.at[k, n], ssend, srecv.at[sem], others[n])

    early_stats = remote(srx.at[pl.ds(0, early)], srx.at[pl.ds(0, early)], ssend, srecv.at[0], peer)
    late_stats = remote(srx.at[early], srx.at[early], ssend, srecv.at[1], peer)
    all_stats = remote(srx, srx, ssend, srecv.at[1], peer)

    for n in range(3):
        gain_copy(n).start()
    once_copy(0).start()
    cross_copy(0).start()
    diag_copy(0).start()
    later_rows = hrx.at[pl.ds(1, n_chunks - 1), pl.ds(pl.multiple_of(me * d_local, d_local), d_local)]
    pltpu.make_async_copy(later_rows, later_rows, own_sem.at[1]).wait()
    peer_copy.start()
    for part in load_w:
        part.start()
    own_t.wait()

    with ns("gainwait"):
        all_gains.wait_recv()
    once_copy(1).start()

    for s in range(4):
        for lo in range(0, d_local, LANES):
            size = min(LANES, d_local - lo)
            row = grx[s, :, lo : lo + size]
            row = jnp.concatenate([row] * (LANES // size), axis=-1)
            gcol[s * d_local + lo : s * d_local + lo + size, :] = jnp.broadcast_to(row, (LANES, LANES)).T[0:size]

    for k in range(1, n_chunks):
        if k > 1:
            once_copy(k).start()
        cross_copy(k).start()
        diag_copy(k).start()

    group = 32

    def normalise(k):
        def square(i, acc):
            at = pl.ds(pl.multiple_of(i * group, group), group)
            part = hrx[k, at, :].astype(jnp.float32)
            return acc + part * part

        sq = lax.fori_loop(0, d_full // group, square, jnp.zeros((group, chunk), jnp.float32), unroll=True)
        inv = lax.rsqrt(jnp.sum(sq, axis=0, keepdims=True) / d_full + NORM_EPS)

        def scale(i, carry):
            at = pl.ds(pl.multiple_of(i * group, group), group)
            gain = gcol[at, :]
            part = hrx[k, at, :].astype(jnp.float32)
            gains = jnp.concatenate([gain] * (chunk // LANES), axis=-1)
            xbuf[at, :] = (part * inv * gains).astype(jnp.bfloat16)
            return carry

        lax.fori_loop(0, d_full // group, scale, 0, unroll=True)

    sub = lax.broadcasted_iota(jnp.int32, (8, chunk), 0)

    def slot_of(j):
        return j % 2 if j < held else 2 + j - held

    def logits(j):
        lo = starts[j]
        size = blocks[j]
        zbuf[slot_of(j), 0:size, :] = jnp.dot(wbuf[lo : lo + size, :], xbuf[...], preferred_element_type=jnp.float32)

    def epilogue(j, want, state):
        lo = starts[j]
        size = blocks[j]

        def tile(i):
            return zbuf[slot_of(j), pl.ds(pl.multiple_of(i * 8, 8), 8), :]

        top = lax.fori_loop(1, size // 8, lambda i, t: jnp.maximum(t, tile(i)), tile(0), unroll=True)
        if state is None:
            total = jnp.zeros((8, chunk), jnp.float32)
            pick = total
        else:
            old, total, pick = state
            top = jnp.maximum(top, old)
            total = total * jnp.exp2((old - top) * LOG2E)

        def add(i, carry):
            total, pick = carry
            z = tile(i)
            total = total + jnp.exp2((z - top) * LOG2E)
            pick = jnp.where(want == lo + i * 8, z, pick)
            return total, pick

        total, pick = lax.fori_loop(0, size // 8, add, (total, pick), unroll=True)
        return top, total, pick

    def finish_chunk(k, state):
        m, total, pick = state
        top = jnp.max(m, axis=0, keepdims=True)
        total = jnp.sum(total * jnp.exp2((m - top) * LOG2E), axis=0, keepdims=True)
        pick = jnp.sum(pick, axis=0, keepdims=True)
        for n, stat in enumerate((top, total, pick)):
            for q in range(chunk // LANES):
                row = n * (chunk // LANES) + q
                stx[k, row : row + 1, :] = stat[:, q * LANES : (q + 1) * LANES]

    with ns("once0"):
        once_copy(0).wait_recv()
    forward_copy(0).start()
    with ns("peer0"):
        peer_copy.wait_recv()
    with ns("fwd0"):
        arrivals(0).wait_recv()
    with ns("wwait"):
        pltpu.make_async_copy(w_ref, wbuf, w_sem).wait()

    def targets_of(k):
        row = tbuf[pl.ds(k // per_chunk, 1), pl.ds(pl.multiple_of(lax.rem(k, per_chunk) * chunk, chunk), chunk)]
        local = row - me * v_local
        local = jnp.where((local >= 0) & (local < v_local), local, jnp.int32(-(1 << 20)))
        return jnp.broadcast_to(local, (8, chunk)) - sub

    def send_stats(k, sem):
        for n in range(3):
            stat_copy(n, k, sem).start()

    def step(k, carry):
        for n in range(n_chunks):
            @pl.when(k == n)
            def _():
                if n:
                    with ns("chunkwait"):
                        arrivals(n).wait_recv()
                if n + 1 < n_chunks:
                    with ns("oncewait"):
                        once_copy(n + 1).wait_recv()
                    forward_copy(n + 1).start()

        @pl.when(k > 1)
        def _():
            send_stats(k - 2, 0)

        normalise(k)
        last_want, *last_state = carry
        want = targets_of(k)
        state = None
        for j in range(n_blocks):
            logits(j)
            if j == 0:
                for i in range(held, n_blocks):
                    last_state = epilogue(i, last_want, last_state)
                finish_chunk(lax.rem(k + n_chunks, n_chunks + 1), last_state)
            elif j <= held:
                state = epilogue(j - 1, want, state)
        if held == n_blocks:
            state = epilogue(held - 1, want, state)
        return (want, *state)

    blank = jnp.zeros((8, chunk), jnp.float32)
    for j in range(held, n_blocks):
        zbuf[slot_of(j), 0 : blocks[j], :] = jnp.zeros((blocks[j], chunk), jnp.float32)
    want, *state = lax.fori_loop(0, n_chunks, step, (jnp.full((8, chunk), -1, jnp.int32), blank, blank, blank))
    send_stats(n_chunks - 2, 0)
    with ns("last"):
        for j in range(held, n_blocks):
            state = epilogue(j, want, state)
        finish_chunk(n_chunks - 1, state)
    send_stats(n_chunks - 1, 1)

    per = chunk // LANES
    for k in range(n_chunks):
        with ns("statwait"):
            if k == 0:
                early_stats.wait_recv()
            if k == early:
                late_stats.wait_recv()
        stats = [stx[k]] + [srx[k, n] for n in range(3)]
        top = stats[0][0:per]
        for st in stats[1:]:
            top = jnp.maximum(top, st[0:per])
        total = jnp.zeros_like(top)
        pick = jnp.zeros_like(top)
        for st in stats:
            total = total + st[per : 2 * per] * jnp.exp2((st[0:per] - top) * LOG2E)
            pick = pick + st[2 * per : 3 * per]
        logp = pick - (top + jnp.log(total))
        seq, pos = divmod(k * chunk, per_seq)
        for q in range(per):
            out_ref[seq : seq + 1, pos + q * LANES : pos + (q + 1) * LANES] = logp[q : q + 1]

    with ns("sendwait"):
        all_sent.wait_send()
        all_gains.wait_send()
        all_stats.wait_send()


def solution(mesh):
    def local_score(hidden, ln_scale, w_head, targets, valid_mask):
        b, l, d_local = hidden.shape
        v_local = w_head.shape[1]
        rows, chunk, block, carried = b * l, 256, 192, 3
        blocks = (block,) * (v_local // block) + ((v_local % block,) if v_local % block else ())
        part = 2048
        w_parts = tuple((lo, min(part, v_local - lo)) for lo in range(0, v_local, part))
        n_chunks = rows // chunk
        once_rows = (d_local * 11 // 12 // 16 * 16, d_local // 3 // 16 * 16) + (d_local // 3 // 16 * 16,) * (n_chunks - 2)
        any_spec = pl.BlockSpec(memory_space=pl.ANY)
        f32 = jnp.float32
        dma = pltpu.SemaphoreType.DMA
        token = pl.pallas_call(
            functools.partial(head_kernel, (d_local, v_local, rows, chunk, blocks, carried, w_parts, once_rows)),
            out_shape=jax.ShapeDtypeStruct((b, l), f32),
            in_specs=[any_spec] * 4,
            out_specs=pl.BlockSpec(memory_space=pltpu.VMEM),
            scratch_shapes=[
                pltpu.VMEM((v_local, 4 * d_local), jnp.bfloat16),
                pltpu.VMEM((n_chunks, 4 * d_local, chunk), jnp.bfloat16),
                pltpu.VMEM((4, 1, d_local), f32),
                pltpu.VMEM((b, l), jnp.int32),
                pltpu.VMEM((4 * d_local, LANES), f32),
                pltpu.VMEM((4 * d_local, chunk), jnp.bfloat16),
                pltpu.VMEM((2 + carried, block, chunk), f32),
                pltpu.VMEM((n_chunks + 1, 8, LANES), f32),
                pltpu.VMEM((n_chunks, 3, 8, LANES), f32),
                dma, dma((2,)), dma((2,)),
                dma, dma, dma((n_chunks,)), dma((n_chunks,)),
                dma, dma, dma, dma((2,)),
            ],
            compiler_params=pltpu.CompilerParams(
                collective_id=0,
                has_side_effects=True,
                vmem_limit_bytes=40 * 1024 * 1024,
            ),
        )(*[
            pltpu.with_memory_space_constraint(x, pltpu.HBM)
            for x in (hidden.transpose(0, 2, 1), ln_scale.reshape(1, d_local), w_head.T, targets)
        ])
        token_logp = valid_mask.astype(f32) * token
        return token_logp, jnp.sum(token_logp, axis=1)

    return jax.shard_map(
        local_score,
        mesh=mesh,
        in_specs=(P("dp", None, "tp"), P("tp"), P(None, "tp"), P("dp", None), P("dp", None)),
        out_specs=(P("dp", None), P("dp")),
        check_vma=False,
    )
```
